16 devices in a mesh: rep: 2 (over y, z), dp: 8 (over x, core).
Axes of the slice: x: 4, y: 2, z: 1, core: 2. Of those that a mesh axis runs over, the one named last changes fastest.
The devices are a block of a 4x4x8 slice.
Arguments:
- x: bfloat16 [16, 2048, 1024], P(('rep', 'dp')), parts along dimension 0
- dy: bfloat16 [16, 2048, 1024], P(('rep', 'dp')), parts along dimension 0
- w_gate: bfloat16 [2, 1024, 2816], replicated
- w_up: bfloat16 [2, 1024, 2816], replicated
- w_down: bfloat16 [2, 2816, 1024], replicated
- m_w_gate: float32 [2, 1024, 2816], P(None, 'dp')
- m_w_up: float32 [2, 1024, 2816], P(None, 'dp')
- m_w_down: float32 [2, 2816, 1024], P(None, 'dp')
- v_w_gate: float32 [2, 1024, 2816], P(None, 'dp')
- v_w_up: float32 [2, 1024, 2816], P(None, 'dp')
- v_w_down: float32 [2, 2816, 1024], P(None, 'dp')
Outputs:
- output 1: bfloat16 [4, 1024, 2816], P('rep'), parts along dimension 0
- output 2: bfloat16 [4, 1024, 2816], P('rep'), parts along dimension 0
- output 3: bfloat16 [4, 2816, 1024], P('rep'), parts along dimension 0
- output 4: float32 [4, 1024, 2816], P('rep', 'dp'), parts along dimension 0
- output 5: float32 [4, 1024, 2816], P('rep', 'dp'), parts along dimension 0
- output 6: float32 [4, 2816, 1024], P('rep', 'dp'), parts along dimension 0
- output 7: float32 [4, 1024, 2816], P('rep', 'dp'), parts along dimension 0
- output 8: float32 [4, 1024, 2816], P('rep', 'dp'), parts along dimension 0
- output 9: float32 [4, 2816, 1024], P('rep', 'dp'), parts along dimension 0
There are 2 independent parts. The reference program is written for one: setup_inputs(seed, part) draws one part's arguments, and reference() takes and returns one part's arrays. A program takes and returns all parts, laid end to end along the dimension named above; an argument that names none is the same for every part.
All inputs are finite; a program needn't handle non-finite values.
Results may differ from the reference program's by a relative error of at most 0.022.
Values are sent between devices in bfloat16 or wider.
A program may use at most 768 MiB of HBM per device.

```python
import jax
import jax.numpy as jnp
from jax import lax

SEQUENCES = 8
TOKENS = 2048
D = 1024
FF = 2816
LAYERS = 2
NAMES = ("w_gate", "w_up", "w_down")
SHAPES = {"w_gate": (LAYERS, D, FF), "w_up": (LAYERS, D, FF), "w_down": (LAYERS, FF, D)}


def bump(key, n, height):
    away = (jnp.arange(n, dtype=jnp.int32) - jax.random.randint(key, (), 0, n, jnp.int32)) % n
    return jnp.where(away < n // 8, height, 1.0)


def together(key, own, strength):
    shared = jax.random.normal(key, own.shape[1:], jnp.float32)
    return (own + strength * shared) * lax.rsqrt(1 + strength * strength)


def setup_inputs(seed: int = 0, part: int = 0) -> dict:
    kx, kdy, ka, kb, kz, kf, kh, kl, *keys = jax.random.split(jax.random.key(seed), 8 + 3 * len(NAMES))
    kx, kdy, ka, kb = (jax.random.fold_in(k, part) for k in (kx, kdy, ka, kb))
    kw, km, kv = (keys[i::3] for i in range(3))
    shape = (SEQUENCES, TOKENS, D)
    much_x, much_dy = jax.random.uniform(kz, (2,), jnp.float32, 0.0, 1.0)
    loud = 2.0 ** jax.random.uniform(jax.random.fold_in(kz, 1), (), jnp.float32, -1.0, 2.0)
    layers = 2.0 ** jax.random.uniform(kl, (LAYERS, 1, 1), jnp.float32, -1.0, 1.0)
    x = together(ka, jax.random.normal(kx, shape, jnp.float32), much_x) * bump(kf, D, 4.0)
    dy = together(kb, jax.random.normal(kdy, shape, jnp.float32), much_dy)
    drawn = {"x": x.astype(jnp.bfloat16), "dy": (loud * dy * (SEQUENCES * TOKENS) ** -0.5).astype(jnp.bfloat16)}
    for key, name in zip(kw, NAMES, strict=True):
        w = jax.random.normal(key, SHAPES[name], jnp.float32) * SHAPES[name][1] ** -0.5
        drawn[name] = (w * {"w_gate": 1.0, "w_up": bump(kh, FF, 4.0), "w_down": layers}[name]).astype(jnp.bfloat16)
    for key, name in zip(km, NAMES, strict=True):
        drawn[f"m_{name}"] = 0.1 * jax.random.normal(key, SHAPES[name], jnp.float32)
    for key, name in zip(kv, NAMES, strict=True):
        drawn[f"v_{name}"] = jax.random.uniform(key, SHAPES[name], jnp.float32, 0.005, 0.015)
    return drawn


def matmul(a, w):
    return jnp.dot(a, w, preferred_element_type=jnp.float32).astype(jnp.bfloat16)


def normed(h):
    wide = h.astype(jnp.float32)
    scale = lax.rsqrt(jnp.mean(wide**2, -1, keepdims=True) + 1e-6)
    return (wide * scale).astype(jnp.bfloat16)


def layer(h, w):
    a = normed(h)
    gate = jnp.dot(a, w["w_gate"], preferred_element_type=jnp.float32)
    up = jnp.dot(a, w["w_up"], preferred_element_type=jnp.float32)
    return h + matmul((jax.nn.silu(gate) * up).astype(jnp.bfloat16), w["w_down"])


def adamw(w, m, v, g):
    m = 0.9 * m + 0.1 * g
    v = 0.95 * v + 0.05 * g * g
    step = m * lax.rsqrt(v + 1e-8) + 0.1 * w
    return (w - 0.02 * step).astype(jnp.bfloat16), m, v


def clipped(gradients, sum_of_squares, count):
    factor = jnp.minimum(1.0, 0.5 * lax.rsqrt(sum_of_squares / count + 1e-30))
    return [g * factor for g in gradients]


def stack(weights, h):
    return lax.scan(lambda h, w: (layer(h, w), None), h, weights)[0]


def reference(x, dy, w_gate, w_up, w_down, m_w_gate, m_w_up, m_w_down, v_w_gate, v_w_up, v_w_down):
    weights = dict(zip(NAMES, (w_gate, w_up, w_down), strict=True))

    def take(so_far, sequence):
        h, by_y = sequence
        _, back = jax.vjp(lambda w: stack(w, h), weights)
        return jax.tree.map(lambda total, term: total + term.astype(jnp.float32), so_far, back(by_y)[0]), None

    none_yet = {name: jnp.zeros(w.shape, jnp.float32) for name, w in weights.items()}
    by_weights, _ = lax.scan(take, none_yet, (x, dy))
    gradients = [by_weights[name].astype(jnp.bfloat16).astype(jnp.float32) for name in NAMES]
    gradients = clipped(gradients, sum(jnp.sum(g * g) for g in gradients), sum(g.size for g in gradients))
    new = [
        adamw(w.astype(jnp.float32), m, v, g)
        for w, m, v, g in zip((w_gate, w_up, w_down), (m_w_gate, m_w_up, m_w_down), (v_w_gate, v_w_up, v_w_down), gradients, strict=True)
    ]
    return tuple(one[which] for which in range(3) for one in new)
```

```python
import functools

import jax
import jax.numpy as jnp
from jax import lax
from jax.experimental import pallas as pl
from jax.experimental.pallas import tpu as pltpu
from jax.sharding import PartitionSpec as P

MESH = pl.DeviceIdType.MESH
F32, BF16 = jnp.float32, jnp.bfloat16
CORES = 2


def places(axis, n):
    me = lax.axis_index(axis)
    chips = n // CORES
    core, chip = lax.rem(me, CORES), lax.div(me, CORES)
    at = lambda away: lax.rem(chip + away, chips) * CORES + core
    return me, core, me + 1 - 2 * core, at(1), at(chips - 1), at(2)


def finish_kernel(n, count, pieces, *refs):
    g_in, w_in, m_in, v_in, w_out, m_out, v_out = (refs[3 * i : 3 * i + 3] for i in range(7))
    g, w, m, v, new = (refs[21 + 3 * i : 24 + 3 * i] for i in range(5))
    parts, load_sem, own_sem, store_sem, part_send, part_recv, send, recv = refs[36:]
    me, core, partner, after, before, across = places("dp", n)

    barrier = pltpu.get_barrier_semaphore()
    peers = [lax.rem(me + away, n) for away in range(1, n)]
    for peer in peers:
        pl.semaphore_signal(barrier, inc=1, device_id={"dp": peer}, device_id_type=MESH)

    loads = []
    for i in range(3):
        loads.append(pltpu.make_async_copy(g_in[i], g[i], load_sem.at[i]))
    for i in (2, 0, 1):
        rows = g[i].shape[1]
        mine = pl.ds(pl.multiple_of(me * rows, 16), rows)
        loads.append(pltpu.make_async_copy(w_in[i].at[:, mine], w[i], load_sem.at[3 + i]))
        loads.append(pltpu.make_async_copy(m_in[i], m[i], load_sem.at[6 + i]))
        loads.append(pltpu.make_async_copy(v_in[i], v[i], load_sem.at[9 + i]))
    for one in loads:
        one.start()

    total = jnp.zeros((8, 128), F32)
    for i in range(3):
        loads[i].wait()
        layers, rows, columns = g[i].shape

        def squares(step, total, ref=g[i], columns=columns, rows=rows):
            block = ref[lax.div(step, rows // 16), pl.ds(pl.multiple_of(lax.rem(step, rows // 16) * 16, 16), 16), :].astype(F32)
            block = block * block
            for at in range(0, columns, 128):
                total += block[:8, at : at + 128] + block[8:, at : at + 128]
            return total

        total = lax.fori_loop(0, layers * rows // 16, squares, total)
    parts[pl.ds(me, 1)] = total[None]
    pl.semaphore_wait(barrier, n - 1)
    part_copies = []
    for k, peer in enumerate(peers):
        part_copies.append(
            pltpu.make_async_remote_copy(
                parts.at[me], parts.at[me], part_send.at[k], part_recv.at[k], device_id={"dp": peer}, device_id_type=MESH
            )
        )
        part_copies[-1].start()
    for one in part_copies:
        one.wait_recv()
    every = parts[0]
    for k in range(1, n):
        every += parts[k]
    mean = jnp.sum(every, keepdims=True) / count
    factor = jnp.minimum(1.0, 0.5 * lax.rsqrt(mean + 1e-30))

    def adamw(i, layer, first, rows):
        step_rows = 16
        columns = g[i].shape[2]

        def body(step, _):
            at = (layer, pl.ds(pl.multiple_of(first + step * step_rows, 16), step_rows), slice(None))
            grad = g[i][at].astype(F32) * factor
            m_new = 0.9 * m[i][at] + 0.1 * grad
            v_new = 0.95 * v[i][at] + 0.05 * grad * grad
            w_old = w[i][at].astype(F32)
            m[i][at] = m_new
            v[i][at] = v_new
            new[i][at] = (w_old - 0.02 * (m_new * lax.rsqrt(v_new + 1e-8) + 0.1 * w_old)).astype(BF16)
            return 0

        lax.fori_loop(0, rows // step_rows, body, 0)

    def rows_of(i, owner, first, rows):
        return pl.ds(pl.multiple_of(owner * g[i].shape[1] + first, 16), rows)

    def remote(kind, number, src, dst, to):
        return pltpu.make_async_remote_copy(
            src, dst, send.at[kind, number], recv.at[kind, number], device_id={"dp": to}, device_id_type=MESH
        )

    def piece(number):
        i, layer, first, rows = pieces[number]
        place = lambda owner, columns=slice(None): w_out[i].at[layer, rows_of(i, owner, first, rows), columns]
        half = g[i].shape[2] // 2
        left, right = pl.ds(0, half), pl.ds(half, half)
        mine = new[i].at[layer, pl.ds(first, rows)]
        copies = {
            "after": remote(0, number, mine, place(me), after),
            "before": remote(1, number, mine, place(me), before),
            "partner": remote(2, number, mine, place(me), partner),
            "on": remote(3, number, place(before, left), place(before, left), after),
            "back": remote(4, number, place(after, right), place(after, right), before),
            "partner_before": remote(5, number, place(before), place(before), partner),
            "partner_after": remote(6, number, place(after), place(after), partner),
            "partner_left": remote(7, number, place(across, left), place(across, left), partner),
            "partner_right": remote(8, number, place(across, right), place(across, right), partner),
        }
        local = pltpu.make_async_copy(mine, place(me), own_sem.at[number])
        stores = [
            pltpu.make_async_copy(t[i].at[layer, pl.ds(first, rows)], o[i].at[layer, pl.ds(first, rows)], store_sem.at[k, number])
            for k, (t, o) in enumerate(((m, m_out), (v, v_out)))
        ]
        return copies, [local, *stores]

    waited = set()
    total_pieces = len(pieces)
    made = [piece(number) for number in range(total_pieces)]

    def compute(number):
        i, layer, first, rows = pieces[number]
        if i not in waited:
            waited.add(i)
            for one in loads[3 + 3 * (2, 0, 1).index(i) :][:3]:
                one.wait()
        adamw(i, layer, first, rows)

    compute(0)
    for number in range(total_pieces + 2):
        if number + 1 < total_pieces:
            compute(number + 1)
        if number < total_pieces:
            copies, local = made[number]
            for kind in ("after", "before", "partner"):
                copies[kind].start()
            for one in local:
                one.start()
        if 1 <= number <= total_pieces:
            copies, _ = made[number - 1]
            copies["after"].wait_recv()
            copies["on"].start()
            copies["partner_before"].start()
            copies["before"].wait_recv()
            copies["back"].start()
            copies["partner_after"].start()
        if 2 <= number:
            copies, _ = made[number - 2]
            copies["on"].wait_recv()
            copies["partner_left"].start()
            copies["back"].wait_recv()
            copies["partner_right"].start()
    for copies, local in made:
        for kind in ("partner", "partner_before", "partner_after", "partner_left", "partner_right"):
            copies[kind].wait_recv()
        for one in copies.values():
            one.wait_send()
        for one in local:
            one.wait()
    for one in part_copies:
        one.wait_send()


def finish(n, gradients, weights, m, v):
    count = float(sum(w.size for w in weights))
    pieces = []
    for i in (2, 0, 1):
        layers, rows, _ = gradients[i].shape
        for layer in range(layers):
            for half in range(2):
                pieces.append((i, layer, half * rows // 2, rows // 2))
    anywhere = pl.BlockSpec(memory_space=pl.ANY)
    shapes = [t.shape for t in gradients]
    of = lambda dtype: [pltpu.VMEM(s, dtype) for s in shapes]
    dma = pltpu.SemaphoreType.DMA
    return pl.pallas_call(
        functools.partial(finish_kernel, n, count, tuple(pieces)),
        out_shape=[jax.ShapeDtypeStruct(t.shape, t.dtype) for t in (*weights, *m, *v)],
        in_specs=[anywhere] * 12,
        out_specs=[anywhere] * 9,
        scratch_shapes=[
            *of(BF16), *of(BF16), *of(F32), *of(F32), *of(BF16),
            pltpu.VMEM((n, 8, 128), F32),
            dma((12,)), dma((len(pieces),)), dma((2, len(pieces))), dma((n - 1,)), dma((n - 1,)),
            dma((9, len(pieces))), dma((9, len(pieces))),
        ],
        compiler_params=pltpu.CompilerParams(collective_id=4, has_side_effects=True, vmem_limit_bytes=48 * 2**20),
        name="finish",
    )(*gradients, *weights, *m, *v)


def dot(a, b, contract):
    return lax.dot_general(a, b, (contract, ((), ())), preferred_element_type=F32)


def normed(h):
    wide = h.astype(F32)
    return (wide * lax.rsqrt(jnp.mean(wide**2, -1, keepdims=True) + 1e-6)).astype(BF16)


def forward(a, w_gate, w_up):
    gate, up = dot(a, w_gate, ((1,), (0,))), dot(a, w_up, ((1,), (0,)))
    return gate, up, (jax.nn.silu(gate) * up).astype(BF16)


def backward(gate, up, by_hidden):
    by_hidden = by_hidden.astype(BF16).astype(F32)
    s = jax.nn.sigmoid(gate)
    by_up = by_hidden * gate * s
    by_gate = by_hidden * up * (s * (1 + gate * (1 - s)))
    return by_gate.astype(BF16), by_up.astype(BF16)


def by_norm(h, by_a):
    wide = h.astype(F32)
    scale = lax.rsqrt(jnp.mean(wide**2, -1, keepdims=True) + 1e-6)
    return scale * by_a - wide * (scale**3 * jnp.mean(by_a * wide, -1, keepdims=True))


def solution(mesh):
    n = mesh.shape["dp"]

    def step(x, dy, w_gate, w_up, w_down, *moments):
        m, v = moments[:3], moments[3:]
        h0, by_y = x[0], dy[0]
        scatter = lambda t: lax.psum_scatter(t, "dp", scatter_dimension=0, tiled=True)
        a0 = normed(h0)
        gate0, up0, hidden0 = forward(a0, w_gate[0], w_up[0])
        h1 = h0 + dot(hidden0, w_down[0], ((1,), (0,))).astype(BF16)
        a1 = normed(h1)
        gate1, up1, hidden1 = forward(a1, w_gate[1], w_up[1])
        g_down1 = scatter(dot(hidden1, by_y, ((0,), (0,))).astype(BF16))
        by_gate1, by_up1 = backward(gate1, up1, dot(by_y, w_down[1], ((1,), (1,))))
        g_gate1 = scatter(dot(a1, by_gate1, ((0,), (0,))).astype(BF16))
        g_up1 = scatter(dot(a1, by_up1, ((0,), (0,))).astype(BF16))
        by_a1 = dot(by_gate1, w_gate[1], ((1,), (1,))) + dot(by_up1, w_up[1], ((1,), (1,)))
        by_h1 = (by_y.astype(F32) + by_norm(h1, by_a1)).astype(BF16)
        g_down0 = scatter(dot(hidden0, by_h1, ((0,), (0,))).astype(BF16))
        by_gate0, by_up0 = backward(gate0, up0, dot(by_h1, w_down[0], ((1,), (1,))))
        g_gate0 = scatter(dot(a0, by_gate0, ((0,), (0,))).astype(BF16))
        g_up0 = scatter(dot(a0, by_up0, ((0,), (0,))).astype(BF16))
        gradients = [jnp.stack(pair) for pair in ((g_gate0, g_gate1), (g_up0, g_up1), (g_down0, g_down1))]
        return tuple(finish(n, gradients, (w_gate, w_up, w_down), m, v))

    sharded = P(None, "dp", None)
    return jax.shard_map(
        step,
        mesh=mesh,
        in_specs=(P(("rep", "dp")), P(("rep", "dp")), P(), P(), P(), *[sharded] * 6),
        out_specs=(*[P("rep")] * 3, *[P("rep", "dp")] * 6),
        check_vma=False,
    )
```

```python
import functools

import jax
import jax.numpy as jnp
from jax import lax
from jax.experimental import pallas as pl
from jax.experimental.pallas import tpu as pltpu
from jax.sharding import PartitionSpec as P

MESH = pl.DeviceIdType.MESH
F32, BF16 = jnp.float32, jnp.bfloat16
CORES = 2


def places(axis, n):
    me = lax.axis_index(axis)
    chips = n // CORES
    core, chip = lax.rem(me, CORES), lax.div(me, CORES)
    at = lambda away: lax.rem(chip + away, chips) * CORES + core
    return me, core, me + 1 - 2 * core, at(1), at(chips - 1), at(2)


def finish_kernel(n, count, pieces, *refs):
    g_in, w_in, m_in, v_in, w_out, m_out, v_out = (refs[3 * i : 3 * i + 3] for i in range(7))
    g, w, m, v, new = (refs[21 + 3 * i : 24 + 3 * i] for i in range(5))
    parts, load_sem, own_sem, store_sem, part_send, part_recv, send, recv = refs[36:]
    me, core, partner, after, before, across = places("dp", n)

    barrier = pltpu.get_barrier_semaphore()
    peers = [lax.rem(me + away, n) for away in range(1, n)]
    for peer in peers:
        pl.semaphore_signal(barrier, inc=1, device_id={"dp": peer}, device_id_type=MESH)

    loads = []
    for i in range(3):
        loads.append(pltpu.make_async_copy(g_in[i], g[i], load_sem.at[i]))
    for i in (2, 0, 1):
        rows = g[i].shape[1]
        mine = pl.ds(pl.multiple_of(me * rows, 16), rows)
        loads.append(pltpu.make_async_copy(w_in[i].at[:, mine], w[i], load_sem.at[3 + i]))
        loads.append(pltpu.make_async_copy(m_in[i], m[i], load_sem.at[6 + i]))
        loads.append(pltpu.make_async_copy(v_in[i], v[i], load_sem.at[9 + i]))
    for one in loads:
        one.start()

    total = jnp.zeros((8, 128), F32)
    for i in range(3):
        loads[i].wait()
        layers, rows, columns = g[i].shape

        def squares(step, total, ref=g[i], columns=columns, rows=rows):
            block = ref[lax.div(step, rows // 16), pl.ds(pl.multiple_of(lax.rem(step, rows // 16) * 16, 16), 16), :].astype(F32)
            block = block * block
            for at in range(0, columns, 128):
                total += block[:8, at : at + 128] + block[8:, at : at + 128]
            return total

        total = lax.fori_loop(0, layers * rows // 16, squares, total)
    parts[pl.ds(me, 1)] = total[None]
    pl.semaphore_wait(barrier, n - 1)
    part_copies = []
    for k, peer in enumerate(peers):
        part_copies.append(
            pltpu.make_async_remote_copy(
                parts.at[me], parts.at[me], part_send.at[k], part_recv.at[k], device_id={"dp": peer}, device_id_type=MESH
            )
        )
        part_copies[-1].start()
    for one in part_copies:
        one.wait_recv()
    every = parts[0]
    for k in range(1, n):
        every += parts[k]
    mean = jnp.sum(every, keepdims=True) / count
    factor = jnp.minimum(1.0, 0.5 * lax.rsqrt(mean + 1e-30))

    def adamw(i, layer, first, rows):
        step_rows = 16
        columns = g[i].shape[2]

        def body(step, _):
            at = (layer, pl.ds(pl.multiple_of(first + step * step_rows, 16), step_rows), slice(None))
            grad = g[i][at].astype(F32) * factor
            m_new = 0.9 * m[i][at] + 0.1 * grad
            v_new = 0.95 * v[i][at] + 0.05 * grad * grad
            w_old = w[i][at].astype(F32)
            m[i][at] = m_new
            v[i][at] = v_new
            new[i][at] = (w_old - 0.02 * (m_new * lax.rsqrt(v_new + 1e-8) + 0.1 * w_old)).astype(BF16)
            return 0

        lax.fori_loop(0, rows // step_rows, body, 0)

    def rows_of(i, owner, first, rows):
        return pl.ds(pl.multiple_of(owner * g[i].shape[1] + first, 16), rows)

    def remote(kind, number, src, dst, to):
        return pltpu.make_async_remote_copy(
            src, dst, send.at[kind, number], recv.at[kind, number], device_id={"dp": to}, device_id_type=MESH
        )

    def piece(number):
        i, layer, first, rows = pieces[number]
        place = lambda owner, columns=slice(None): w_out[i].at[layer, rows_of(i, owner, first, rows), columns]
        half = g[i].shape[2] // 2
        left, right = pl.ds(0, half), pl.ds(half, half)
        mine = new[i].at[layer, pl.ds(first, rows)]
        copies = {
            "after": remote(0, number, mine, place(me), after),
            "before": remote(1, number, mine, place(me), before),
            "partner": remote(2, number, mine, place(me), partner),
            "on": remote(3, number, place(before, left), place(before, left), after),
            "back": remote(4, number, place(after, right), place(after, right), before),
            "partner_before": remote(5, number, place(before), place(before), partner),
            "partner_after": remote(6, number, place(after), place(after), partner),
            "partner_left": remote(7, number, place(across, left), place(across, left), partner),
            "partner_right": remote(8, number, place(across, right), place(across, right), partner),
        }
        local = pltpu.make_async_copy(mine, place(me), own_sem.at[number])
        stores = [
            pltpu.make_async_copy(t[i].at[layer, pl.ds(first, rows)], o[i].at[layer, pl.ds(first, rows)], store_sem.at[k, number])
            for k, (t, o) in enumerate(((m, m_out), (v, v_out)))
        ]
        return copies, [local, *stores]

    waited = set()
    total_pieces = len(pieces)
    made = [piece(number) for number in range(total_pieces)]

    def compute(number):
        i, layer, first, rows = pieces[number]
        if i not in waited:
            waited.add(i)
            for one in loads[3 + 3 * (2, 0, 1).index(i) :][:3]:
                one.wait()
        adamw(i, layer, first, rows)

    compute(0)
    for number in range(total_pieces + 2):
        if number + 1 < total_pieces:
            compute(number + 1)
        if number < total_pieces:
            copies, local = made[number]
            for kind in ("after", "before", "partner"):
                copies[kind].start()
            for one in local:
                one.start()
        if 1 <= number <= total_pieces:
            copies, _ = made[number - 1]
            copies["after"].wait_recv()
            copies["on"].start()
            copies["partner_before"].start()
            copies["before"].wait_recv()
            copies["back"].start()
            copies["partner_after"].start()
        if 2 <= number:
            copies, _ = made[number - 2]
            copies["on"].wait_recv()
            copies["partner_left"].start()
            copies["back"].wait_recv()
            copies["partner_right"].start()
    for copies, local in made:
        for kind in ("partner", "partner_before", "partner_after", "partner_left", "partner_right"):
            copies[kind].wait_recv()
        for one in copies.values():
            one.wait_send()
        for one in local:
            one.wait()
    for one in part_copies:
        one.wait_send()


def finish(n, gradients, weights, m, v):
    count = float(sum(w.size for w in weights))
    pieces = []
    for i in (2, 0, 1):
        layers, rows, _ = gradients[i].shape
        for layer in range(layers):
            for half in range(2):
                pieces.append((i, layer, half * rows // 2, rows // 2))
    anywhere = pl.BlockSpec(memory_space=pl.ANY)
    shapes = [t.shape for t in gradients]
    of = lambda dtype: [pltpu.VMEM(s, dtype) for s in shapes]
    dma = pltpu.SemaphoreType.DMA
    return pl.pallas_call(
        functools.partial(finish_kernel, n, count, tuple(pieces)),
        out_shape=[jax.ShapeDtypeStruct(t.shape, t.dtype) for t in (*weights, *m, *v)],
        in_specs=[anywhere] * 12,
        out_specs=[anywhere] * 9,
        scratch_shapes=[
            *of(BF16), *of(BF16), *of(F32), *of(F32), *of(BF16),
            pltpu.VMEM((n, 8, 128), F32),
            dma((12,)), dma((len(pieces),)), dma((2, len(pieces))), dma((n - 1,)), dma((n - 1,)),
            dma((9, len(pieces))), dma((9, len(pieces))),
        ],
        compiler_params=pltpu.CompilerParams(collective_id=4, has_side_effects=True, vmem_limit_bytes=48 * 2**20),
        name="finish",
    )(*gradients, *weights, *m, *v)


def dot(a, b, contract=((1,), (0,))):
    return lax.dot_general(a, b, (contract, ((), ())), preferred_element_type=F32)


def normed(h):
    wide = h.astype(F32)
    return (wide * lax.rsqrt(jnp.mean(wide * wide, -1, keepdims=True) + 1e-6)).astype(BF16)


def by_norm(h, by_a):
    wide = h.astype(F32)
    scale = lax.rsqrt(jnp.mean(wide * wide, -1, keepdims=True) + 1e-6)
    return scale * by_a - wide * (scale * scale * scale * jnp.mean(by_a * wide, -1, keepdims=True))


def by_units(gate, up, by_hidden):
    by_hidden = by_hidden.astype(BF16).astype(F32)
    s = jax.nn.sigmoid(gate)
    silu = gate * s
    return silu * up, by_hidden * up * (s + silu * (1.0 - s)), by_hidden * silu


def forward_kernel(tiles, x, w_gate, w_up, w_down, gate_out, up_out, hidden_t, a_t, h_out, next_a, next_a_t, wg, wu, wd, sem):
    tile = pl.program_id(0)
    loads = [pltpu.make_async_copy(src.at[0], dst, sem.at[k]) for k, (src, dst) in enumerate(((w_gate, wg), (w_up, wu), (w_down, wd)))]

    @pl.when(tile == 0)
    def _():
        for one in loads:
            one.start()

    a = normed(x[...])
    a_t[...] = a.T

    @pl.when(tile == 0)
    def _():
        loads[0].wait()
        loads[1].wait()

    columns = wg.shape[1]
    width = 256
    hidden = []
    for at in range(0, columns, width):
        gate = dot(a, wg[:, at : at + width])
        up = dot(a, wu[:, at : at + width])
        gate_out[:, at : at + width] = gate
        up_out[:, at : at + width] = up
        hidden.append((gate * jax.nn.sigmoid(gate) * up).astype(BF16))
        hidden_t[at : at + width, :] = hidden[-1].T

    @pl.when(tile == 0)
    def _():
        loads[2].wait()

    h = x[...] + dot(jnp.concatenate(hidden, 1), wd[...]).astype(BF16)
    h_out[...] = h
    b = normed(h)
    next_a[...] = b
    next_a_t[...] = b.T


def layer_0(x, w_gate, w_up, w_down):
    tokens, d = x.shape
    ff = w_gate.shape[2]
    rows = 256
    anywhere = pl.BlockSpec(memory_space=pl.ANY)
    tall = lambda n: pl.BlockSpec((rows, n), lambda i: (i, 0))
    wide = lambda n: pl.BlockSpec((n, rows), lambda i: (0, i))
    return pl.pallas_call(
        functools.partial(forward_kernel, tokens // rows),
        grid=(tokens // rows,),
        in_specs=[tall(d), anywhere, anywhere, anywhere],
        out_specs=[tall(ff), tall(ff), wide(ff), wide(d), tall(d), tall(d), wide(d)],
        out_shape=[
            jax.ShapeDtypeStruct((tokens, ff), F32),
            jax.ShapeDtypeStruct((tokens, ff), F32),
            jax.ShapeDtypeStruct((ff, tokens), BF16),
            jax.ShapeDtypeStruct((d, tokens), BF16),
            jax.ShapeDtypeStruct((tokens, d), BF16),
            jax.ShapeDtypeStruct((tokens, d), BF16),
            jax.ShapeDtypeStruct((d, tokens), BF16),
        ],
        scratch_shapes=[pltpu.VMEM((d, ff), BF16), pltpu.VMEM((d, ff), BF16), pltpu.VMEM((ff, d), BF16), pltpu.SemaphoreType.DMA((3,))],
        compiler_params=pltpu.CompilerParams(vmem_limit_bytes=60 * 2**20),
        name="forward",
    )(x, w_gate, w_up, w_down)


SLOTS = 6
HELD = 4
SENT = 3


class Exchange:
    def __init__(self, n, refs, kinds):
        self.mine, self.pair, self.out2, self.out3, self.in2, self.in3, self.pair_sem, self.sem2, self.sem3 = refs
        self.kinds = kinds
        self.me, self.core, self.partner, self.after, self.before, _ = places("dp", n)
        chips = n // CORES
        chip = lax.div(self.me, CORES)
        self.chip = chip
        self.chip_after, self.chip_before, self.chip_across = (lax.rem(chip + k, chips) for k in (1, chips - 1, chips // 2))

    @staticmethod
    def scratch(n, rows, width):
        chips, half, dma = n // CORES, width // 2, pltpu.SemaphoreType.DMA
        return [
            pltpu.VMEM((HELD, chips, CORES, rows, width), BF16),
            pltpu.VMEM((SLOTS, chips, rows, width), BF16),
            pltpu.VMEM((2, SENT, rows, width), BF16),
            pltpu.VMEM((2, SENT, rows, half), BF16),
            pltpu.VMEM((2, SLOTS, rows, width), BF16),
            pltpu.VMEM((2, SLOTS, rows, half), BF16),
            dma((2, SLOTS)), dma((2, 2, SLOTS)), dma((2, 2, SLOTS)),
        ]

    def barrier(self):
        barrier = pltpu.get_barrier_semaphore()
        for peer in (self.partner, self.after, self.before):
            pl.semaphore_signal(barrier, inc=1, device_id={"dp": peer}, device_id_type=MESH)
        pl.semaphore_wait(barrier, 3)

    def copy1(self, p, rows):
        slot = lax.rem(p, SLOTS)
        return pltpu.make_async_remote_copy(
            self.mine.at[lax.rem(p, HELD), :, 1 - self.core, pl.ds(0, rows)], self.pair.at[slot, :, pl.ds(0, rows)],
            self.pair_sem.at[0, slot], self.pair_sem.at[1, slot], device_id={"dp": self.partner}, device_id_type=MESH,
        )

    def copies(self, p, rows, out, into, sem):
        slot = lax.rem(p, SLOTS)
        return [
            pltpu.make_async_remote_copy(
                out.at[way, lax.rem(p, SENT), pl.ds(0, rows)], into.at[way, slot, pl.ds(0, rows)],
                sem.at[0, way, slot], sem.at[1, way, slot], device_id={"dp": to}, device_id_type=MESH,
            )
            for way, to in enumerate((self.after, self.before))
        ]

    def over(self, rows, body):
        def step(i, _):
            body(pl.ds(pl.multiple_of(i * 16, 16), 16))
            return 0

        lax.fori_loop(0, rows // 16, step, 0)

    def of_chip(self, p, chip, at, columns):
        a = self.mine[lax.rem(p, HELD), chip, self.core, at, columns].astype(F32)
        return a + self.pair[lax.rem(p, SLOTS), chip, at, columns].astype(F32)

    def stage1(self, p, rows, _):
        self.copy1(p, rows).start()

    def stage2(self, p, rows, _):
        self.copy1(p, rows).wait()
        slot = lax.rem(p, SENT)
        half = self.out3.shape[-1]
        left, right = slice(0, half), slice(half, 2 * half)

        def body(at):
            self.out2[0, slot, at, left] = self.of_chip(p, self.chip_across, at, left).astype(BF16)
            self.out2[0, slot, at, right] = self.of_chip(p, self.chip_after, at, right).astype(BF16)
            self.out2[1, slot, at, left] = self.of_chip(p, self.chip_before, at, left).astype(BF16)
            self.out2[1, slot, at, right] = self.of_chip(p, self.chip_across, at, right).astype(BF16)

        self.over(rows, body)
        for one in self.copies(p, rows, self.out2, self.in2, self.sem2):
            one.start()

    def stage3(self, p, rows, _):
        for one in self.copies(p, rows, self.out2, self.in2, self.sem2):
            one.wait()
        slot, arrived = lax.rem(p, SENT), lax.rem(p, SLOTS)
        half = self.out3.shape[-1]
        left, right = slice(0, half), slice(half, 2 * half)

        def body(at):
            self.out3[0, slot, at] = (self.of_chip(p, self.chip_after, at, left) + self.in2[0, arrived, at, left].astype(F32)).astype(BF16)
            self.out3[1, slot, at] = (self.of_chip(p, self.chip_before, at, right) + self.in2[1, arrived, at, right].astype(F32)).astype(BF16)

        self.over(rows, body)
        for one in self.copies(p, rows, self.out3, self.in3, self.sem3):
            one.start()

    def stage4(self, p, rows, keep):
        for one in self.copies(p, rows, self.out3, self.in3, self.sem3):
            one.wait()
        arrived = lax.rem(p, SLOTS)
        half = self.out3.shape[-1]
        left, right = slice(0, half), slice(half, 2 * half)

        def body(at):
            a = self.of_chip(p, self.chip, at, left) + (self.in3[0, arrived, at].astype(F32) + self.in2[1, arrived, at, left].astype(F32))
            b = self.of_chip(p, self.chip, at, right) + (self.in2[0, arrived, at, right].astype(F32) + self.in3[1, arrived, at].astype(F32))
            keep(p, at, a.astype(BF16), b.astype(BF16))

        self.over(rows, body)

    def move(self, step, low, high):
        for lag, stage in enumerate((self.stage1, self.stage2, self.stage3, self.stage4)):
            for first, end, rows, keep in self.kinds:
                if high - 1 - lag < first or low - lag >= end:
                    continue
                p = step - lag
                if low - lag >= first and high - 1 - lag < end:
                    stage(p, rows, keep)
                else:
                    pl.when((p >= first) & (p < end))(functools.partial(stage, p, rows, keep))


def keep_columns(first, gate, up, width):
    def keep(p, at, left, right):
        columns = pl.ds(pl.multiple_of((p - first) * width, width), width)
        gate[at, columns] = left
        up[at, columns] = right

    return keep


def keep_down(first, down, rows, width):
    def keep(p, at, left, right):
        half = width // 2
        which = p - first
        at = pl.ds(pl.multiple_of(lax.rem(which, 2) * rows + at.start, 16), at.size)
        start = lax.div(which, 2) * width
        down[at, pl.ds(pl.multiple_of(start, half), half)] = left
        down[at, pl.ds(pl.multiple_of(start + half, half), half)] = right

    return keep


def down_packet(exchange, step, first, hidden_t, by_out):
    n_rows = hidden_t.shape[0]
    _, chips, cores, rows, width = exchange.mine.shape
    which = step - first
    start = pl.multiple_of(lax.rem(which, 2) * rows, 16)
    columns = pl.ds(pl.multiple_of(lax.div(which, 2) * width, width), width)
    share = n_rows // (chips * cores)
    lhs = jnp.concatenate([hidden_t[pl.ds(pl.multiple_of(k * share + start, 16), rows), :] for k in range(chips * cores)], 0)
    block = dot(lhs, by_out[:, columns]).astype(BF16)
    exchange.mine[lax.rem(step, HELD)] = block.reshape(chips, cores, rows, width)


def wide_packet(exchange, step, a_t, by_both):
    _, chips, cores, _, width = exchange.mine.shape
    rows = a_t.shape[0] // (chips * cores)
    half = width // 2
    for k in range(2):
        columns = slice(k * half, k * half + half)
        block = dot(a_t[...], by_both[:, columns]).astype(BF16)
        exchange.mine[lax.rem(step, HELD), :, :, pl.ds(0, rows), columns] = block.reshape(chips, cores, rows, half)


MB = 512


def top_kernel(n, *refs):
    (a_in, at_in, h_in, dy_in, w_gate, w_up, w_down), refs = refs[:7], refs[7:]
    (g_gate, g_up, g_down, by_h, bg_hbm, bu_hbm), refs = refs[:6], refs[6:]
    (a, a_t, dy, wg, wu, hidden_t, wd, both, h_tile, by_tile, load_sem, wd_sem, both_sem, tile_sem, by_sem), refs = refs[:15], refs[15:]
    tokens, d = a.shape
    ff = wg.shape[1]
    width = 256
    chunks = ff // width
    downs = 4
    wide_rows, down_rows = d // n, ff // n // 2
    exchange = Exchange(
        n, refs,
        (
            (0, chunks, wide_rows, keep_columns(0, g_gate, g_up, width)),
            (chunks, chunks + downs, down_rows, keep_down(chunks, g_down, down_rows, 2 * width)),
        ),
    )
    layer = w_gate.shape[0] - 1
    first, rest = pl.ds(0, width), pl.ds(width, ff - width)
    loads = [
        pltpu.make_async_copy(a_in, a, load_sem.at[0]),
        pltpu.make_async_copy(w_gate.at[layer, :, first], wg.at[:, first], load_sem.at[1]),
        pltpu.make_async_copy(w_up.at[layer, :, first], wu.at[:, first], load_sem.at[2]),
        pltpu.make_async_copy(dy_in, dy, load_sem.at[3]),
        pltpu.make_async_copy(at_in, a_t, load_sem.at[4]),
        pltpu.make_async_copy(w_gate.at[layer, :, rest], wg.at[:, rest], load_sem.at[5]),
        pltpu.make_async_copy(w_up.at[layer, :, rest], wu.at[:, rest], load_sem.at[6]),
    ]

    def down_chunk(c):
        slot = lax.rem(c, 2)
        return pltpu.make_async_copy(w_down.at[layer, pl.ds(pl.multiple_of(c * width, width), width)], wd.at[slot], wd_sem.at[slot])

    for one in loads[:4]:
        one.start()
    down_chunk(0).start()
    for one in loads[4:]:
        one.start()
    exchange.barrier()

    def store_both(c, k):
        slot = lax.rem(c, 2)
        return pltpu.make_async_copy(
            both.at[slot, :, pl.ds(k * width, width)],
            (bg_hbm, bu_hbm)[k].at[:, pl.ds(pl.multiple_of(c * width, width), width)],
            both_sem.at[k, slot],
        )

    def chunk(c, _):
        slot = lax.rem(c, 2)

        @pl.when(c == 0)
        def _():
            for one in loads[:5]:
                one.wait()

        @pl.when(c == 1)
        def _():
            for one in loads[5:]:
                one.wait()

        @pl.when(c >= 2)
        def _():
            for k in range(2):
                store_both(c - 2, k).wait()

        down_chunk(c).wait()

        @pl.when(c + 1 < chunks)
        def _():
            down_chunk(c + 1).start()

        columns = pl.ds(pl.multiple_of(c * width, width), width)
        wg_c, wu_c, wd_c = wg[:, columns], wu[:, columns], wd[slot]
        for at in range(0, tokens, MB):
            rows = slice(at, at + MB)
            hidden, by_gate, by_up = by_units(dot(a[rows], wg_c), dot(a[rows], wu_c), dot(dy[rows], wd_c, ((1,), (1,))))
            hidden_t[columns, rows] = hidden.astype(BF16).T
            both[slot, rows, :width] = by_gate.astype(BF16)
            both[slot, rows, width:] = by_up.astype(BF16)
        wide_packet(exchange, c, a_t, both.at[slot])
        for k in range(2):
            store_both(c, k).start()
        exchange.move(c, 0, chunks)
        return 0

    lax.fori_loop(0, chunks, chunk, 0)
    for c in (chunks - 2, chunks - 1):
        for k in range(2):
            store_both(c, k).wait()

    tile_rows = 256
    tiles = tokens // tile_rows
    split = a_t.shape[1]

    def tile_loads(t):
        slot = lax.rem(t, 2)
        rows = pl.ds(pl.multiple_of(t * tile_rows, tile_rows), tile_rows)
        got = []
        for k, src in enumerate((bg_hbm, bu_hbm)):
            to = pl.ds(pl.multiple_of((slot * 2 + k) * tile_rows, tile_rows), tile_rows)
            got.append(pltpu.make_async_copy(src.at[rows, pl.ds(0, split)], a_t.at[to], tile_sem.at[2 * k, slot]))
            got.append(pltpu.make_async_copy(src.at[rows, pl.ds(split, ff - split)], a.at[to, pl.ds(0, ff - split)], tile_sem.at[2 * k + 1, slot]))
        got.append(pltpu.make_async_copy(h_in.at[rows], h_tile.at[slot], tile_sem.at[4, slot]))
        return got

    def tile_store(t):
        slot = lax.rem(t, 2)
        return pltpu.make_async_copy(by_tile.at[slot], by_h.at[pl.ds(pl.multiple_of(t * tile_rows, tile_rows), tile_rows)], by_sem.at[slot])

    for one in tile_loads(0):
        one.start()

    def down(step, _):
        down_packet(exchange, step, chunks, hidden_t, dy)
        exchange.move(step, chunks, chunks + downs)
        return 0

    lax.fori_loop(chunks, chunks + downs, down, 0)

    def tile(step, _):
        t = step - chunks - downs
        slot = lax.rem(t, 2)
        for one in tile_loads(t):
            one.wait()

        @pl.when(t + 1 < tiles)
        def _():
            for one in tile_loads(t + 1):
                one.start()

        @pl.when(t >= 2)
        def _():
            tile_store(t - 2).wait()

        total = None
        for k, w in enumerate((wg, wu)):
            at = pl.ds(pl.multiple_of((slot * 2 + k) * tile_rows, tile_rows), tile_rows)
            term = dot(a_t[at], w[:, :split], ((1,), (1,))) + dot(a[at, : ff - split], w[:, split:], ((1,), (1,)))
            total = term if total is None else total + term
        rows = pl.ds(pl.multiple_of(t * tile_rows, tile_rows), tile_rows)
        by_tile[slot] = (dy[rows].astype(F32) + by_norm(h_tile[slot], total)).astype(BF16)
        tile_store(t).start()
        exchange.move(step, chunks + downs, chunks + downs + tiles)
        return 0

    lax.fori_loop(chunks + downs, chunks + downs + tiles, tile, 0)
    for t in (tiles - 2, tiles - 1):
        tile_store(t).wait()


def top_layer(n, a, a_t, h, dy, w_gate, w_up, w_down):
    tokens, d = a.shape
    ff = w_gate.shape[2]
    width = 256
    anywhere, inside = pl.BlockSpec(memory_space=pl.ANY), pl.BlockSpec(memory_space=pltpu.VMEM)
    dma = pltpu.SemaphoreType.DMA
    return pl.pallas_call(
        functools.partial(top_kernel, n),
        in_specs=[anywhere] * 7,
        out_specs=[inside] * 3 + [anywhere] * 3,
        out_shape=[
            jax.ShapeDtypeStruct((d // n, ff), BF16),
            jax.ShapeDtypeStruct((d // n, ff), BF16),
            jax.ShapeDtypeStruct((ff // n, d), BF16),
            jax.ShapeDtypeStruct((tokens, d), BF16),
            jax.ShapeDtypeStruct((tokens, ff), BF16),
            jax.ShapeDtypeStruct((tokens, ff), BF16),
        ],
        scratch_shapes=[
            pltpu.VMEM((tokens, d), BF16), pltpu.VMEM((d, tokens), BF16), pltpu.VMEM((tokens, d), BF16),
            pltpu.VMEM((d, ff), BF16), pltpu.VMEM((d, ff), BF16), pltpu.VMEM((ff, tokens), BF16),
            pltpu.VMEM((2, width, d), BF16), pltpu.VMEM((2, tokens, 2 * width), BF16),
            pltpu.VMEM((2, 256, d), BF16), pltpu.VMEM((2, 256, d), BF16),
            dma((7,)), dma((2,)), dma((2, 2)), dma((5, 2)), dma((2,)),
            *Exchange.scratch(n, ff // n // 2, 2 * width),
        ],
        compiler_params=pltpu.CompilerParams(collective_id=2, has_side_effects=True, vmem_limit_bytes=67043328),
        name="top",
    )(a, a_t, h, dy, w_gate, w_up, w_down)


def bottom_kernel(n, *refs):
    (by_in, ht_in, at_in, gate_in, up_in, w_down), refs = refs[:6], refs[6:]
    (g_gate, g_up, g_down), refs = refs[:3], refs[3:]
    (by, hidden_t, a_t, wd, gate, up, both, load_sem, wd_sem, unit_sem), refs = refs[:10], refs[10:]
    tokens, d = by.shape
    ff = hidden_t.shape[0]
    width = 256
    chunks = ff // width
    downs = 4
    wide_rows, down_rows = d // n, ff // n // 2
    exchange = Exchange(
        n, refs,
        (
            (0, downs, down_rows, keep_down(0, g_down, down_rows, 2 * width)),
            (downs, downs + chunks, wide_rows, keep_columns(downs, g_gate, g_up, width)),
        ),
    )
    loads = [
        pltpu.make_async_copy(ht_in, hidden_t, load_sem.at[0]),
        pltpu.make_async_copy(by_in, by, load_sem.at[1]),
        pltpu.make_async_copy(at_in, a_t, load_sem.at[2]),
    ]

    def chunk_loads(c):
        slot = lax.rem(c, 2)
        columns = pl.ds(pl.multiple_of(c * width, width), width)
        return [
            pltpu.make_async_copy(w_down.at[0, columns], wd.at[slot], wd_sem.at[slot]),
            pltpu.make_async_copy(gate_in.at[:, columns], gate.at[slot], unit_sem.at[0, slot]),
            pltpu.make_async_copy(up_in.at[:, columns], up.at[slot], unit_sem.at[1, slot]),
        ]

    for one in (*loads, *chunk_loads(0)):
        one.start()
    exchange.barrier()
    for one in loads[:2]:
        one.wait()

    def down(step, _):
        down_packet(exchange, step, 0, hidden_t, by)
        exchange.move(step, 0, downs)
        return 0

    lax.fori_loop(0, downs, down, 0)
    loads[2].wait()

    def chunk(step, _):
        c = step - downs
        slot = lax.rem(c, 2)
        for one in chunk_loads(c):
            one.wait()

        @pl.when(c + 1 < chunks)
        def _():
            for one in chunk_loads(c + 1):
                one.start()

        wd_c = wd[slot]
        for at in range(0, tokens, MB):
            rows = slice(at, at + MB)
            _, by_gate, by_up = by_units(gate[slot, rows], up[slot, rows], dot(by[rows], wd_c, ((1,), (1,))))
            both[rows, :width] = by_gate.astype(BF16)
            both[rows, width:] = by_up.astype(BF16)
        wide_packet(exchange, step, a_t, both)
        exchange.move(step, downs, downs + chunks)
        return 0

    lax.fori_loop(downs, downs + chunks, chunk, 0)
    for step in range(downs + chunks, downs + chunks + 3):
        exchange.move(step, step, step + 1)


def bottom_layer(n, by, hidden_t, a_t, gate, up, w_down):
    tokens, d = by.shape
    ff = hidden_t.shape[0]
    width = 256
    anywhere, inside = pl.BlockSpec(memory_space=pl.ANY), pl.BlockSpec(memory_space=pltpu.VMEM)
    dma = pltpu.SemaphoreType.DMA
    return pl.pallas_call(
        functools.partial(bottom_kernel, n),
        in_specs=[anywhere] * 6,
        out_specs=[inside] * 3,
        out_shape=[
            jax.ShapeDtypeStruct((d // n, ff), BF16),
            jax.ShapeDtypeStruct((d // n, ff), BF16),
            jax.ShapeDtypeStruct((ff // n, d), BF16),
        ],
        scratch_shapes=[
            pltpu.VMEM((tokens, d), BF16), pltpu.VMEM((ff, tokens), BF16), pltpu.VMEM((d, tokens), BF16),
            pltpu.VMEM((2, width, d), BF16), pltpu.VMEM((2, tokens, width), F32), pltpu.VMEM((2, tokens, width), F32),
            pltpu.VMEM((tokens, 2 * width), BF16),
            dma((3,)), dma((2,)), dma((2, 2)),
            *Exchange.scratch(n, ff // n // 2, 2 * width),
        ],
        compiler_params=pltpu.CompilerParams(collective_id=3, has_side_effects=True, vmem_limit_bytes=67043328),
        name="bottom",
    )(by, hidden_t, a_t, gate, up, w_down)


def solution(mesh):
    n = mesh.shape["dp"]

    def step(x, dy, w_gate, w_up, w_down, *moments):
        gate, up, hidden_t, a_t, h, next_a, next_a_t = layer_0(x[0], w_gate, w_up, w_down)
        *top, by_h, _, _ = top_layer(n, next_a, next_a_t, h, dy[0], w_gate, w_up, w_down)
        bottom = bottom_layer(n, by_h, hidden_t, a_t, gate, up, w_down)
        gradients = [jnp.stack(pair) for pair in zip(bottom, top, strict=True)]
        return tuple(finish(n, gradients, (w_gate, w_up, w_down), moments[:3], moments[3:]))

    sharded = P(None, "dp", None)
    return jax.shard_map(
        step,
        mesh=mesh,
        in_specs=(P(("rep", "dp")), P(("rep", "dp")), P(), P(), P(), *[sharded] * 6),
        out_specs=(*[P("rep")] * 3, *[P("rep", "dp")] * 6),
        check_vma=False,
    )
```

```python
import functools

import jax
import jax.numpy as jnp
from jax import lax
from jax.experimental import pallas as pl
from jax.experimental.pallas import tpu as pltpu
from jax.sharding import PartitionSpec as P

MESH = pl.DeviceIdType.MESH
F32, BF16 = jnp.float32, jnp.bfloat16
CORES = 2


def places(axis, n):
    me = lax.axis_index(axis)
    chips = n // CORES
    core, chip = lax.rem(me, CORES), lax.div(me, CORES)
    at = lambda away: lax.rem(chip + away, chips) * CORES + core
    return me, core, me + 1 - 2 * core, at(1), at(chips - 1), at(2)


def finish_kernel(n, count, pieces, *refs):
    layers = 2
    g_in, refs = [refs[layers * i : layers * i + layers] for i in range(3)], refs[3 * layers :]
    w_in, m_in, v_in, w, m, v = (refs[3 * i : 3 * i + 3] for i in range(6))
    g, refs = refs[18:21], refs[21:]
    parts, load_sem, part_send, part_recv, send, recv = refs
    me, core, partner, after, before, across = places("dp", n)

    barrier = pltpu.get_barrier_semaphore()
    peers = [lax.rem(me + away, n) for away in range(1, n)]
    for peer in peers:
        pl.semaphore_signal(barrier, inc=1, device_id={"dp": peer}, device_id_type=MESH)

    def rows_of(i, owner, first, rows):
        return pl.ds(pl.multiple_of(owner * g[i].shape[1] + first, 16), rows)

    order = (2, 0, 1)
    g_loads = [[pltpu.make_async_copy(g_in[i][k], g[i].at[k], load_sem.at[layers * i + k]) for k in range(layers)] for i in order]
    loads = {}
    at = 3 * layers
    for i in order:
        rows = rows_of(i, me, 0, g[i].shape[1])
        loads[i] = [
            pltpu.make_async_copy(w_in[i].at[:, rows], w[i].at[:, rows], load_sem.at[at]),
            pltpu.make_async_copy(m_in[i], m[i], load_sem.at[at + 1]),
            pltpu.make_async_copy(v_in[i], v[i], load_sem.at[at + 2]),
        ]
        at += 3
    for one in (*sum(g_loads, []), *sum((loads[i] for i in order), [])):
        one.start()

    total = jnp.zeros((8, 128), F32)
    for i, its_loads in zip(order, g_loads, strict=True):
        _, rows, columns = g[i].shape
        for one in its_loads:
            one.wait()

        def squares(step, total, ref=g[i], columns=columns, rows=rows):
            block = ref[lax.div(step, rows // 16), pl.ds(pl.multiple_of(lax.rem(step, rows // 16) * 16, 16), 16), :].astype(F32)
            block = block * block
            sums = [block[:8, at : at + 128] + block[8:, at : at + 128] for at in range(0, columns, 128)]
            while len(sums) > 1:
                sums = [a + b for a, b in zip(sums[::2], sums[1::2])] + ([sums[-1]] if len(sums) % 2 else [])
            return total + sums[0]

        total = lax.fori_loop(0, layers * rows // 16, squares, total)
    parts[pl.ds(me, 1)] = total[None]
    pl.semaphore_wait(barrier, n - 1)
    part_copies = []
    for k, peer in enumerate(peers):
        part_copies.append(
            pltpu.make_async_remote_copy(
                parts.at[me], parts.at[me], part_send.at[k], part_recv.at[k], device_id={"dp": peer}, device_id_type=MESH
            )
        )
        part_copies[-1].start()
    for one in part_copies:
        one.wait_recv()
    every = parts[0]
    for k in range(1, n):
        every += parts[k]
    mean = jnp.sum(every, keepdims=True) / count
    factor = jnp.minimum(1.0, 0.5 * lax.rsqrt(mean + 1e-30))

    def adamw(i, layer, first, rows):
        step_rows = 16

        def body(step, _):
            start = first + step * step_rows
            at = (layer, pl.ds(pl.multiple_of(start, 16), step_rows), slice(None))
            mine = (layer, rows_of(i, me, start, step_rows), slice(None))
            grad = g[i][at].astype(F32) * factor
            m_new = 0.9 * m[i][at] + 0.1 * grad
            v_new = 0.95 * v[i][at] + 0.05 * grad * grad
            w_old = w[i][mine].astype(F32)
            m[i][at] = m_new
            v[i][at] = v_new
            w[i][mine] = (w_old - 0.02 * (m_new * lax.rsqrt(v_new + 1e-8) + 0.1 * w_old)).astype(BF16)
            return 0

        lax.fori_loop(0, rows // step_rows, body, 0)

    def piece(number):
        i, layer, first, rows = pieces[number]
        half = g[i].shape[2] // 2
        left, right = pl.ds(0, half), pl.ds(half, half)

        def copy(kind, to, owner, columns=slice(None)):
            place = w[i].at[layer, rows_of(i, owner, first, rows), columns]
            return pltpu.make_async_remote_copy(
                place, place, send.at[kind, number], recv.at[kind, number], device_id={"dp": to}, device_id_type=MESH
            )

        return {
            "after": copy(0, after, me),
            "before": copy(1, before, me),
            "partner": copy(2, partner, me),
            "on": copy(3, after, before, left),
            "back": copy(4, before, after, right),
            "partner_before": copy(5, partner, before),
            "partner_after": copy(6, partner, after),
            "partner_left": copy(7, partner, across, left),
            "partner_right": copy(8, partner, across, right),
        }

    waited = set()
    total_pieces = len(pieces)
    made = [piece(number) for number in range(total_pieces)]

    def compute(number):
        i, layer, first, rows = pieces[number]
        if i not in waited:
            waited.add(i)
            for one in loads[i]:
                one.wait()
        adamw(i, layer, first, rows)

    compute(0)
    for number in range(total_pieces + 2):
        if number + 1 < total_pieces:
            compute(number + 1)
        if number < total_pieces:
            for kind in ("after", "before", "partner"):
                made[number][kind].start()
        if 1 <= number <= total_pieces:
            copies = made[number - 1]
            copies["after"].wait_recv()
            copies["on"].start()
            copies["partner_before"].start()
            copies["before"].wait_recv()
            copies["back"].start()
            copies["partner_after"].start()
        if 2 <= number:
            copies = made[number - 2]
            copies["on"].wait_recv()
            copies["partner_left"].start()
            copies["back"].wait_recv()
            copies["partner_right"].start()
    for copies in made:
        for kind in ("partner", "partner_before", "partner_after", "partner_left", "partner_right"):
            copies[kind].wait_recv()
        for one in copies.values():
            one.wait_send()
    for one in part_copies:
        one.wait_send()


def store_kernel(*refs):
    *refs, sem = refs
    some = len(refs) // 2
    copies = [pltpu.make_async_copy(refs[k], refs[some + k], sem.at[k]) for k in range(some)]
    for one in copies:
        one.start()
    for one in copies:
        one.wait()


def finish(n, gradients, weights, m, v):
    count = float(sum(w.size for w in weights))
    layers = len(gradients[0])
    pieces = []
    for i in (2, 0, 1):
        rows, _ = gradients[i][0].shape
        for layer in range(layers):
            for half in range(2):
                pieces.append((i, layer, half * rows // 2, rows // 2))
    anywhere, inside = pl.BlockSpec(memory_space=pl.ANY), pl.BlockSpec(memory_space=pltpu.VMEM)
    dma = pltpu.SemaphoreType.DMA
    results = [*weights, *m, *v]
    ready = pl.pallas_call(
        functools.partial(finish_kernel, n, count, tuple(pieces)),
        out_shape=[pltpu.VMEM(t.shape, t.dtype) for t in results],
        in_specs=[anywhere] * (3 * layers + 9),
        out_specs=[inside] * 9,
        scratch_shapes=[
            *[pltpu.VMEM((layers, *one[0].shape), BF16) for one in gradients],
            pltpu.VMEM((n, 8, 128), F32),
            dma((3 * layers + 9,)), dma((n - 1,)), dma((n - 1,)), dma((9, len(pieces))), dma((9, len(pieces))),
        ],
        compiler_params=pltpu.CompilerParams(collective_id=4, has_side_effects=True, vmem_limit_bytes=7 * 2**20),
        name="finish",
    )(*sum(gradients, ()), *weights, *m, *v)
    return pl.pallas_call(
        store_kernel,
        out_shape=[jax.ShapeDtypeStruct(t.shape, t.dtype) for t in results],
        in_specs=[inside] * 9,
        out_specs=[anywhere] * 9,
        scratch_shapes=[dma((9,))],
        compiler_params=pltpu.CompilerParams(vmem_limit_bytes=7*2**20),
        name="store",
    )(*[pltpu.with_memory_space_constraint(t, pltpu.VMEM) for t in ready])


def dot(a, b, contract=((1,), (0,))):
    return lax.dot_general(a, b, (contract, ((), ())), preferred_element_type=F32)


def normed(h):
    wide = h.astype(F32)
    return (wide * lax.rsqrt(jnp.mean(wide * wide, -1, keepdims=True) + 1e-6)).astype(BF16)


def by_norm(h, by_a):
    wide = h.astype(F32)
    scale = lax.rsqrt(jnp.mean(wide * wide, -1, keepdims=True) + 1e-6)
    return scale * by_a - wide * (scale * scale * scale * jnp.mean(by_a * wide, -1, keepdims=True))


def by_units(gate, up, by_hidden):
    by_hidden = by_hidden.astype(BF16).astype(F32)
    s = jax.nn.sigmoid(gate)
    silu = gate * s
    return silu * up, by_hidden * up * (s + silu * (1.0 - s)), by_hidden * silu


def forward_kernel(tiles, x, w_gate, w_up, w_down, gate_out, up_out, hidden_t, a_t, h_out, next_a, next_a_t, wg, wu, wd, sem):
    tile = pl.program_id(0)
    loads = [pltpu.make_async_copy(src.at[0], dst, sem.at[k]) for k, (src, dst) in enumerate(((w_gate, wg), (w_up, wu), (w_down, wd)))]

    @pl.when(tile == 0)
    def _():
        for one in loads:
            one.start()

    a = normed(x[...])
    a_t[...] = a.T

    @pl.when(tile == 0)
    def _():
        loads[0].wait()
        loads[1].wait()

    columns = wg.shape[1]
    width = 256
    hidden = []
    for at in range(0, columns, width):
        gate = dot(a, wg[:, at : at + width])
        up = dot(a, wu[:, at : at + width])
        gate_out[:, at : at + width] = gate
        up_out[:, at : at + width] = up
        hidden.append((gate * jax.nn.sigmoid(gate) * up).astype(BF16))
        hidden_t[at : at + width, :] = hidden[-1].T

    @pl.when(tile == 0)
    def _():
        loads[2].wait()

    h = x[...] + dot(jnp.concatenate(hidden, 1), wd[...]).astype(BF16)
    h_out[...] = h
    b = normed(h)
    next_a[...] = b
    next_a_t[...] = b.T


def layer_0(x, w_gate, w_up, w_down):
    tokens, d = x.shape
    ff = w_gate.shape[2]
    rows = 256
    anywhere = pl.BlockSpec(memory_space=pl.ANY)
    tall = lambda n: pl.BlockSpec((rows, n), lambda i: (i, 0))
    wide = lambda n: pl.BlockSpec((n, rows), lambda i: (0, i))
    return pl.pallas_call(
        functools.partial(forward_kernel, tokens // rows),
        grid=(tokens // rows,),
        in_specs=[tall(d), anywhere, anywhere, anywhere],
        out_specs=[tall(ff), tall(ff), wide(ff), wide(d), tall(d), tall(d), wide(d)],
        out_shape=[
            jax.ShapeDtypeStruct((tokens, ff), F32),
            jax.ShapeDtypeStruct((tokens, ff), F32),
            jax.ShapeDtypeStruct((ff, tokens), BF16),
            jax.ShapeDtypeStruct((d, tokens), BF16),
            jax.ShapeDtypeStruct((tokens, d), BF16),
            jax.ShapeDtypeStruct((tokens, d), BF16),
            jax.ShapeDtypeStruct((d, tokens), BF16),
        ],
        scratch_shapes=[pltpu.VMEM((d, ff), BF16), pltpu.VMEM((d, ff), BF16), pltpu.VMEM((ff, d), BF16), pltpu.SemaphoreType.DMA((3,))],
        compiler_params=pltpu.CompilerParams(vmem_limit_bytes=60 * 2**20),
        name="forward",
    )(x, w_gate, w_up, w_down)


SENT = 3


class Exchange:
    def __init__(self, n, refs, kinds, lags):
        self.lags = lags
        self.mine, self.pair, self.out2, self.out3, self.in2, self.in3, self.pair_sem, self.sem2, self.sem3 = refs
        self.kinds = kinds
        self.me, self.core, self.partner, self.after, self.before, _ = places("dp", n)
        chips = n // CORES
        chip = lax.div(self.me, CORES)
        self.chip = chip
        self.chip_after, self.chip_before, self.chip_across = (lax.rem(chip + k, chips) for k in (1, chips - 1, chips // 2))

    @staticmethod
    def scratch(n, rows, width, lags):
        chips, half, dma = n // CORES, width // 2, pltpu.SemaphoreType.DMA
        held, slots = lags[3] + 1, lags[3] + 3
        return [
            pltpu.VMEM((held, chips, CORES, rows, width), BF16),
            pltpu.VMEM((slots, chips, rows, width), BF16),
            pltpu.VMEM((2, SENT, rows, width), BF16),
            pltpu.VMEM((2, SENT, rows, half), BF16),
            pltpu.VMEM((2, slots, rows, width), BF16),
            pltpu.VMEM((2, slots, rows, half), BF16),
            dma((2, slots)), dma((2, 2, slots)), dma((2, 2, slots)),
        ]

    def slot(self, p):
        return lax.rem(p, self.pair.shape[0])

    def held(self, p):
        return lax.rem(p, self.mine.shape[0])

    def barrier(self):
        barrier = pltpu.get_barrier_semaphore()
        for peer in (self.partner, self.after, self.before):
            pl.semaphore_signal(barrier, inc=1, device_id={"dp": peer}, device_id_type=MESH)
        pl.semaphore_wait(barrier, 3)

    def copy1(self, p, rows):
        slot = self.slot(p)
        return pltpu.make_async_remote_copy(
            self.mine.at[self.held(p), :, 1 - self.core, pl.ds(0, rows)], self.pair.at[slot, :, pl.ds(0, rows)],
            self.pair_sem.at[0, slot], self.pair_sem.at[1, slot], device_id={"dp": self.partner}, device_id_type=MESH,
        )

    def copies(self, p, rows, out, into, sem):
        slot = self.slot(p)
        return [
            pltpu.make_async_remote_copy(
                out.at[way, lax.rem(p, SENT), pl.ds(0, rows)], into.at[way, slot, pl.ds(0, rows)],
                sem.at[0, way, slot], sem.at[1, way, slot], device_id={"dp": to}, device_id_type=MESH,
            )
            for way, to in enumerate((self.after, self.before))
        ]

    def over(self, rows, body):
        body(pl.ds(0, rows))

    def of_chip(self, p, chip, at, columns):
        a = self.mine[self.held(p), chip, self.core, at, columns].astype(F32)
        return a + self.pair[self.slot(p), chip, at, columns].astype(F32)

    def stage1(self, p, rows, _):
        self.copy1(p, rows).start()

    def stage2(self, p, rows, _):
        self.copy1(p, rows).wait()
        slot = lax.rem(p, SENT)
        half = self.out3.shape[-1]
        left, right = slice(0, half), slice(half, 2 * half)

        def body(at):
            self.out2[0, slot, at, left] = self.of_chip(p, self.chip_across, at, left).astype(BF16)
            self.out2[0, slot, at, right] = self.of_chip(p, self.chip_after, at, right).astype(BF16)
            self.out2[1, slot, at, left] = self.of_chip(p, self.chip_before, at, left).astype(BF16)
            self.out2[1, slot, at, right] = self.of_chip(p, self.chip_across, at, right).astype(BF16)

        self.over(rows, body)
        for one in self.copies(p, rows, self.out2, self.in2, self.sem2):
            one.start()

    def stage3(self, p, rows, _):
        for one in self.copies(p, rows, self.out2, self.in2, self.sem2):
            one.wait()
        slot, arrived = lax.rem(p, SENT), self.slot(p)
        half = self.out3.shape[-1]
        left, right = slice(0, half), slice(half, 2 * half)

        def body(at):
            self.out3[0, slot, at] = (self.of_chip(p, self.chip_after, at, left) + self.in2[0, arrived, at, left].astype(F32)).astype(BF16)
            self.out3[1, slot, at] = (self.of_chip(p, self.chip_before, at, right) + self.in2[1, arrived, at, right].astype(F32)).astype(BF16)

        self.over(rows, body)
        for one in self.copies(p, rows, self.out3, self.in3, self.sem3):
            one.start()

    def stage4(self, p, rows, keep):
        for one in self.copies(p, rows, self.out3, self.in3, self.sem3):
            one.wait()
        arrived = self.slot(p)
        half = self.out3.shape[-1]
        left, right = slice(0, half), slice(half, 2 * half)

        def body(at):
            a = self.of_chip(p, self.chip, at, left) + (self.in3[0, arrived, at].astype(F32) + self.in2[1, arrived, at, left].astype(F32))
            b = self.of_chip(p, self.chip, at, right) + (self.in2[0, arrived, at, right].astype(F32) + self.in3[1, arrived, at].astype(F32))
            keep(p, at, a.astype(BF16), b.astype(BF16))

        self.over(rows, body)

    def move(self, step, low, high):
        for lag, stage in zip(self.lags, (self.stage1, self.stage2, self.stage3, self.stage4), strict=True):
            for first, end, rows, keep in self.kinds:
                if high - 1 - lag < first or low - lag >= end:
                    continue
                p = step - lag
                if low - lag >= first and high - 1 - lag < end:
                    stage(p, rows, keep)
                else:
                    pl.when((p >= first) & (p < end))(functools.partial(stage, p, rows, keep))


def keep_columns(first, gate, up, width):
    def keep(p, at, left, right):
        columns = pl.ds(pl.multiple_of((p - first) * width, width), width)
        gate[at, columns] = left
        up[at, columns] = right

    return keep


def keep_down(first, down, rows, width):
    def keep(p, at, left, right):
        half = width // 2
        which = p - first
        at = pl.ds(pl.multiple_of(lax.rem(which, 2) * rows + at.start, 16), at.size)
        start = lax.div(which, 2) * width
        down[at, pl.ds(pl.multiple_of(start, half), half)] = left
        down[at, pl.ds(pl.multiple_of(start + half, half), half)] = right

    return keep


def down_packet(exchange, step, first, hidden_t, by_out):
    n_rows = hidden_t.shape[0]
    _, chips, cores, rows, width = exchange.mine.shape
    which = step - first
    start = pl.multiple_of(lax.rem(which, 2) * rows, 16)
    columns = pl.ds(pl.multiple_of(lax.div(which, 2) * width, width), width)
    share = n_rows // (chips * cores)
    by_out = by_out[:, columns]
    for k in range(chips * cores):
        lhs = hidden_t[pl.ds(pl.multiple_of(k * share + start, 16), rows), :]
        exchange.mine[exchange.held(step), k // cores, k % cores] = dot(lhs, by_out).astype(BF16)


def wide_packet(exchange, step, a_t, by_both):
    _, chips, cores, _, width = exchange.mine.shape
    rows = a_t.shape[0] // (chips * cores)
    half = width // 2
    for k in range(2):
        columns = slice(k * half, k * half + half)
        block = dot(a_t[...], by_both[:, columns]).astype(BF16)
        exchange.mine[exchange.held(step), :, :, pl.ds(0, rows), columns] = block.reshape(chips, cores, rows, half)


MB = 512
TOP_LAGS = (0, 1, 2, 3)
BOTTOM_LAGS = (0, 1, 3, 5)


def top_kernel(n, *refs):
    (a_in, at_in, h_in, dy_in, w_gate, w_up, w_down), refs = refs[:7], refs[7:]
    (g_gate, g_up, g_down, by_h, bg_hbm, bu_hbm), refs = refs[:6], refs[6:]
    (a, a_t, dy, wg, wu, hidden_t, wd, both, h_tile, by_tile, load_sem, wd_sem, both_sem, tile_sem, by_sem), refs = refs[:15], refs[15:]
    tokens, d = a.shape
    ff = wg.shape[1]
    width = 256
    chunks = ff // width
    downs = 4
    wide_rows, down_rows = d // n, ff // n // 2
    exchange = Exchange(
        n, refs,
        (
            (0, chunks, wide_rows, keep_columns(0, g_gate, g_up, width)),
            (chunks, chunks + downs, down_rows, keep_down(chunks, g_down, down_rows, 2 * width)),
        ),
        TOP_LAGS,
    )
    layer = w_gate.shape[0] - 1
    first, rest = pl.ds(0, width), pl.ds(width, ff - width)
    loads = [
        pltpu.make_async_copy(a_in, a, load_sem.at[0]),
        pltpu.make_async_copy(w_gate.at[layer, :, first], wg.at[:, first], load_sem.at[1]),
        pltpu.make_async_copy(w_up.at[layer, :, first], wu.at[:, first], load_sem.at[2]),
        pltpu.make_async_copy(dy_in, dy, load_sem.at[3]),
        pltpu.make_async_copy(at_in, a_t, load_sem.at[4]),
        pltpu.make_async_copy(w_gate.at[layer, :, rest], wg.at[:, rest], load_sem.at[5]),
        pltpu.make_async_copy(w_up.at[layer, :, rest], wu.at[:, rest], load_sem.at[6]),
    ]

    def down_chunk(c):
        slot = lax.rem(c, 2)
        return pltpu.make_async_copy(w_down.at[layer, pl.ds(pl.multiple_of(c * width, width), width)], wd.at[slot], wd_sem.at[slot])

    for one in loads[:4]:
        one.start()
    down_chunk(0).start()
    for one in loads[4:]:
        one.start()
    exchange.barrier()

    def store_both(c, k):
        slot = lax.rem(c, 2)
        return pltpu.make_async_copy(
            both.at[slot, :, pl.ds(k * width, width)],
            (bg_hbm, bu_hbm)[k].at[:, pl.ds(pl.multiple_of(c * width, width), width)],
            both_sem.at[k, slot],
        )

    def chunk(c, _):
        slot = lax.rem(c, 2)

        @pl.when(c == 0)
        def _():
            for one in loads[:5]:
                one.wait()

        @pl.when(c == 1)
        def _():
            for one in loads[5:]:
                one.wait()

        @pl.when(c >= 2)
        def _():
            for k in range(2):
                store_both(c - 2, k).wait()

        down_chunk(c).wait()

        @pl.when(c + 1 < chunks)
        def _():
            down_chunk(c + 1).start()

        columns = pl.ds(pl.multiple_of(c * width, width), width)
        wg_c, wu_c, wd_c = wg[:, columns], wu[:, columns], wd[slot]
        for at in range(0, tokens, MB):
            rows = slice(at, at + MB)
            hidden, by_gate, by_up = by_units(dot(a[rows], wg_c), dot(a[rows], wu_c), dot(dy[rows], wd_c, ((1,), (1,))))
            hidden_t[columns, rows] = hidden.astype(BF16).T
            both[slot, rows, :width] = by_gate.astype(BF16)
            both[slot, rows, width:] = by_up.astype(BF16)
        wide_packet(exchange, c, a_t, both.at[slot])
        for k in range(2):
            store_both(c, k).start()
        exchange.move(c, 0, chunks)
        return 0

    lax.fori_loop(0, chunks, chunk, 0)
    for c in (chunks - 2, chunks - 1):
        for k in range(2):
            store_both(c, k).wait()

    tile_rows = 256
    tiles = tokens // tile_rows
    split = a_t.shape[1]

    def tile_loads(t):
        slot = lax.rem(t, 2)
        rows = pl.ds(pl.multiple_of(t * tile_rows, tile_rows), tile_rows)
        got = []
        for k, src in enumerate((bg_hbm, bu_hbm)):
            to = pl.ds(pl.multiple_of((slot * 2 + k) * tile_rows, tile_rows), tile_rows)
            got.append(pltpu.make_async_copy(src.at[rows, pl.ds(0, split)], a_t.at[to], tile_sem.at[2 * k, slot]))
            got.append(pltpu.make_async_copy(src.at[rows, pl.ds(split, ff - split)], a.at[to, pl.ds(0, ff - split)], tile_sem.at[2 * k + 1, slot]))
        got.append(pltpu.make_async_copy(h_in.at[rows], h_tile.at[slot], tile_sem.at[4, slot]))
        return got

    def tile_store(t):
        slot = lax.rem(t, 2)
        return pltpu.make_async_copy(by_tile.at[slot], by_h.at[pl.ds(pl.multiple_of(t * tile_rows, tile_rows), tile_rows)], by_sem.at[slot])

    for one in tile_loads(0):
        one.start()

    def tile(step, _):
        t = step - chunks

        @pl.when(t < downs)
        def _():
            down_packet(exchange, step, chunks, hidden_t, dy)

        exchange.move(step, chunks, chunks + tiles)
        slot = lax.rem(t, 2)
        for one in tile_loads(t):
            one.wait()

        @pl.when(t + 1 < tiles)
        def _():
            for one in tile_loads(t + 1):
                one.start()

        @pl.when(t >= 2)
        def _():
            tile_store(t - 2).wait()

        total = None
        for k, w in enumerate((wg, wu)):
            at = pl.ds(pl.multiple_of((slot * 2 + k) * tile_rows, tile_rows), tile_rows)
            term = dot(a_t[at], w[:, :split], ((1,), (1,))) + dot(a[at, : ff - split], w[:, split:], ((1,), (1,)))
            total = term if total is None else total + term
        rows = pl.ds(pl.multiple_of(t * tile_rows, tile_rows), tile_rows)
        by_tile[slot] = (dy[rows].astype(F32) + by_norm(h_tile[slot], total)).astype(BF16)
        tile_store(t).start()
        return 0

    lax.fori_loop(chunks, chunks + tiles, tile, 0)
    for t in (tiles - 2, tiles - 1):
        tile_store(t).wait()


def top_layer(n, a, a_t, h, dy, w_gate, w_up, w_down):
    tokens, d = a.shape
    ff = w_gate.shape[2]
    width = 256
    anywhere, inside = pl.BlockSpec(memory_space=pl.ANY), pl.BlockSpec(memory_space=pltpu.VMEM)
    dma = pltpu.SemaphoreType.DMA
    return pl.pallas_call(
        functools.partial(top_kernel, n),
        in_specs=[anywhere] * 7,
        out_specs=[inside] * 3 + [anywhere] * 3,
        out_shape=[
            jax.ShapeDtypeStruct((d // n, ff), BF16),
            jax.ShapeDtypeStruct((d // n, ff), BF16),
            jax.ShapeDtypeStruct((ff // n, d), BF16),
            jax.ShapeDtypeStruct((tokens, d), BF16),
            jax.ShapeDtypeStruct((tokens, ff), BF16),
            jax.ShapeDtypeStruct((tokens, ff), BF16),
        ],
        scratch_shapes=[
            pltpu.VMEM((tokens, d), BF16), pltpu.VMEM((d, tokens), BF16), pltpu.VMEM((tokens, d), BF16),
            pltpu.VMEM((d, ff), BF16), pltpu.VMEM((d, ff), BF16), pltpu.VMEM((ff, tokens), BF16),
            pltpu.VMEM((2, width, d), BF16), pltpu.VMEM((2, tokens, 2 * width), BF16),
            pltpu.VMEM((2, 256, d), BF16), pltpu.VMEM((2, 256, d), BF16),
            dma((7,)), dma((2,)), dma((2, 2)), dma((5, 2)), dma((2,)),
            *Exchange.scratch(n, ff // n // 2, 2 * width, TOP_LAGS),
        ],
        compiler_params=pltpu.CompilerParams(collective_id=2, has_side_effects=True, vmem_limit_bytes=67043328),
        name="top",
    )(a, a_t, h, dy, w_gate, w_up, w_down)


def bottom_kernel(n, *refs):
    (by_in, ht_in, at_in, gate_in, up_in, w_down), refs = refs[:6], refs[6:]
    (g_gate, g_up, g_down), refs = refs[:3], refs[3:]
    (by, hidden_t, a_t, wd, gate, up, both, load_sem, wd_sem, unit_sem), refs = refs[:10], refs[10:]
    tokens, d = by.shape
    ff = hidden_t.shape[0]
    width = 256
    chunks = ff // width
    downs = 4
    wide_rows, down_rows = d // n, ff // n // 2
    exchange = Exchange(
        n, refs,
        (
            (0, downs, down_rows, keep_down(0, g_down, down_rows, 2 * width)),
            (downs, downs + chunks, wide_rows, keep_columns(downs, g_gate, g_up, width)),
        ),
        BOTTOM_LAGS,
    )
    share = ff // n
    halves = lambda ref, k: ref.at[:, pl.ds(k * 2 * width, 2 * width)]
    loads = [pltpu.make_async_copy(halves(by_in, 0), halves(by, 0), load_sem.at[0])]
    for k in range(2):
        for to in range(n):
            rows = pl.ds(to * share + k * down_rows, down_rows)
            loads.append(pltpu.make_async_copy(ht_in.at[rows], hidden_t.at[rows], load_sem.at[3 + k * n + to]))
    loads.append(pltpu.make_async_copy(halves(by_in, 1), halves(by, 1), load_sem.at[1]))
    loads.append(pltpu.make_async_copy(at_in, a_t, load_sem.at[2]))

    def chunk_loads(c):
        slot = lax.rem(c, 2)
        columns = pl.ds(pl.multiple_of(c * width, width), width)
        return [
            pltpu.make_async_copy(w_down.at[0, columns], wd.at[slot], wd_sem.at[slot]),
            pltpu.make_async_copy(gate_in.at[:, columns], gate.at[slot], unit_sem.at[0, slot]),
            pltpu.make_async_copy(up_in.at[:, columns], up.at[slot], unit_sem.at[1, slot]),
        ]

    for one in (*loads, *chunk_loads(0)):
        one.start()
    exchange.barrier()

    def down(step, _):
        @pl.when(step == 0)
        def _():
            for one in loads[: 1 + n]:
                one.wait()

        @pl.when(step == 1)
        def _():
            for one in loads[1 + n :]:
                one.wait()

        down_packet(exchange, step, 0, hidden_t, by)
        exchange.move(step, 0, downs)
        return 0

    lax.fori_loop(0, downs, down, 0)

    def chunk(step, _):
        c = step - downs
        slot = lax.rem(c, 2)
        for one in chunk_loads(c):
            one.wait()

        @pl.when(c + 1 < chunks)
        def _():
            for one in chunk_loads(c + 1):
                one.start()

        wd_c = wd[slot]
        for at in range(0, tokens, MB):
            rows = slice(at, at + MB)
            _, by_gate, by_up = by_units(gate[slot, rows], up[slot, rows], dot(by[rows], wd_c, ((1,), (1,))))
            both[rows, :width] = by_gate.astype(BF16)
            both[rows, width:] = by_up.astype(BF16)
        wide_packet(exchange, step, a_t, both)
        exchange.move(step, downs, downs + chunks)
        return 0

    lax.fori_loop(downs, downs + chunks, chunk, 0)
    for step in range(downs + chunks, downs + chunks + BOTTOM_LAGS[-1]):
        exchange.move(step, step, step + 1)


def bottom_layer(n, by, hidden_t, a_t, gate, up, w_down):
    tokens, d = by.shape
    ff = hidden_t.shape[0]
    width = 256
    anywhere, inside = pl.BlockSpec(memory_space=pl.ANY), pl.BlockSpec(memory_space=pltpu.VMEM)
    dma = pltpu.SemaphoreType.DMA
    return pl.pallas_call(
        functools.partial(bottom_kernel, n),
        in_specs=[anywhere] * 6,
        out_specs=[inside] * 3,
        out_shape=[
            jax.ShapeDtypeStruct((d // n, ff), BF16),
            jax.ShapeDtypeStruct((d // n, ff), BF16),
            jax.ShapeDtypeStruct((ff // n, d), BF16),
        ],
        scratch_shapes=[
            pltpu.VMEM((tokens, d), BF16), pltpu.VMEM((ff, tokens), BF16), pltpu.VMEM((d, tokens), BF16),
            pltpu.VMEM((2, width, d), BF16), pltpu.VMEM((2, tokens, width), F32), pltpu.VMEM((2, tokens, width), F32),
            pltpu.VMEM((tokens, 2 * width), BF16),
            dma((3 + 2 * n,)), dma((2,)), dma((2, 2)),
            *Exchange.scratch(n, ff // n // 2, 2 * width, BOTTOM_LAGS),
        ],
        compiler_params=pltpu.CompilerParams(collective_id=3, has_side_effects=True, vmem_limit_bytes=67043328),
        name="bottom",
    )(by, hidden_t, a_t, gate, up, w_down)


def solution(mesh):
    n = mesh.shape["dp"]

    def step(x, dy, w_gate, w_up, w_down, *moments):
        gate, up, hidden_t, a_t, h, next_a, next_a_t = layer_0(x[0], w_gate, w_up, w_down)
        *top, by_h, _, _ = top_layer(n, next_a, next_a_t, h, dy[0], w_gate, w_up, w_down)
        bottom = bottom_layer(n, by_h, hidden_t, a_t, gate, up, w_down)
        gradients = list(zip(bottom, top, strict=True))
        return tuple(finish(n, gradients, (w_gate, w_up, w_down), moments[:3], moments[3:]))

    sharded = P(None, "dp", None)
    return jax.shard_map(
        step,
        mesh=mesh,
        in_specs=(P(("rep", "dp")), P(("rep", "dp")), P(), P(), P(), *[sharded] * 6),
        out_specs=(*[P("rep")] * 3, *[P("rep", "dp")] * 6),
        check_vma=False,
    )
```

```python
import functools

import jax
import jax.numpy as jnp
from jax import lax
from jax.experimental import pallas as pl
from jax.experimental.pallas import tpu as pltpu
from jax.sharding import PartitionSpec as P

MESH = pl.DeviceIdType.MESH
F32, BF16 = jnp.float32, jnp.bfloat16
CORES = 2


def places(axis, n):
    me = lax.axis_index(axis)
    chips = n // CORES
    core, chip = lax.rem(me, CORES), lax.div(me, CORES)
    at = lambda away: lax.rem(chip + away, chips) * CORES + core
    return me, core, me + 1 - 2 * core, at(1), at(chips - 1), at(2)


def finish_kernel(n, count, pieces, *refs):
    layers = 2
    squares, refs = refs[:layers], refs[layers:]
    g_in, refs = [refs[layers * i : layers * i + layers] for i in range(3)], refs[3 * layers :]
    w_in, m_in, v_in, w, m, v = (refs[3 * i : 3 * i + 3] for i in range(6))
    g, refs = refs[18:21], refs[21:]
    parts, load_sem, part_send, part_recv, send, recv = refs
    me, core, partner, after, before, across = places("dp", n)

    barrier = pltpu.get_barrier_semaphore()
    peers = [lax.rem(me + away, n) for away in range(1, n)]
    for peer in peers:
        pl.semaphore_signal(barrier, inc=1, device_id={"dp": peer}, device_id_type=MESH)

    def rows_of(i, owner, first, rows):
        return pl.ds(pl.multiple_of(owner * g[i].shape[1] + first, 16), rows)

    order = (2, 0, 1)
    loads = {}
    for i in order:
        rows = rows_of(i, me, 0, g[i].shape[1])
        pairs = [(w_in[i].at[:, rows], w[i].at[:, rows]), (m_in[i], m[i]), (v_in[i], v[i])]
        pairs += [(g_in[i][k], g[i].at[k]) for k in range(layers)]
        loads[i] = [pltpu.make_async_copy(src, dst, load_sem.at[i, k]) for k, (src, dst) in enumerate(pairs)]
    for one in loads[order[0]]:
        one.start()

    total = squares[0][...] + squares[1][...]
    parts[pl.ds(me, 1)] = total[None]
    pl.semaphore_wait(barrier, n - 1)
    part_copies = []
    for k, peer in enumerate(peers):
        part_copies.append(
            pltpu.make_async_remote_copy(
                parts.at[me], parts.at[me], part_send.at[k], part_recv.at[k], device_id={"dp": peer}, device_id_type=MESH
            )
        )
        part_copies[-1].start()
    for one in part_copies:
        one.wait_recv()
    every = parts[0]
    for k in range(1, n):
        every += parts[k]
    mean = jnp.sum(every, keepdims=True) / count
    factor = jnp.minimum(1.0, 0.5 * lax.rsqrt(mean + 1e-30))

    def adamw(i, layer, first, rows):
        step_rows = 16

        def body(step, _):
            start = first + step * step_rows
            at = (layer, pl.ds(pl.multiple_of(start, 16), step_rows), slice(None))
            mine = (layer, rows_of(i, me, start, step_rows), slice(None))
            grad = g[i][at].astype(F32) * factor
            m_new = 0.9 * m[i][at] + 0.1 * grad
            v_new = 0.95 * v[i][at] + 0.05 * grad * grad
            w_old = w[i][mine].astype(F32)
            m[i][at] = m_new
            v[i][at] = v_new
            w[i][mine] = (w_old - 0.02 * (m_new * lax.rsqrt(v_new + 1e-8) + 0.1 * w_old)).astype(BF16)
            return 0

        lax.fori_loop(0, rows // step_rows, body, 0)

    def piece(number):
        i, layer, first, rows = pieces[number]
        half = g[i].shape[2] // 2
        left, right = pl.ds(0, half), pl.ds(half, half)

        def copy(kind, to, owner, columns=slice(None)):
            place = w[i].at[layer, rows_of(i, owner, first, rows), columns]
            return pltpu.make_async_remote_copy(
                place, place, send.at[kind, number], recv.at[kind, number], device_id={"dp": to}, device_id_type=MESH
            )

        return {
            "after": copy(0, after, me),
            "before": copy(1, before, me),
            "partner": copy(2, partner, me),
            "on": copy(3, after, before, left),
            "back": copy(4, before, after, right),
            "partner_before": copy(5, partner, before),
            "partner_after": copy(6, partner, after),
            "partner_left": copy(7, partner, across, left),
            "partner_right": copy(8, partner, across, right),
        }

    waited = set()
    total_pieces = len(pieces)
    made = [piece(number) for number in range(total_pieces)]

    def compute(number):
        i, layer, first, rows = pieces[number]
        if i not in waited:
            waited.add(i)
            for one in loads[i]:
                one.wait()
        adamw(i, layer, first, rows)

    def own_piece(number):
        compute(number)
        for kind in ("after", "before", "partner"):
            made[number][kind].start()

    own_piece(0)
    for i in order[1:]:
        for one in loads[i]:
            one.start()
    for number in range(total_pieces + 2):
        if number + 1 < total_pieces:
            own_piece(number + 1)
        if 1 <= number <= total_pieces:
            copies = made[number - 1]
            copies["after"].wait_recv()
            copies["on"].start()
            copies["partner_before"].start()
            copies["before"].wait_recv()
            copies["back"].start()
            copies["partner_after"].start()
        if 2 <= number:
            copies = made[number - 2]
            copies["on"].wait_recv()
            copies["partner_left"].start()
            copies["back"].wait_recv()
            copies["partner_right"].start()
    for copies in made:
        for kind in ("partner", "partner_before", "partner_after", "partner_left", "partner_right"):
            copies[kind].wait_recv()
        for one in copies.values():
            one.wait_send()
    for one in part_copies:
        one.wait_send()


def store_kernel(*refs):
    *refs, sem = refs
    some = len(refs) // 2
    copies = [pltpu.make_async_copy(refs[k], refs[some + k], sem.at[k]) for k in range(some)]
    for one in copies:
        one.start()
    for one in copies:
        one.wait()


def finish(n, gradients, squares, weights, m, v):
    count = float(sum(w.size for w in weights))
    layers = len(gradients[0])
    pieces = []
    for i in (2, 0, 1):
        rows, _ = gradients[i][0].shape
        for layer in range(layers):
            half = rows // 2
            cuts = [half, half]
            if (i, layer) == (2, 0):
                cuts = [48, half - 48, half]
            elif (i, layer) == (1, layers - 1):
                cuts = [half, half // 2, half // 4, half // 4]
            for cut in cuts:
                pieces.append((i, layer, sum(p[3] for p in pieces if p[:2] == (i, layer)), cut))
    anywhere, inside = pl.BlockSpec(memory_space=pl.ANY), pl.BlockSpec(memory_space=pltpu.VMEM)
    dma = pltpu.SemaphoreType.DMA
    results = [*weights, *m, *v]
    ready = pl.pallas_call(
        functools.partial(finish_kernel, n, count, tuple(pieces)),
        out_shape=[pltpu.VMEM(t.shape, t.dtype) for t in results],
        in_specs=[inside] * layers + [anywhere] * (3 * layers + 9),
        out_specs=[inside] * 9,
        scratch_shapes=[
            *[pltpu.VMEM((layers, *one[0].shape), BF16) for one in gradients],
            pltpu.VMEM((n, 8, 128), F32),
            dma((3, layers + 3)), dma((n - 1,)), dma((n - 1,)), dma((9, len(pieces))), dma((9, len(pieces))),
        ],
        compiler_params=pltpu.CompilerParams(collective_id=4, has_side_effects=True, vmem_limit_bytes=7 * 2**20),
        name="finish",
    )(*squares, *sum(gradients, ()), *weights, *m, *v)
    return pl.pallas_call(
        store_kernel,
        out_shape=[jax.ShapeDtypeStruct(t.shape, t.dtype) for t in results],
        in_specs=[inside] * 9,
        out_specs=[anywhere] * 9,
        scratch_shapes=[dma((9,))],
        compiler_params=pltpu.CompilerParams(vmem_limit_bytes=7*2**20),
        name="store",
    )(*[pltpu.with_memory_space_constraint(t, pltpu.VMEM) for t in ready])


def dot(a, b, contract=((1,), (0,))):
    return lax.dot_general(a, b, (contract, ((), ())), preferred_element_type=F32)


def normed(h):
    wide = h.astype(F32)
    return (wide * lax.rsqrt(jnp.mean(wide * wide, -1, keepdims=True) + 1e-6)).astype(BF16)


def by_norm(h, by_a):
    wide = h.astype(F32)
    scale = lax.rsqrt(jnp.mean(wide * wide, -1, keepdims=True) + 1e-6)
    return scale * by_a - wide * (scale * scale * scale * jnp.mean(by_a * wide, -1, keepdims=True))


def by_units(gate, up, by_hidden):
    by_hidden = by_hidden.astype(BF16).astype(F32)
    s = jax.nn.sigmoid(gate)
    silu = gate * s
    return silu * up, by_hidden * up * (s + silu * (1.0 - s)), by_hidden * silu


def forward_kernel(tiles, x, w_gate, w_up, w_down, gate_out, up_out, hidden_t, a_t, h_out, next_a, next_a_t, wg, wu, wd, sem):
    tile = pl.program_id(0)
    loads = [pltpu.make_async_copy(src.at[0], dst, sem.at[k]) for k, (src, dst) in enumerate(((w_gate, wg), (w_up, wu), (w_down, wd)))]

    @pl.when(tile == 0)
    def _():
        for one in loads[:2]:
            one.start()

    a = normed(x[...])
    a_t[...] = a.T

    @pl.when(tile == 0)
    def _():
        loads[0].wait()
        loads[1].wait()
        loads[2].start()

    columns = wg.shape[1]
    width = 256
    hidden = []
    for at in range(0, columns, width):
        gate = dot(a, wg[:, at : at + width])
        up = dot(a, wu[:, at : at + width])
        gate_out[:, at : at + width] = gate
        up_out[:, at : at + width] = up
        hidden.append((gate * jax.nn.sigmoid(gate) * up).astype(BF16))
        hidden_t[at : at + width, :] = hidden[-1].T

    @pl.when(tile == 0)
    def _():
        loads[2].wait()

    h = x[...] + dot(jnp.concatenate(hidden, 1), wd[...]).astype(BF16)
    h_out[...] = h
    b = normed(h)
    next_a[...] = b
    next_a_t[...] = b.T


def layer_0(x, w_gate, w_up, w_down):
    tokens, d = x.shape
    ff = w_gate.shape[2]
    rows = 256
    anywhere = pl.BlockSpec(memory_space=pl.ANY)
    tall = lambda n: pl.BlockSpec((rows, n), lambda i: (i, 0))
    wide = lambda n: pl.BlockSpec((n, rows), lambda i: (0, i))
    return pl.pallas_call(
        functools.partial(forward_kernel, tokens // rows),
        grid=(tokens // rows,),
        in_specs=[tall(d), anywhere, anywhere, anywhere],
        out_specs=[tall(ff), tall(ff), wide(ff), wide(d), tall(d), tall(d), wide(d)],
        out_shape=[
            jax.ShapeDtypeStruct((tokens, ff), F32),
            jax.ShapeDtypeStruct((tokens, ff), F32),
            jax.ShapeDtypeStruct((ff, tokens), BF16),
            jax.ShapeDtypeStruct((d, tokens), BF16),
            jax.ShapeDtypeStruct((tokens, d), BF16),
            jax.ShapeDtypeStruct((tokens, d), BF16),
            jax.ShapeDtypeStruct((d, tokens), BF16),
        ],
        scratch_shapes=[pltpu.VMEM((d, ff), BF16), pltpu.VMEM((d, ff), BF16), pltpu.VMEM((ff, d), BF16), pltpu.SemaphoreType.DMA((3,))],
        compiler_params=pltpu.CompilerParams(vmem_limit_bytes=60 * 2**20),
        name="forward",
    )(x, w_gate, w_up, w_down)


class Exchange:
    def __init__(self, n, refs, kinds, lags):
        self.mine, self.pair, self.out2, self.out3, self.in2, self.in3, self.own, self.side, self.pair_sem, self.sem2, self.sem3 = refs
        self.kinds = kinds
        self.lags = lags
        self.me, self.core, self.partner, self.after, self.before, _ = places("dp", n)
        chips = n // CORES
        self.chip = lax.div(self.me, CORES)
        self.chip_after, self.chip_before, self.chip_across = (lax.rem(self.chip + k, chips) for k in (1, chips - 1, chips // 2))
        half = self.out3.shape[-1]
        self.left, self.right = slice(0, half), slice(half, 2 * half)

    @staticmethod
    def scratch(n, rows, width, lags):
        chips, half, dma = n // CORES, width // 2, pltpu.SemaphoreType.DMA
        _, two, three, four = lags
        slots1, slots2, slots3 = two + 3, 2 * (three - two) + 2, 2 * (four - three) + 2
        return [
            pltpu.VMEM((two + 1, chips, CORES, rows, width), BF16),
            pltpu.VMEM((slots1, chips, rows, width), BF16),
            pltpu.VMEM((2, three - two + 1, rows, width), BF16),
            pltpu.VMEM((2, four - three + 1, rows, half), BF16),
            pltpu.VMEM((2, slots2, rows, width), BF16),
            pltpu.VMEM((2, slots3, rows, half), BF16),
            pltpu.VMEM((four - two + 1, rows, width), F32),
            pltpu.VMEM((2, three - two + 1, rows, half), F32),
            dma((2, slots1)), dma((2, 2, slots2)), dma((2, 2, slots3)),
        ]

    def held(self, p):
        return lax.rem(p, self.mine.shape[0])

    def barrier(self):
        barrier = pltpu.get_barrier_semaphore()
        for peer in (self.partner, self.after, self.before):
            pl.semaphore_signal(barrier, inc=1, device_id={"dp": peer}, device_id_type=MESH)
        pl.semaphore_wait(barrier, 3)

    def copy1(self, p, rows):
        slot = lax.rem(p, self.pair.shape[0])
        return pltpu.make_async_remote_copy(
            self.mine.at[self.held(p), :, 1 - self.core, pl.ds(0, rows)], self.pair.at[slot, :, pl.ds(0, rows)],
            self.pair_sem.at[0, slot], self.pair_sem.at[1, slot], device_id={"dp": self.partner}, device_id_type=MESH,
        )

    def copies(self, p, rows, out, into, sem):
        slot = lax.rem(p, into.shape[1])
        return [
            pltpu.make_async_remote_copy(
                out.at[way, lax.rem(p, out.shape[1]), pl.ds(0, rows)], into.at[way, slot, pl.ds(0, rows)],
                sem.at[0, way, slot], sem.at[1, way, slot], device_id={"dp": to}, device_id_type=MESH,
            )
            for way, to in enumerate((self.after, self.before))
        ]

    def copies2(self, p, rows):
        return self.copies(p, rows, self.out2, self.in2, self.sem2)

    def copies3(self, p, rows):
        return self.copies(p, rows, self.out3, self.in3, self.sem3)

    def stage1(self, p, rows, _):
        self.copy1(p, rows).start()

    def stage2(self, p, rows, _):
        self.copy1(p, rows).wait()
        slot, own, side = (lax.rem(p, t.shape[k]) for t, k in ((self.out2, 1), (self.own, 0), (self.side, 1)))
        at = slice(0, rows)

        def of_chip(chip, columns):
            a = self.mine[self.held(p), chip, self.core, at, columns].astype(F32)
            return a + self.pair[lax.rem(p, self.pair.shape[0]), chip, at, columns].astype(F32)

        self.out2[0, slot, at, self.left] = of_chip(self.chip_across, self.left).astype(BF16)
        self.out2[0, slot, at, self.right] = of_chip(self.chip_after, self.right).astype(BF16)
        self.out2[1, slot, at, self.left] = of_chip(self.chip_before, self.left).astype(BF16)
        self.out2[1, slot, at, self.right] = of_chip(self.chip_across, self.right).astype(BF16)
        for one in self.copies2(p, rows):
            one.start()
        self.side[0, side, at] = of_chip(self.chip_after, self.left)
        self.side[1, side, at] = of_chip(self.chip_before, self.right)
        for columns in (self.left, self.right):
            self.own[own, at, columns] = of_chip(self.chip, columns)

    def stage3(self, p, rows, _):
        for one in self.copies2(p, rows):
            one.wait()
        slot, arrived, own, side = (lax.rem(p, t.shape[k]) for t, k in ((self.out3, 1), (self.in2, 1), (self.own, 0), (self.side, 1)))
        at = slice(0, rows)
        self.out3[0, slot, at] = (self.side[0, side, at] + self.in2[0, arrived, at, self.left].astype(F32)).astype(BF16)
        self.out3[1, slot, at] = (self.side[1, side, at] + self.in2[1, arrived, at, self.right].astype(F32)).astype(BF16)
        for one in self.copies3(p, rows):
            one.start()
        self.own[own, at, self.left] += self.in2[1, arrived, at, self.left].astype(F32)
        self.own[own, at, self.right] += self.in2[0, arrived, at, self.right].astype(F32)

    def stage4(self, p, rows, keep):
        for one in self.copies3(p, rows):
            one.wait()
        arrived, own = lax.rem(p, self.in3.shape[1]), lax.rem(p, self.own.shape[0])
        at = slice(0, rows)
        a = self.own[own, at, self.left] + self.in3[0, arrived, at].astype(F32)
        b = self.own[own, at, self.right] + self.in3[1, arrived, at].astype(F32)
        keep(p, a.astype(BF16), b.astype(BF16))

    def move(self, step, low, high):
        for lag, stage in zip(self.lags, (self.stage1, self.stage2, self.stage3, self.stage4), strict=True):
            for first, end, rows, keep in self.kinds:
                if high - 1 - lag < first or low - lag >= end:
                    continue
                p = step - lag
                if low - lag >= first and high - 1 - lag < end:
                    stage(p, rows, keep)
                else:
                    pl.when((p >= first) & (p < end))(functools.partial(stage, p, rows, keep))


def add_squares(total, *blocks):
    for block in blocks:
        wide = block.astype(F32)
        wide = wide * wide
        rows, columns = wide.shape
        sums = [wide[r : r + 8, c : c + 128] for r in range(0, rows, 8) for c in range(0, columns, 128)]
        while len(sums) > 1:
            sums = [a + b for a, b in zip(sums[::2], sums[1::2])] + ([sums[-1]] if len(sums) % 2 else [])
        total[...] += sums[0]


def keep_columns(first, gate, up, width, squares):
    def keep(p, left, right):
        columns = pl.ds(pl.multiple_of((p - first) * width, width), width)
        gate[:, columns] = left
        up[:, columns] = right
        add_squares(squares, left, right)

    return keep


def keep_down(first, down, rows, width, squares):
    def keep(p, left, right):
        half = width // 2
        which = p - first
        at = pl.ds(pl.multiple_of(lax.rem(which, 2) * rows, 16), rows)
        start = lax.div(which, 2) * width
        down[at, pl.ds(pl.multiple_of(start, half), half)] = left
        down[at, pl.ds(pl.multiple_of(start + half, half), half)] = right
        add_squares(squares, left, right)

    return keep


def down_packet(exchange, step, first, hidden_t, by_out):
    n_rows = hidden_t.shape[0]
    _, chips, cores, rows, width = exchange.mine.shape
    which = step - first
    start = pl.multiple_of(lax.rem(which, 2) * rows, 16)
    columns = pl.ds(pl.multiple_of(lax.div(which, 2) * width, width), width)
    share = n_rows // (chips * cores)
    by_out = by_out[:, columns]
    for k in range(chips * cores):
        lhs = hidden_t[pl.ds(pl.multiple_of(k * share + start, 16), rows), :]
        exchange.mine[exchange.held(step), k // cores, k % cores] = dot(lhs, by_out).astype(BF16)


def wide_packet(exchange, step, a_t, by_both):
    _, chips, cores, _, width = exchange.mine.shape
    rows = a_t.shape[0] // (chips * cores)
    half = width // 2
    for k in range(2):
        columns = slice(k * half, k * half + half)
        block = dot(a_t[...], by_both[:, columns]).astype(BF16)
        exchange.mine[exchange.held(step), :, :, pl.ds(0, rows), columns] = block.reshape(chips, cores, rows, half)


MB = 512
TOP_LAGS = (0, 1, 3, 5)
BOTTOM_LAGS = (0, 1, 3, 5)


def top_kernel(n, *refs):
    (a_in, at_in, h_in, dy_in, w_gate, w_up, w_down), refs = refs[:7], refs[7:]
    (g_gate, g_up, g_down, squares, by_h, bg_hbm, bu_hbm), refs = refs[:7], refs[7:]
    (a, a_t, dy, wg, wu, hidden_t, wd, both, h_tile, by_tile, load_sem, wd_sem, both_sem, tile_sem, by_sem), refs = refs[:15], refs[15:]
    tokens, d = a.shape
    ff = wg.shape[1]
    width = 256
    chunks = ff // width
    downs = 4
    wide_rows, down_rows = d // n, ff // n // 2
    exchange = Exchange(
        n, refs,
        (
            (0, chunks, wide_rows, keep_columns(0, g_gate, g_up, width, squares)),
            (chunks, chunks + downs, down_rows, keep_down(chunks, g_down, down_rows, 2 * width, squares)),
        ),
        TOP_LAGS,
    )
    layer = w_gate.shape[0] - 1
    first, rest = pl.ds(0, width), pl.ds(width, ff - width)
    loads = [
        pltpu.make_async_copy(a_in, a, load_sem.at[0]),
        pltpu.make_async_copy(w_gate.at[layer, :, first], wg.at[:, first], load_sem.at[1]),
        pltpu.make_async_copy(w_up.at[layer, :, first], wu.at[:, first], load_sem.at[2]),
        pltpu.make_async_copy(dy_in, dy, load_sem.at[3]),
        pltpu.make_async_copy(at_in, a_t, load_sem.at[4]),
        pltpu.make_async_copy(w_gate.at[layer, :, rest], wg.at[:, rest], load_sem.at[5]),
        pltpu.make_async_copy(w_up.at[layer, :, rest], wu.at[:, rest], load_sem.at[6]),
    ]

    def down_chunk(c):
        slot = lax.rem(c, 2)
        return pltpu.make_async_copy(w_down.at[layer, pl.ds(pl.multiple_of(c * width, width), width)], wd.at[slot], wd_sem.at[slot])

    for one in loads[:5]:
        one.start()
    down_chunk(0).start()
    squares[...] = jnp.zeros_like(squares)
    exchange.barrier()

    def store_both(c, k):
        slot = lax.rem(c, 2)
        return pltpu.make_async_copy(
            both.at[slot, :, pl.ds(k * width, width)],
            (bg_hbm, bu_hbm)[k].at[:, pl.ds(pl.multiple_of(c * width, width), width)],
            both_sem.at[k, slot],
        )

    def chunk(c, _):
        slot = lax.rem(c, 2)

        @pl.when(c == 0)
        def _():
            for one in loads[:5]:
                one.wait()
            for one in loads[5:]:
                one.start()

        @pl.when(c == 1)
        def _():
            for one in loads[5:]:
                one.wait()

        @pl.when(c >= 2)
        def _():
            for k in range(2):
                store_both(c - 2, k).wait()

        down_chunk(c).wait()

        @pl.when(c + 1 < chunks)
        def _():
            down_chunk(c + 1).start()

        columns = pl.ds(pl.multiple_of(c * width, width), width)
        wg_c, wu_c, wd_c = wg[:, columns], wu[:, columns], wd[slot]
        for at in range(0, tokens, MB):
            rows = slice(at, at + MB)
            hidden, by_gate, by_up = by_units(dot(a[rows], wg_c), dot(a[rows], wu_c), dot(dy[rows], wd_c, ((1,), (1,))))
            hidden_t[columns, rows] = hidden.astype(BF16).T
            both[slot, rows, :width] = by_gate.astype(BF16)
            both[slot, rows, width:] = by_up.astype(BF16)
        wide_packet(exchange, c, a_t, both.at[slot])
        for k in range(2):
            store_both(c, k).start()
        exchange.move(c, 0, chunks)
        return 0

    lax.fori_loop(0, chunks, chunk, 0)
    for c in (chunks - 2, chunks - 1):
        for k in range(2):
            store_both(c, k).wait()

    tile_rows = 256
    tiles = tokens // tile_rows
    split = a_t.shape[1]

    def tile_loads(t):
        slot = lax.rem(t, 2)
        rows = pl.ds(pl.multiple_of(t * tile_rows, tile_rows), tile_rows)
        got = []
        for k, src in enumerate((bg_hbm, bu_hbm)):
            to = pl.ds(pl.multiple_of((slot * 2 + k) * tile_rows, tile_rows), tile_rows)
            got.append(pltpu.make_async_copy(src.at[rows, pl.ds(0, split)], a_t.at[to], tile_sem.at[2 * k, slot]))
            got.append(pltpu.make_async_copy(src.at[rows, pl.ds(split, ff - split)], a.at[to, pl.ds(0, ff - split)], tile_sem.at[2 * k + 1, slot]))
        got.append(pltpu.make_async_copy(h_in.at[rows], h_tile.at[slot], tile_sem.at[4, slot]))
        return got

    def tile_store(t):
        slot = lax.rem(t, 2)
        return pltpu.make_async_copy(by_tile.at[slot], by_h.at[pl.ds(pl.multiple_of(t * tile_rows, tile_rows), tile_rows)], by_sem.at[slot])

    for one in tile_loads(0):
        one.start()

    def tile(step, _):
        t = step - chunks

        @pl.when(t < downs)
        def _():
            down_packet(exchange, step, chunks, hidden_t, dy)

        exchange.move(step, chunks, chunks + tiles)
        slot = lax.rem(t, 2)
        for one in tile_loads(t):
            one.wait()

        @pl.when(t + 1 < tiles)
        def _():
            for one in tile_loads(t + 1):
                one.start()

        @pl.when(t >= 2)
        def _():
            tile_store(t - 2).wait()

        total = None
        for k, w in enumerate((wg, wu)):
            at = pl.ds(pl.multiple_of((slot * 2 + k) * tile_rows, tile_rows), tile_rows)
            term = dot(a_t[at], w[:, :split], ((1,), (1,))) + dot(a[at, : ff - split], w[:, split:], ((1,), (1,)))
            total = term if total is None else total + term
        rows = pl.ds(pl.multiple_of(t * tile_rows, tile_rows), tile_rows)
        by_tile[slot] = (dy[rows].astype(F32) + by_norm(h_tile[slot], total)).astype(BF16)
        tile_store(t).start()
        return 0

    lax.fori_loop(chunks, chunks + tiles, tile, 0)
    for step in range(chunks + tiles, chunks + downs + TOP_LAGS[-1]):
        exchange.move(step, step, step + 1)
    for t in (tiles - 2, tiles - 1):
        tile_store(t).wait()


def top_layer(n, a, a_t, h, dy, w_gate, w_up, w_down):
    tokens, d = a.shape
    ff = w_gate.shape[2]
    width = 256
    anywhere, inside = pl.BlockSpec(memory_space=pl.ANY), pl.BlockSpec(memory_space=pltpu.VMEM)
    dma = pltpu.SemaphoreType.DMA
    return pl.pallas_call(
        functools.partial(top_kernel, n),
        in_specs=[anywhere] * 7,
        out_specs=[inside] * 4 + [anywhere] * 3,
        out_shape=[
            jax.ShapeDtypeStruct((d // n, ff), BF16),
            jax.ShapeDtypeStruct((d // n, ff), BF16),
            jax.ShapeDtypeStruct((ff // n, d), BF16),
            jax.ShapeDtypeStruct((8, 128), F32),
            jax.ShapeDtypeStruct((tokens, d), BF16),
            jax.ShapeDtypeStruct((tokens, ff), BF16),
            jax.ShapeDtypeStruct((tokens, ff), BF16),
        ],
        scratch_shapes=[
            pltpu.VMEM((tokens, d), BF16), pltpu.VMEM((d, tokens), BF16), pltpu.VMEM((tokens, d), BF16),
            pltpu.VMEM((d, ff), BF16), pltpu.VMEM((d, ff), BF16), pltpu.VMEM((ff, tokens), BF16),
            pltpu.VMEM((2, width, d), BF16), pltpu.VMEM((2, tokens, 2 * width), BF16),
            pltpu.VMEM((2, 256, d), BF16), pltpu.VMEM((2, 256, d), BF16),
            dma((7,)), dma((2,)), dma((2, 2)), dma((5, 2)), dma((2,)),
            *Exchange.scratch(n, ff // n // 2, 2 * width, TOP_LAGS),
        ],
        compiler_params=pltpu.CompilerParams(collective_id=2, has_side_effects=True, vmem_limit_bytes=67043328),
        name="top",
    )(a, a_t, h, dy, w_gate, w_up, w_down)


def bottom_kernel(n, *refs):
    (by_in, ht_in, at_in, gate_in, up_in, w_down), refs = refs[:6], refs[6:]
    (g_gate, g_up, g_down, squares), refs = refs[:4], refs[4:]
    (by, hidden_t, a_t, wd, gate, up, both, load_sem, wd_sem, unit_sem), refs = refs[:10], refs[10:]
    tokens, d = by.shape
    ff = hidden_t.shape[0]
    width = 256
    chunks = ff // width
    downs = 4
    wide_rows, down_rows = d // n, ff // n // 2
    exchange = Exchange(
        n, refs,
        (
            (0, downs, down_rows, keep_down(0, g_down, down_rows, 2 * width, squares)),
            (downs, downs + chunks, wide_rows, keep_columns(downs, g_gate, g_up, width, squares)),
        ),
        BOTTOM_LAGS,
    )
    share = ff // n
    halves = lambda ref, k: ref.at[:, pl.ds(k * 2 * width, 2 * width)]
    loads = [pltpu.make_async_copy(halves(by_in, 0), halves(by, 0), load_sem.at[0])]
    for k in range(2):
        for to in range(n):
            rows = pl.ds(to * share + k * down_rows, down_rows)
            loads.append(pltpu.make_async_copy(ht_in.at[rows], hidden_t.at[rows], load_sem.at[3 + k * n + to]))
    loads.append(pltpu.make_async_copy(halves(by_in, 1), halves(by, 1), load_sem.at[1]))
    loads.append(pltpu.make_async_copy(at_in, a_t, load_sem.at[2]))

    def chunk_loads(c):
        slot = lax.rem(c, 2)
        columns = pl.ds(pl.multiple_of(c * width, width), width)
        return [
            pltpu.make_async_copy(w_down.at[0, columns], wd.at[slot], wd_sem.at[slot]),
            pltpu.make_async_copy(gate_in.at[:, columns], gate.at[slot], unit_sem.at[0, slot]),
            pltpu.make_async_copy(up_in.at[:, columns], up.at[slot], unit_sem.at[1, slot]),
        ]

    first, second, third = loads[: 1 + n], loads[1 + n : 1 + 2 * n], (*loads[1 + 2 * n :], *chunk_loads(0))
    for one in first:
        one.start()
    squares[...] = jnp.zeros_like(squares)
    exchange.barrier()

    def down(step, _):
        @pl.when(step == 0)
        def _():
            for one in first:
                one.wait()
            for one in second:
                one.start()

        @pl.when(step == 1)
        def _():
            for one in second:
                one.wait()
            for one in third:
                one.start()

        @pl.when(step == 2)
        def _():
            for one in third[:2]:
                one.wait()

        down_packet(exchange, step, 0, hidden_t, by)
        exchange.move(step, 0, downs)
        return 0

    lax.fori_loop(0, downs, down, 0)

    def chunk(step, _):
        c = step - downs
        slot = lax.rem(c, 2)
        for one in chunk_loads(c):
            one.wait()

        @pl.when(c + 1 < chunks)
        def _():
            for one in chunk_loads(c + 1):
                one.start()

        wd_c = wd[slot]
        for at in range(0, tokens, MB):
            rows = slice(at, at + MB)
            _, by_gate, by_up = by_units(gate[slot, rows], up[slot, rows], dot(by[rows], wd_c, ((1,), (1,))))
            both[rows, :width] = by_gate.astype(BF16)
            both[rows, width:] = by_up.astype(BF16)
        wide_packet(exchange, step, a_t, both)
        exchange.move(step, downs, downs + chunks)
        return 0

    lax.fori_loop(downs, downs + chunks, chunk, 0)
    for step in range(downs + chunks, downs + chunks + BOTTOM_LAGS[-1]):
        exchange.move(step, step, step + 1)


def bottom_layer(n, by, hidden_t, a_t, gate, up, w_down):
    tokens, d = by.shape
    ff = hidden_t.shape[0]
    width = 256
    anywhere, inside = pl.BlockSpec(memory_space=pl.ANY), pl.BlockSpec(memory_space=pltpu.VMEM)
    dma = pltpu.SemaphoreType.DMA
    return pl.pallas_call(
        functools.partial(bottom_kernel, n),
        in_specs=[anywhere] * 6,
        out_specs=[inside] * 4,
        out_shape=[
            jax.ShapeDtypeStruct((d // n, ff), BF16),
            jax.ShapeDtypeStruct((d // n, ff), BF16),
            jax.ShapeDtypeStruct((ff // n, d), BF16),
            jax.ShapeDtypeStruct((8, 128), F32),
        ],
        scratch_shapes=[
            pltpu.VMEM((tokens, d), BF16), pltpu.VMEM((ff, tokens), BF16), pltpu.VMEM((d, tokens), BF16),
            pltpu.VMEM((2, width, d), BF16), pltpu.VMEM((2, tokens, width), F32), pltpu.VMEM((2, tokens, width), F32),
            pltpu.VMEM((tokens, 2 * width), BF16),
            dma((3 + 2 * n,)), dma((2,)), dma((2, 2)),
            *Exchange.scratch(n, ff // n // 2, 2 * width, BOTTOM_LAGS),
        ],
        compiler_params=pltpu.CompilerParams(collective_id=3, has_side_effects=True, vmem_limit_bytes=67043328),
        name="bottom",
    )(by, hidden_t, a_t, gate, up, w_down)


def solution(mesh):
    n = mesh.shape["dp"]

    def step(x, dy, w_gate, w_up, w_down, *moments):
        gate, up, hidden_t, a_t, h, next_a, next_a_t = layer_0(x[0], w_gate, w_up, w_down)
        *top, squares_1, by_h, _, _ = top_layer(n, next_a, next_a_t, h, dy[0], w_gate, w_up, w_down)
        *bottom, squares_0 = bottom_layer(n, by_h, hidden_t, a_t, gate, up, w_down)
        gradients = list(zip(bottom, top, strict=True))
        return tuple(finish(n, gradients, (squares_0, squares_1), (w_gate, w_up, w_down), moments[:3], moments[3:]))

    sharded = P(None, "dp", None)
    return jax.shard_map(
        step,
        mesh=mesh,
        in_specs=(P(("rep", "dp")), P(("rep", "dp")), P(), P(), P(), *[sharded] * 6),
        out_specs=(*[P("rep")] * 3, *[P("rep", "dp")] * 6),
        check_vma=False,
    )
```

```python
import functools

import jax
import jax.numpy as jnp
from jax import lax
from jax.experimental import pallas as pl
from jax.experimental.pallas import tpu as pltpu
from jax.sharding import PartitionSpec as P

MESH = pl.DeviceIdType.MESH
F32, BF16 = jnp.float32, jnp.bfloat16
CORES = 2
BUFFERS = 2
WEIGHTS = 3
MIB = 2**20
ALL_VMEM = 67043328
TRANSPOSED = ((1,), (1,))


def turn(t):
    return lax.rem(t, BUFFERS)


def repeat(low, high, body):
    def step(i, nothing):
        body(i)
        return nothing

    lax.fori_loop(low, high, step, None)


def split(refs, *sizes):
    left = iter(refs)
    runs = [[next(left) for _ in range(size)] for size in sizes]
    return *runs, list(left)


def local_copies(pairs, sem, *at):
    return [pltpu.make_async_copy(src, dst, sem.at[(k, *at)]) for k, (src, dst) in enumerate(pairs)]


def places(axis, n):
    me = lax.axis_index(axis)
    chips = n // CORES
    core, chip = lax.rem(me, CORES), lax.div(me, CORES)
    at = lambda away: lax.rem(chip + away, chips) * CORES + core
    return me, core, me + 1 - 2 * core, at(1), at(chips - 1), at(2)


class Spread:
    KINDS = 9

    def __init__(self, n, send, recv):
        self.send, self.recv = send, recv
        self.me, _, self.partner, self.after, self.before, self.across = places("dp", n)

    @staticmethod
    def semaphores(pieces):
        return [pltpu.SemaphoreType.DMA((Spread.KINDS, pieces))] * 2

    def barrier(self):
        barrier = pltpu.get_barrier_semaphore()
        for peer in (self.partner, self.after, self.before):
            pl.semaphore_signal(barrier, inc=1, device_id={"dp": peer}, device_id_type=MESH)
        pl.semaphore_wait(barrier, 3)

    def copies(self, number, place, width, own=None, far=None):
        far = far or place
        every, left, right = pl.ds(0, width), pl.ds(0, width // 2), pl.ds(width // 2, width // 2)

        class Copies(dict):
            def __missing__(_, kind):
                to, src, dst = routes[kind]
                sems = (t.at[list(routes).index(kind), number] for t in (self.send, self.recv))
                return pltpu.make_async_remote_copy(src, dst, *sems, device_id={"dp": to}, device_id_type=MESH)

        me, after, before, across = self.me, self.after, self.before, self.across
        own = place(me, every) if own is None else own
        routes = {
            "after": (after, own, place(me, every)),
            "before": (before, own, place(me, every)),
            "partner": (self.partner, own, place(me, every)),
            "on": (after, place(before, left), far(before, left)),
            "back": (before, place(after, right), far(after, right)),
            "partner_before": (self.partner, place(before, every), far(before, every)),
            "partner_after": (self.partner, place(after, every), far(after, every)),
            "partner_left": (self.partner, far(across, left), far(across, left)),
            "partner_right": (self.partner, far(across, right), far(across, right)),
        }
        return Copies()

    @staticmethod
    def start(copies):
        for kind in ("after", "before", "partner"):
            copies[kind].start()

    @staticmethod
    def pass_on(copies):
        copies["after"].wait_recv()
        copies["on"].start()
        copies["partner_before"].start()
        copies["before"].wait_recv()
        copies["back"].start()
        copies["partner_after"].start()

    @staticmethod
    def pass_last(copies):
        copies["on"].wait_recv()
        copies["partner_left"].start()
        copies["back"].wait_recv()
        copies["partner_right"].start()

    @staticmethod
    def end(copies):
        for kind in ("partner", "partner_before", "partner_after", "partner_left", "partner_right"):
            copies[kind].wait_recv()
        for kind in (*Spread.NEAR, *Spread.THEN, *Spread.LAST):
            copies[kind].wait_send()


    NEAR, THEN, LAST = ("after", "before", "partner"), ("on", "back", "partner_before", "partner_after"), ("partner_left", "partner_right")

    @staticmethod
    def end_near(copies):
        for kind in Spread.NEAR:
            copies[kind].wait()

    @staticmethod
    def start_far(copies):
        for kind in Spread.THEN:
            copies[kind].start()

    @staticmethod
    def end_far(copies):
        for kind in Spread.THEN:
            copies[kind].wait_send()
        for kind in (*Spread.THEN[2:], *Spread.LAST):
            copies[kind].wait_recv()
        for kind in Spread.LAST:
            copies[kind].wait_send()


EARLY = ((0, 32), (1, 32))


def finish_kernel(n, count, layers, pieces, *refs):
    some = len(EARLY)
    squares, *g_in = zip(*[iter(refs[: layers + layers * WEIGHTS])] * layers)
    refs = refs[layers + layers * WEIGHTS :]
    w_in, m_in, v_in, near_m, near_v, far_m, far_v, near_g, w, m, v, far_g, g, refs = split(
        refs, *[WEIGHTS] * 3, *[some] * 5, *[WEIGHTS] * 3, some, WEIGHTS
    )
    parts, m_tile, v_tile, g_tile, load_sem, early_sem, tile_sem, part_send, part_recv, send, recv = refs
    spread = Spread(n, send, recv)
    me = spread.me

    barrier = pltpu.get_barrier_semaphore()
    peers = [lax.rem(me + away, n) for away in range(1, n)]
    for peer in peers:
        pl.semaphore_signal(barrier, inc=1, device_id={"dp": peer}, device_id_type=MESH)

    def rows_of(i, owner, first, rows):
        return pl.ds(pl.multiple_of(owner * g[i].shape[1] + first, 16), rows)

    order = (2, 0, 1)
    loads = {}
    for i in order:
        rows = rows_of(i, me, 0, g[i].shape[1])
        pairs = [(w_in[i].at[:, rows], w[i].at[:, rows]), (m_in[i], m[i]), (v_in[i], v[i])]
        pairs += [(g_in[i][k], g[i].at[k]) for k in range(layers)]
        loads[i] = [pltpu.make_async_copy(src, dst, load_sem.at[i, k]) for k, (src, dst) in enumerate(pairs)]
    first_weight, *other_weights = order
    for one in loads[first_weight]:
        one.start()

    total = sum(t[...] for t in squares)
    parts[pl.ds(me, 1)] = total[None]
    early = []
    for k, (i, some) in enumerate(EARLY):
        near = lambda owner, columns, ref=near_g[k]: ref.at[owner, :, columns]
        far = lambda owner, columns, ref=far_g[k]: ref.at[owner, :, columns]
        early.append(spread.copies(len(pieces) + k, near, g[i].shape[2], None, far))
    pl.semaphore_wait(barrier, n - 1)
    part_copies = []
    for k, peer in enumerate(peers):
        part_copies.append(
            pltpu.make_async_remote_copy(
                parts.at[me], parts.at[me], part_send.at[k], part_recv.at[k], device_id={"dp": peer}, device_id_type=MESH
            )
        )
        part_copies[-1].start()
    for copies in early:
        spread.start_far(copies)
    for one in part_copies:
        one.wait_recv()
    every = parts[0]
    for k in range(1, n):
        every += parts[k]
    mean = jnp.sum(every, keepdims=True) / count
    factor = jnp.minimum(1.0, 0.5 * lax.rsqrt(mean + 1e-30))

    def stepped(grad, m_old, v_old, w_old):
        grad = grad.astype(F32) * factor
        m_new = 0.9 * m_old + 0.1 * grad
        v_new = 0.95 * v_old + 0.05 * grad * grad
        w_old = w_old.astype(F32)
        return m_new, v_new, (w_old - 0.02 * (m_new * lax.rsqrt(v_new + 1e-8) + 0.1 * w_old)).astype(BF16)

    step_rows, width = 16, 256

    def adamw(i, layer, first, rows):
        def body(step):
            start = first + step * step_rows
            at = (layer, pl.ds(pl.multiple_of(start, 16), step_rows), slice(None))
            mine = (layer, rows_of(i, me, start, step_rows), slice(None))
            m[i][at], v[i][at], w[i][mine] = stepped(g[i][at], m[i][at], v[i][at], w[i][mine])

        repeat(0, rows // step_rows, body)

    waited = set()

    def compute(i, layer, first, rows):
        if i not in waited:
            waited.add(i)
            for one in loads[i]:
                one.wait()
        adamw(i, layer, first, rows)

    made = []
    for number, (i, layer, first, rows) in enumerate(pieces):
        place = lambda owner, columns, i=i, layer=layer, first=first, rows=rows: w[i].at[layer, rows_of(i, owner, first, rows), columns]
        made.append(spread.copies(number, place, g[i].shape[2]))

    def own_piece(number):
        compute(*pieces[number])
        spread.start(made[number])

    other = lambda device: device + spread.partner - me
    units = []
    for k, (i, some) in enumerate(EARLY):
        near, far = (near_m[k], near_v[k], near_g[k]), (far_m[k], far_v[k], far_g[k])
        for refs, owners in (
            (near, (spread.partner, spread.after, spread.before)),
            (far, (other(spread.after), other(spread.before), spread.across, other(spread.across))),
        ):
            units += [(refs, i, owner, first, g[i].shape[1] - some) for owner in owners for first in range(0, some, step_rows)]

    def unit_loads(number):
        refs, _, owner, first, _ = units[number]
        slot = number % BUFFERS
        tiles = zip(refs, (m_tile, v_tile, g_tile), strict=True)
        return local_copies([(src.at[owner, pl.ds(first, step_rows)], dst.at[slot]) for src, dst in tiles], tile_sem, slot)

    def unit_rows(number):
        _, i, owner, first, start = units[number]
        return rows_of(i, owner, start + first, step_rows)

    last = layers - 1
    old_rows = local_copies(
        [tuple(t[i].at[last, unit_rows(number)] for t in (w_in, w)) for number, (_, i, _, _, _) in enumerate(units)], early_sem
    )

    def unit(number):
        (_, i, _, _, _), slot = units[number], number % BUFFERS
        if number + 1 < len(units):
            for one in unit_loads(number + 1):
                one.start()
        for one in (*unit_loads(number), old_rows[number]):
            one.wait()

        def body(step):
            columns = pl.ds(pl.multiple_of(step * width, width), width)
            its, at = (last, unit_rows(number), columns), (slot, slice(None), columns)
            *_, w[i][its] = stepped(g_tile[at], m_tile[at], v_tile[at], w[i][its])

        repeat(0, g[i].shape[-1] // width, body)

    own_piece(0)
    for i in other_weights:
        for one in loads[i]:
            one.start()
    for one in old_rows:
        one.start()
    total_pieces, done = len(pieces), 0
    for number in range(total_pieces + 2):
        if number + 1 < total_pieces:
            own_piece(number + 1)
        if number == 0:
            for copies in early:
                spread.pass_last(copies)
        if 1 <= number <= total_pieces:
            spread.pass_on(made[number - 1])
        if 2 <= number:
            spread.pass_last(made[number - 2])
        if number == 2:
            for copies in early:
                spread.end_far(copies)
            for one in unit_loads(0):
                one.start()
        if 3 <= number < total_pieces:
            for k in range(min(3, len(units) - done)):
                unit(done + k)
            done += min(3, len(units) - done)
    for k in range(done, len(units)):
        unit(k)
    for i, some in EARLY:
        compute(i, last, g[i].shape[1] - some, some)
    for copies in made:
        spread.end(copies)
    for one in part_copies:
        one.wait_send()


def store_kernel(*refs):
    *refs, sem = refs
    some = len(refs) // 2
    copies = local_copies([(refs[k], refs[some + k]) for k in range(some)], sem)
    for one in copies:
        one.start()
    for one in copies:
        one.wait()


def early_shapes(n, blocks, dtype, times=1):
    return [jax.ShapeDtypeStruct((n, some, blocks[i][0].shape[-1]), dtype) for _ in range(times) for i, some in EARLY]


def finish(n, gradients, squares, weights, m, v, early):
    count = float(sum(w.size for w in weights))
    layers = len(gradients[0])
    pieces = []
    for i in (2, 0, 1):
        rows, _ = gradients[i][0].shape
        for layer in range(layers):
            half = rows // 2
            cuts = [half, half]
            if (i, layer) == (2, 0):
                cuts = [48, half - 48, half]
            elif layer == layers - 1 and i in dict(EARLY):
                rest = half - dict(EARLY)[i]
                cuts = [half, rest - 16, 16] if i == 1 else [half, rest]
            for cut in cuts:
                pieces.append((i, layer, sum(p[3] for p in pieces if p[:2] == (i, layer)), cut))
    anywhere, inside = pl.BlockSpec(memory_space=pl.ANY), pl.BlockSpec(memory_space=pltpu.VMEM)
    dma = pltpu.SemaphoreType.DMA
    results = [*weights, *m, *v]
    tile = lambda dtype: pltpu.VMEM((BUFFERS, 16, max(gradients[i][0].shape[1] for i, _ in EARLY)), dtype)
    ready = pl.pallas_call(
        functools.partial(finish_kernel, n, count, layers, tuple(pieces)),
        out_shape=[pltpu.VMEM(t.shape, t.dtype) for t in results]
        + early_shapes(n, gradients, BF16),
        in_specs=[inside] * layers + [anywhere] * (WEIGHTS * layers + len(results) + len(early)),
        out_specs=[inside] * len(results) + [anywhere] * len(EARLY),
        scratch_shapes=[
            *[pltpu.VMEM((layers, *one[0].shape), BF16) for one in gradients],
            pltpu.VMEM((n, 8, 128), F32), tile(F32), tile(F32), tile(BF16),
            dma((WEIGHTS, layers + 3)), dma((sum(some for _, some in EARLY) // 16 * (n - 1),)), dma((3, BUFFERS)), *[dma((n - 1,))] * 2,
            *Spread.semaphores(len(pieces) + len(EARLY)),
        ],
        compiler_params=pltpu.CompilerParams(collective_id=4, has_side_effects=True, vmem_limit_bytes=8 * MIB),
        name="finish",
    )(*squares, *sum(gradients, ()), *weights, *m, *v, *early)[: len(results)]
    return pl.pallas_call(
        store_kernel,
        out_shape=[jax.ShapeDtypeStruct(t.shape, t.dtype) for t in results],
        in_specs=[inside] * len(results),
        out_specs=[anywhere] * len(results),
        scratch_shapes=[dma((len(results),))],
        compiler_params=pltpu.CompilerParams(vmem_limit_bytes=8 * MIB),
        name="store",
    )(*[pltpu.with_memory_space_constraint(t, pltpu.VMEM) for t in ready])


def dot(a, b, contract=((1,), (0,))):
    return lax.dot_general(a, b, (contract, ((), ())), preferred_element_type=F32)


def normed(h):
    wide = h.astype(F32)
    return (wide * lax.rsqrt(jnp.mean(wide * wide, -1, keepdims=True) + 1e-6)).astype(BF16)


def by_norm(h, by_a):
    wide = h.astype(F32)
    scale = lax.rsqrt(jnp.mean(wide * wide, -1, keepdims=True) + 1e-6)
    return scale * by_a - wide * (scale * scale * scale * jnp.mean(by_a * wide, -1, keepdims=True))


def by_units(gate, up, by_hidden):
    by_hidden = by_hidden.astype(BF16).astype(F32)
    s = jax.nn.sigmoid(gate)
    silu = gate * s
    return silu * up, by_hidden * up * (s + silu * (1.0 - s)), by_hidden * silu


def forward_kernel(n, *refs):
    (x_in, w_gate, w_up, w_down), moments, outs, early, refs = split(refs, 4, 2 * len(EARLY), 7, 2 * len(EARLY))
    gate_out, up_out, ht_out, at_out, h_out, b_out, bt_out = outs
    (wg, wu, wd, hidden, x, gate, up, hidden_t, a_t, h, b, b_t, w_sem, x_sem, sem, late_sem, send, recv) = refs
    spread = Spread(n, send, recv)
    rows = x.shape[1]
    tiles = x_in.shape[0] // rows
    ff = wg.shape[1]
    width = 256
    groups = [range(at, min(at + 3 * width, ff), width) for at in range(0, ff, 3 * width)]
    tall = lambda ref, t: ref.at[pl.ds(pl.multiple_of(t * rows, rows), rows)]
    wide = lambda ref, t: ref.at[:, pl.ds(pl.multiple_of(t * rows, rows), rows)]

    def load_x(t):
        return pltpu.make_async_copy(tall(x_in, t), x.at[lax.rem(t, x.shape[0])], x_sem.at[lax.rem(t, x.shape[0])])

    def stores(t, first):
        slot = turn(t)
        if first:
            pairs = [(gate, tall(gate_out, t)), (up, tall(up_out, t)), (hidden_t, wide(ht_out, t)), (a_t, wide(at_out, t))]
        else:
            pairs = [(h, tall(h_out, t)), (b, tall(b_out, t)), (b_t, wide(bt_out, t))]
        return local_copies([(src.at[slot], dst) for src, dst in pairs], sem if first else late_sem, slot)

    w_loads = []
    for k, group in enumerate(groups):
        columns = slice(group[0], group[-1] + width)
        w_loads.append([
            pltpu.make_async_copy(src.at[0, :, columns], dst.at[:, columns], w_sem.at[j, k]) for j, (src, dst) in enumerate(((w_gate, wg), (w_up, wu)))
        ])
    down_load = pltpu.make_async_copy(w_down.at[0], wd, w_sem.at[2, 0])
    for one in (load_x(0), *w_loads[0], *w_loads[1], load_x(1)):
        one.start()
    spread.barrier()
    pieces = []
    for number, (src, dst) in enumerate(zip(moments, early, strict=True)):
        some = dst.shape[1]
        own = src.at[src.shape[0] - 1, pl.ds(src.shape[1] - some, some)]
        pieces.append(spread.copies(number, lambda owner, columns, dst=dst: dst.at[owner, :, columns], dst.shape[2], own))
    for copies in pieces:
        spread.start(copies)

    def first_part(t, group, a):
        slot = turn(t)
        for at in group:
            columns = slice(at, at + width)
            g, u = dot(a, wg[:, columns]), dot(a, wu[:, columns])
            gate[slot, :, columns] = g
            up[slot, :, columns] = u
            units = (g * jax.nn.sigmoid(g) * u).astype(BF16)
            hidden[:, columns] = units
            hidden_t[slot, columns] = units.T

    def second_part(t):
        slot = turn(t)
        out = x[lax.rem(t, x.shape[0])] + dot(hidden[...], wd[...]).astype(BF16)
        h[slot] = out
        after = normed(out)
        b[slot] = after
        b_t[slot] = after.T

    def normed_tile(t):
        a = normed(x[lax.rem(t, x.shape[0])])
        a_t[turn(t)] = a.T
        return a

    load_x(0).wait()
    a = normed_tile(0)
    for k, group in enumerate(groups):
        for one in w_loads[k]:
            one.wait()
        for one in w_loads[k + 2] if k + 2 < len(groups) else ([down_load] if k + 2 == len(groups) else []):
            one.start()
        first_part(0, group, a)
    for one in stores(0, True):
        one.start()
    down_load.wait()

    def tile(t):
        load_x(t).wait()

        @pl.when(t + 1 < tiles)
        def _():
            load_x(t + 1).start()

        @pl.when(t >= BUFFERS)
        def _():
            for one in stores(t - BUFFERS, True):
                one.wait()

        @pl.when(t > BUFFERS)
        def _():
            for one in stores(t - 1 - BUFFERS, False):
                one.wait()

        a = normed_tile(t)
        second_part(t - 1)
        first_part(t, range(0, ff, width), a)
        for one in (*stores(t - 1, False), *stores(t, True)):
            one.start()

    repeat(1, tiles, tile)
    last = tiles - 1
    for one in stores(last - BUFFERS, False):
        one.wait()
    second_part(last)
    for one in stores(last, False):
        one.start()
    for copies in pieces:
        spread.end_near(copies)
    for t in (last - 1, last):
        for one in (*stores(t, True), *stores(t, False)):
            one.wait()


def layer_0(n, x, w_gate, w_up, w_down, m, v):
    tokens, d = x.shape
    ff = w_gate.shape[2]
    rows = 256
    anywhere = pl.BlockSpec(memory_space=pl.ANY)
    dma = pltpu.SemaphoreType.DMA
    vmem = lambda *shape: pltpu.VMEM(shape, BF16)
    return pl.pallas_call(
        functools.partial(forward_kernel, n),
        in_specs=[anywhere] * (4 + 2 * len(EARLY)),
        out_specs=[anywhere] * (7 + 2 * len(EARLY)),
        out_shape=[
            jax.ShapeDtypeStruct((tokens, ff), F32),
            jax.ShapeDtypeStruct((tokens, ff), F32),
            jax.ShapeDtypeStruct((ff, tokens), BF16),
            jax.ShapeDtypeStruct((d, tokens), BF16),
            jax.ShapeDtypeStruct((tokens, d), BF16),
            jax.ShapeDtypeStruct((tokens, d), BF16),
            jax.ShapeDtypeStruct((d, tokens), BF16),
            *early_shapes(n, m, F32, 2),
        ],
        scratch_shapes=[
            vmem(d, ff), vmem(d, ff), vmem(ff, d), vmem(rows, ff), vmem(3, rows, d),
            *[pltpu.VMEM((BUFFERS, rows, ff), F32)] * 2, *[vmem(BUFFERS, *t) for t in ((ff, rows), (d, rows), (rows, d), (rows, d), (d, rows))],
            dma((WEIGHTS, 4)), dma((3,)), dma((4, BUFFERS)), dma((3, BUFFERS)), *Spread.semaphores(2 * len(EARLY)),
        ],
        compiler_params=pltpu.CompilerParams(collective_id=1, has_side_effects=True, vmem_limit_bytes=60 * MIB),
        name="forward",
    )(x, w_gate, w_up, w_down, *[t[i] for t in (m, v) for i, _ in EARLY])


class Exchange:
    def __init__(self, n, refs, kinds, lags):
        self.mine, self.pair, self.out2, self.out3, self.in2, self.in3, self.own, self.side, self.pair_sem, self.sem2, self.sem3 = refs
        self.kinds = kinds
        self.lags = lags
        self.me, self.core, self.partner, self.after, self.before, _ = places("dp", n)
        chips = n // CORES
        self.chip = lax.div(self.me, CORES)
        self.chip_after, self.chip_before, self.chip_across = (lax.rem(self.chip + k, chips) for k in (1, chips - 1, chips // 2))
        half = self.out3.shape[-1]
        self.left, self.right = slice(0, half), slice(half, 2 * half)

    @staticmethod
    def scratch(n, rows, width, lags):
        chips, half, dma = n // CORES, width // 2, pltpu.SemaphoreType.DMA
        _, two, three, four = lags
        slots1, slots2, slots3 = two + 3, 2 * (three - two) + 2, 2 * (four - three) + 2
        return [
            pltpu.VMEM((two + 1, chips, CORES, rows, width), BF16),
            pltpu.VMEM((slots1, chips, rows, width), BF16),
            pltpu.VMEM((2, three - two + 1, rows, width), BF16),
            pltpu.VMEM((2, four - three + 1, rows, half), BF16),
            pltpu.VMEM((2, slots2, rows, width), BF16),
            pltpu.VMEM((2, slots3, rows, half), BF16),
            pltpu.VMEM((four - two + 1, rows, width), F32),
            pltpu.VMEM((2, three - two + 1, rows, half), F32),
            dma((2, slots1)), dma((2, 2, slots2)), dma((2, 2, slots3)),
        ]

    def held(self, p):
        return lax.rem(p, self.mine.shape[0])

    def barrier(self):
        barrier = pltpu.get_barrier_semaphore()
        for peer in (self.partner, self.after, self.before):
            pl.semaphore_signal(barrier, inc=1, device_id={"dp": peer}, device_id_type=MESH)
        pl.semaphore_wait(barrier, 3)

    def copy1(self, p, rows):
        slot = lax.rem(p, self.pair.shape[0])
        return pltpu.make_async_remote_copy(
            self.mine.at[self.held(p), :, 1 - self.core, pl.ds(0, rows)], self.pair.at[slot, :, pl.ds(0, rows)],
            self.pair_sem.at[0, slot], self.pair_sem.at[1, slot], device_id={"dp": self.partner}, device_id_type=MESH,
        )

    def copies(self, p, rows, out, into, sem):
        slot = lax.rem(p, into.shape[1])
        return [
            pltpu.make_async_remote_copy(
                out.at[way, lax.rem(p, out.shape[1]), pl.ds(0, rows)], into.at[way, slot, pl.ds(0, rows)],
                sem.at[0, way, slot], sem.at[1, way, slot], device_id={"dp": to}, device_id_type=MESH,
            )
            for way, to in enumerate((self.after, self.before))
        ]

    def copies2(self, p, rows):
        return self.copies(p, rows, self.out2, self.in2, self.sem2)

    def copies3(self, p, rows):
        return self.copies(p, rows, self.out3, self.in3, self.sem3)

    def stage1(self, p, rows, _):
        self.copy1(p, rows).start()

    def stage2(self, p, rows, _):
        self.copy1(p, rows).wait()
        slot, own, side = (lax.rem(p, t.shape[k]) for t, k in ((self.out2, 1), (self.own, 0), (self.side, 1)))
        at = slice(0, rows)

        def of_chip(chip, columns):
            a = self.mine[self.held(p), chip, self.core, at, columns].astype(F32)
            return a + self.pair[lax.rem(p, self.pair.shape[0]), chip, at, columns].astype(F32)

        self.out2[0, slot, at, self.left] = of_chip(self.chip_across, self.left).astype(BF16)
        self.out2[0, slot, at, self.right] = of_chip(self.chip_after, self.right).astype(BF16)
        self.out2[1, slot, at, self.left] = of_chip(self.chip_before, self.left).astype(BF16)
        self.out2[1, slot, at, self.right] = of_chip(self.chip_across, self.right).astype(BF16)
        for one in self.copies2(p, rows):
            one.start()
        self.side[0, side, at] = of_chip(self.chip_after, self.left)
        self.side[1, side, at] = of_chip(self.chip_before, self.right)
        for columns in (self.left, self.right):
            self.own[own, at, columns] = of_chip(self.chip, columns)

    def stage3(self, p, rows, _):
        for one in self.copies2(p, rows):
            one.wait()
        slot, arrived, own, side = (lax.rem(p, t.shape[k]) for t, k in ((self.out3, 1), (self.in2, 1), (self.own, 0), (self.side, 1)))
        at = slice(0, rows)
        self.out3[0, slot, at] = (self.side[0, side, at] + self.in2[0, arrived, at, self.left].astype(F32)).astype(BF16)
        self.out3[1, slot, at] = (self.side[1, side, at] + self.in2[1, arrived, at, self.right].astype(F32)).astype(BF16)
        for one in self.copies3(p, rows):
            one.start()
        self.own[own, at, self.left] += self.in2[1, arrived, at, self.left].astype(F32)
        self.own[own, at, self.right] += self.in2[0, arrived, at, self.right].astype(F32)

    def stage4(self, p, rows, keep):
        for one in self.copies3(p, rows):
            one.wait()
        arrived, own = lax.rem(p, self.in3.shape[1]), lax.rem(p, self.own.shape[0])
        at = slice(0, rows)
        a = self.own[own, at, self.left] + self.in3[0, arrived, at].astype(F32)
        b = self.own[own, at, self.right] + self.in3[1, arrived, at].astype(F32)
        keep(p, a.astype(BF16), b.astype(BF16))

    def finish(self, step, packets):
        for step in range(step, packets + self.lags[-1]):
            self.move(step, step, step + 1)

    def move(self, step, low, high):
        for lag, stage in zip(self.lags, (self.stage1, self.stage2, self.stage3, self.stage4), strict=True):
            for first, end, rows, keep in self.kinds:
                if high - 1 - lag < first or low - lag >= end:
                    continue
                p = step - lag
                if low - lag >= first and high - 1 - lag < end:
                    stage(p, rows, keep)
                else:
                    pl.when((p >= first) & (p < end))(functools.partial(stage, p, rows, keep))


def add_squares(total, *blocks):
    for block in blocks:
        wide = block.astype(F32)
        wide = wide * wide
        rows, columns = wide.shape
        sums = [wide[r : r + 8, c : c + 128] for r in range(0, rows, 8) for c in range(0, columns, 128)]
        while len(sums) > 1:
            sums = [a + b for a, b in zip(sums[::2], sums[1::2])] + ([sums[-1]] if len(sums) % 2 else [])
        total[...] += sums[0]


def keep_columns(first, gate, up, width, squares):
    def keep(p, left, right):
        columns = pl.ds(pl.multiple_of((p - first) * width, width), width)
        gate[:, columns] = left
        up[:, columns] = right
        add_squares(squares, left, right)

    return keep


def keep_down(first, down, rows, width, squares):
    def keep(p, left, right):
        half = width // 2
        which = p - first
        at = pl.ds(pl.multiple_of(lax.rem(which, 2) * rows, 16), rows)
        start = lax.div(which, 2) * width
        down[at, pl.ds(pl.multiple_of(start, half), half)] = left
        down[at, pl.ds(pl.multiple_of(start + half, half), half)] = right
        add_squares(squares, left, right)

    return keep


def down_packet(exchange, step, first, hidden_t, by_out):
    n_rows = hidden_t.shape[0]
    _, chips, cores, rows, width = exchange.mine.shape
    which = step - first
    start = pl.multiple_of(lax.rem(which, 2) * rows, 16)
    columns = pl.ds(pl.multiple_of(lax.div(which, 2) * width, width), width)
    share = n_rows // (chips * cores)
    by_out = by_out[:, columns]
    for k in range(chips * cores):
        lhs = hidden_t[pl.ds(pl.multiple_of(k * share + start, 16), rows), :]
        exchange.mine[exchange.held(step), k // cores, k % cores] = dot(lhs, by_out).astype(BF16)


def wide_packet(exchange, step, a_t, by_both):
    _, chips, cores, _, width = exchange.mine.shape
    rows = a_t.shape[0] // (chips * cores)
    half = width // 2
    for k in range(2):
        columns = slice(k * half, k * half + half)
        block = dot(a_t[...], by_both[:, columns]).astype(BF16)
        exchange.mine[exchange.held(step), :, :, pl.ds(0, rows), columns] = block.reshape(chips, cores, rows, half)


MB = 512
LAGS = (0, 1, 3, 5)


def top_kernel(n, *refs):
    several = 2 * len(EARLY)
    ins, near, outs, far, (send, recv), refs = split(refs, 7, several, 7, several, 2)
    a_in, at_in, h_in, dy_in, w_gate, w_up, w_down = ins
    g_gate, g_up, g_down, squares, by_h, bg_hbm, bu_hbm = outs
    spread = Spread(n, send, recv)
    (a, a_t, dy, wg, wu, hidden_t, wd, both, h_tile, by_tile, load_sem, wd_sem, both_sem, tile_sem, by_sem), refs = split(refs, 15)
    tokens, d = a.shape
    ff = wg.shape[1]
    width = 256
    chunks = ff // width
    downs = 4
    wide_rows, down_rows = d // n, ff // n // 2
    exchange = Exchange(
        n, refs,
        (
            (0, chunks, wide_rows, keep_columns(0, g_gate, g_up, width, squares)),
            (chunks, chunks + downs, down_rows, keep_down(chunks, g_down, down_rows, 2 * width, squares)),
        ),
        LAGS,
    )
    layer = w_gate.shape[0] - 1
    first, rest = pl.ds(0, width), pl.ds(width, ff - width)
    columns_of = lambda columns: [(src.at[layer, :, columns], dst.at[:, columns]) for src, dst in ((w_gate, wg), (w_up, wu))]
    loads = local_copies([(a_in, a), (dy_in, dy), (at_in, a_t), *columns_of(first), *columns_of(rest)], load_sem)
    def down_chunk(c):
        slot = turn(c)
        return pltpu.make_async_copy(w_down.at[layer, pl.ds(pl.multiple_of(c * width, width), width)], wd.at[slot], wd_sem.at[slot])

    loads, later_loads = split(loads, 5)
    for one in (*loads, down_chunk(0)):
        one.start()
    squares[...] = jnp.zeros_like(squares)
    exchange.barrier()

    early = []
    for number, (src, dst) in enumerate(zip(near, far, strict=True)):
        places = [lambda owner, columns, ref=ref: ref.at[owner, :, columns] for ref in (src, dst)]
        early.append(spread.copies(number, places[0], src.shape[2], None, places[1]))
    for copies in early:
        spread.start_far(copies)

    def store_both(c):
        slot = turn(c)
        to = pl.ds(pl.multiple_of(c * width, width), width)
        return local_copies([(both.at[slot, :, pl.ds(k * width, width)], ref.at[:, to]) for k, ref in enumerate((bg_hbm, bu_hbm))], both_sem, slot)

    def chunk(c):
        slot = turn(c)

        @pl.when(c == 0)
        def _():
            for one in loads:
                one.wait()
            for one in later_loads:
                one.start()

        @pl.when(c == 1)
        def _():
            for one in later_loads:
                one.wait()

        @pl.when(c >= BUFFERS)
        def _():
            for one in store_both(c - BUFFERS):
                one.wait()

        @pl.when(c == chunks // 2)
        def _():
            for copies in early:
                spread.pass_last(copies)

        down_chunk(c).wait()

        @pl.when(c + 1 < chunks)
        def _():
            down_chunk(c + 1).start()

        columns = pl.ds(pl.multiple_of(c * width, width), width)
        wg_c, wu_c, wd_c = wg[:, columns], wu[:, columns], wd[slot]
        for at in range(0, tokens, MB):
            rows = slice(at, at + MB)
            hidden, by_gate, by_up = by_units(dot(a[rows], wg_c), dot(a[rows], wu_c), dot(dy[rows], wd_c, TRANSPOSED))
            hidden_t[columns, rows] = hidden.astype(BF16).T
            both[slot, rows, :width] = by_gate.astype(BF16)
            both[slot, rows, width:] = by_up.astype(BF16)
        wide_packet(exchange, c, a_t, both.at[slot])
        for one in store_both(c):
            one.start()
        exchange.move(c, 0, chunks)

    repeat(0, chunks, chunk)
    for c in range(chunks - BUFFERS, chunks):
        for one in store_both(c):
            one.wait()

    tile_rows = 256
    tiles = tokens // tile_rows
    split_at = a_t.shape[1]

    def tile_loads(t):
        slot = turn(t)
        rows = pl.ds(pl.multiple_of(t * tile_rows, tile_rows), tile_rows)
        pairs = [(h_in.at[rows], h_tile.at[slot])]
        for k, src in enumerate((bg_hbm, bu_hbm)):
            to = pl.ds(pl.multiple_of((slot * 2 + k) * tile_rows, tile_rows), tile_rows)
            pairs.append((src.at[rows, pl.ds(0, split_at)], a_t.at[to]))
            pairs.append((src.at[rows, pl.ds(split_at, ff - split_at)], a.at[to, pl.ds(0, ff - split_at)]))
        return local_copies(pairs, tile_sem, slot)

    def tile_store(t):
        slot = turn(t)
        return pltpu.make_async_copy(by_tile.at[slot], by_h.at[pl.ds(pl.multiple_of(t * tile_rows, tile_rows), tile_rows)], by_sem.at[slot])

    for one in tile_loads(0):
        one.start()

    def tile(step):
        t = step - chunks

        @pl.when(t < downs)
        def _():
            down_packet(exchange, step, chunks, hidden_t, dy)

        exchange.move(step, chunks, chunks + tiles)
        slot = turn(t)
        for one in tile_loads(t):
            one.wait()

        @pl.when(t + 1 < tiles)
        def _():
            for one in tile_loads(t + 1):
                one.start()

        @pl.when(t >= BUFFERS)
        def _():
            tile_store(t - BUFFERS).wait()

        total = None
        for k, w in enumerate((wg, wu)):
            at = pl.ds(pl.multiple_of((slot * 2 + k) * tile_rows, tile_rows), tile_rows)
            term = dot(a_t[at], w[:, :split_at], TRANSPOSED) + dot(a[at, : ff - split_at], w[:, split_at:], TRANSPOSED)
            total = term if total is None else total + term
        rows = pl.ds(pl.multiple_of(t * tile_rows, tile_rows), tile_rows)
        by_tile[slot] = (dy[rows].astype(F32) + by_norm(h_tile[slot], total)).astype(BF16)
        tile_store(t).start()

    repeat(chunks, chunks + tiles, tile)
    exchange.finish(chunks + tiles, chunks + downs)
    for t in range(tiles - BUFFERS, tiles):
        tile_store(t).wait()
    for copies in early:
        spread.end_far(copies)


def top_layer(n, a, a_t, h, dy, w_gate, w_up, w_down, near):
    tokens, d = a.shape
    ff = w_gate.shape[2]
    width = 256
    anywhere, inside = pl.BlockSpec(memory_space=pl.ANY), pl.BlockSpec(memory_space=pltpu.VMEM)
    dma = pltpu.SemaphoreType.DMA
    return pl.pallas_call(
        functools.partial(top_kernel, n),
        in_specs=[anywhere] * (7 + len(near)),
        out_specs=[inside] * 4 + [anywhere] * (3 + len(near)),
        out_shape=[
            jax.ShapeDtypeStruct((d // n, ff), BF16),
            jax.ShapeDtypeStruct((d // n, ff), BF16),
            jax.ShapeDtypeStruct((ff // n, d), BF16),
            jax.ShapeDtypeStruct((8, 128), F32),
            jax.ShapeDtypeStruct((tokens, d), BF16),
            jax.ShapeDtypeStruct((tokens, ff), BF16),
            jax.ShapeDtypeStruct((tokens, ff), BF16),
            *[jax.ShapeDtypeStruct(t.shape, t.dtype) for t in near],
        ],
        scratch_shapes=[
            *Spread.semaphores(len(near)),
            *[pltpu.VMEM(t, BF16) for t in ((tokens, d), (d, tokens), (tokens, d), (d, ff), (d, ff), (ff, tokens))],
            *[pltpu.VMEM((BUFFERS, *t), BF16) for t in ((width, d), (tokens, 2 * width), (width, d), (width, d))],
            dma((7,)), dma((BUFFERS,)), dma((2, BUFFERS)), dma((5, BUFFERS)), dma((BUFFERS,)),
            *Exchange.scratch(n, ff // n // 2, 2 * width, LAGS),
        ],
        compiler_params=pltpu.CompilerParams(collective_id=2, has_side_effects=True, vmem_limit_bytes=ALL_VMEM),
        name="top",
    )(a, a_t, h, dy, w_gate, w_up, w_down, *near)


def bottom_kernel(n, *refs):
    some = len(EARLY)
    ins, summed, (g_gate, g_up, g_down, squares), near, (send, recv), refs = split(refs, 6, some, 4, some, 2)
    by_in, ht_in, at_in, gate_in, up_in, w_down = ins
    spread = Spread(n, send, recv)
    (by, hidden_t, a_t, wd, gate, up, both, load_sem, unit_sem), refs = split(refs, 9)
    tokens, d = by.shape
    ff = hidden_t.shape[0]
    width = 256
    chunks = ff // width
    downs = 4
    wide_rows, down_rows = d // n, ff // n // 2
    exchange = Exchange(
        n, refs,
        (
            (0, downs, down_rows, keep_down(0, g_down, down_rows, 2 * width, squares)),
            (downs, downs + chunks, wide_rows, keep_columns(downs, g_gate, g_up, width, squares)),
        ),
        LAGS,
    )
    share = ff // n
    halves = lambda ref, k: ref.at[:, pl.ds(k * 2 * width, 2 * width)]
    pairs = [(halves(by_in, 0), halves(by, 0))]
    for k in range(2):
        for to in range(n):
            rows = pl.ds(to * share + k * down_rows, down_rows)
            pairs.append((ht_in.at[rows], hidden_t.at[rows]))
    pairs += [(halves(by_in, 1), halves(by, 1)), (at_in, a_t)]
    loads = local_copies(pairs, load_sem)

    def chunk_loads(c):
        slot = turn(c)
        columns = pl.ds(pl.multiple_of(c * width, width), width)
        pairs = [(w_down.at[0, columns], wd.at[slot]), (gate_in.at[:, columns], gate.at[slot]), (up_in.at[:, columns], up.at[slot])]
        return local_copies(pairs, unit_sem, slot)

    first, second, third = split(loads, 1 + n, n)
    third += chunk_loads(0)
    for one in first:
        one.start()
    squares[...] = jnp.zeros_like(squares)
    exchange.barrier()

    early = []
    for number, (src, dst) in enumerate(zip(summed, near, strict=True)):
        some = dst.shape[1]
        own = src.at[pl.ds(src.shape[0] - some, some)]
        early.append(spread.copies(number, lambda owner, columns, dst=dst: dst.at[owner, :, columns], dst.shape[2], own))
    for copies in early:
        spread.start(copies)

    def down(step):
        @pl.when(step == 0)
        def _():
            for one in first:
                one.wait()
            for one in second:
                one.start()

        @pl.when(step == 1)
        def _():
            for one in second:
                one.wait()
            for one in third:
                one.start()

        @pl.when(step == 2)
        def _():
            for one in third[:2]:
                one.wait()

        down_packet(exchange, step, 0, hidden_t, by)
        exchange.move(step, 0, downs)

    repeat(0, downs, down)

    def chunk(step):
        c = step - downs
        slot = turn(c)
        for one in chunk_loads(c):
            one.wait()

        @pl.when(c + 1 < chunks)
        def _():
            for one in chunk_loads(c + 1):
                one.start()

        wd_c = wd[slot]
        for at in range(0, tokens, MB):
            rows = slice(at, at + MB)
            _, by_gate, by_up = by_units(gate[slot, rows], up[slot, rows], dot(by[rows], wd_c, TRANSPOSED))
            both[rows, :width] = by_gate.astype(BF16)
            both[rows, width:] = by_up.astype(BF16)
        wide_packet(exchange, step, a_t, both)
        exchange.move(step, downs, downs + chunks)

    repeat(downs, downs + chunks, chunk)
    exchange.finish(downs + chunks, downs + chunks)
    for copies in early:
        spread.end_near(copies)


def bottom_layer(n, by, hidden_t, a_t, gate, up, w_down, summed):
    tokens, d = by.shape
    ff = hidden_t.shape[0]
    width = 256
    anywhere, inside = pl.BlockSpec(memory_space=pl.ANY), pl.BlockSpec(memory_space=pltpu.VMEM)
    dma = pltpu.SemaphoreType.DMA
    return pl.pallas_call(
        functools.partial(bottom_kernel, n),
        in_specs=[anywhere] * (6 + len(summed)),
        out_specs=[inside] * 4 + [anywhere] * len(summed),
        out_shape=[
            jax.ShapeDtypeStruct((d // n, ff), BF16),
            jax.ShapeDtypeStruct((d // n, ff), BF16),
            jax.ShapeDtypeStruct((ff // n, d), BF16),
            jax.ShapeDtypeStruct((8, 128), F32),
            *[jax.ShapeDtypeStruct((n, some, ff), BF16) for _, some in EARLY],
        ],
        scratch_shapes=[
            *Spread.semaphores(len(summed)),
            *[pltpu.VMEM(t, BF16) for t in ((tokens, d), (ff, tokens), (d, tokens), (BUFFERS, width, d))],
            *[pltpu.VMEM((BUFFERS, tokens, width), F32)] * 2, pltpu.VMEM((tokens, 2 * width), BF16),
            dma((3 + 2 * n,)), dma((3, BUFFERS)),
            *Exchange.scratch(n, ff // n // 2, 2 * width, LAGS),
        ],
        compiler_params=pltpu.CompilerParams(collective_id=3, has_side_effects=True, vmem_limit_bytes=ALL_VMEM),
        name="bottom",
    )(by, hidden_t, a_t, gate, up, w_down, *summed)


def solution(mesh):
    n = mesh.shape["dp"]

    def step(x, dy, w_gate, w_up, w_down, *moments):
        m, v = split(moments, WEIGHTS)
        gate, up, hidden_t, a_t, h, next_a, next_a_t, *early = layer_0(n, x[0], w_gate, w_up, w_down, m, v)
        top = top_layer(n, next_a, next_a_t, h, dy[0], w_gate, w_up, w_down, early)
        top, (squares_1, by_h, _, _), far = split(top, WEIGHTS, 4)
        bottom = bottom_layer(n, by_h, hidden_t, a_t, gate, up, w_down, [top[i] for i, _ in EARLY])
        bottom, (squares_0,), near = split(bottom, WEIGHTS, 1)
        gradients = list(zip(bottom, top, strict=True))
        return tuple(finish(n, gradients, (squares_0, squares_1), (w_gate, w_up, w_down), m, v, (*early, *far, *near)))

    sharded = P(None, "dp", None)
    return jax.shard_map(
        step,
        mesh=mesh,
        in_specs=(P(("rep", "dp")), P(("rep", "dp")), P(), P(), P(), *[sharded] * 6),
        out_specs=(*[P("rep")] * 3, *[P("rep", "dp")] * 6),
        check_vma=False,
    )
```

```python
import functools

import jax
import jax.numpy as jnp
from jax import lax
from jax.experimental import pallas as pl
from jax.experimental.pallas import tpu as pltpu
from jax.sharding import PartitionSpec as P

MESH = pl.DeviceIdType.MESH
F32, BF16 = jnp.float32, jnp.bfloat16
CORES = 2
BUFFERS = 2
WEIGHTS = 3
MIB = 2**20
ALL_VMEM = 67043328
TRANSPOSED = ((1,), (1,))


def turn(t):
    return lax.rem(t, BUFFERS)


def repeat(low, high, body):
    def step(i, nothing):
        body(i)
        return nothing

    lax.fori_loop(low, high, step, None)


def split(refs, *sizes):
    left = iter(refs)
    runs = [[next(left) for _ in range(size)] for size in sizes]
    return *runs, list(left)


def local_copies(pairs, sem, *at):
    return [pltpu.make_async_copy(src, dst, sem.at[(k, *at)]) for k, (src, dst) in enumerate(pairs)]


def places(axis, n):
    me = lax.axis_index(axis)
    chips = n // CORES
    core, chip = lax.rem(me, CORES), lax.div(me, CORES)
    at = lambda away: lax.rem(chip + away, chips) * CORES + core
    return me, core, me + 1 - 2 * core, at(1), at(chips - 1), at(2)


class Spread:
    KINDS = 9

    def __init__(self, n, send, recv):
        self.send, self.recv = send, recv
        self.me, _, self.partner, self.after, self.before, self.across = places("dp", n)

    @staticmethod
    def semaphores(pieces):
        return [pltpu.SemaphoreType.DMA((Spread.KINDS, pieces))] * 2

    def barrier(self):
        barrier = pltpu.get_barrier_semaphore()
        for peer in (self.partner, self.after, self.before):
            pl.semaphore_signal(barrier, inc=1, device_id={"dp": peer}, device_id_type=MESH)
        pl.semaphore_wait(barrier, 3)

    def copies(self, number, place, width, own=None, far=None):
        far = far or place
        every, left, right = pl.ds(0, width), pl.ds(0, width // 2), pl.ds(width // 2, width // 2)

        class Copies(dict):
            def __missing__(_, kind):
                to, src, dst = routes[kind]
                sems = (t.at[list(routes).index(kind), number] for t in (self.send, self.recv))
                return pltpu.make_async_remote_copy(src, dst, *sems, device_id={"dp": to}, device_id_type=MESH)

        me, after, before, across = self.me, self.after, self.before, self.across
        own = place(me, every) if own is None else own
        routes = {
            "after": (after, own, place(me, every)),
            "before": (before, own, place(me, every)),
            "partner": (self.partner, own, place(me, every)),
            "on": (after, place(before, left), far(before, left)),
            "back": (before, place(after, right), far(after, right)),
            "partner_before": (self.partner, place(before, every), far(before, every)),
            "partner_after": (self.partner, place(after, every), far(after, every)),
            "partner_left": (self.partner, far(across, left), far(across, left)),
            "partner_right": (self.partner, far(across, right), far(across, right)),
        }
        return Copies()

    @staticmethod
    def start(copies):
        for kind in ("after", "before", "partner"):
            copies[kind].start()

    @staticmethod
    def pass_on(copies):
        copies["after"].wait_recv()
        copies["on"].start()
        copies["partner_before"].start()
        copies["before"].wait_recv()
        copies["back"].start()
        copies["partner_after"].start()

    @staticmethod
    def pass_last(copies):
        copies["on"].wait_recv()
        copies["partner_left"].start()
        copies["back"].wait_recv()
        copies["partner_right"].start()

    @staticmethod
    def end(copies):
        for kind in ("partner", "partner_before", "partner_after", "partner_left", "partner_right"):
            copies[kind].wait_recv()
        for kind in (*Spread.NEAR, *Spread.THEN, *Spread.LAST):
            copies[kind].wait_send()


    NEAR, THEN, LAST = ("after", "before", "partner"), ("on", "back", "partner_before", "partner_after"), ("partner_left", "partner_right")

    @staticmethod
    def end_near(copies):
        for kind in Spread.NEAR:
            copies[kind].wait()

    @staticmethod
    def start_far(copies):
        for kind in Spread.THEN:
            copies[kind].start()

    @staticmethod
    def end_far(copies):
        for kind in Spread.THEN:
            copies[kind].wait_send()
        for kind in (*Spread.THEN[2:], *Spread.LAST):
            copies[kind].wait_recv()
        for kind in Spread.LAST:
            copies[kind].wait_send()


EARLY = ((0, 32), (1, 32))


def finish_kernel(n, count, layers, pieces, *refs):
    some = len(EARLY)
    squares, *g_in = zip(*[iter(refs[: layers + layers * WEIGHTS])] * layers)
    refs = refs[layers + layers * WEIGHTS :]
    w_in, m_in, v_in, near_m, near_v, far_m, far_v, near_g, w, m, v, far_g, g, refs = split(
        refs, *[WEIGHTS] * 3, *[some] * 5, *[WEIGHTS] * 3, some, WEIGHTS
    )
    parts, m_tile, v_tile, g_tile, load_sem, early_sem, tile_sem, part_send, part_recv, send, recv = refs
    spread = Spread(n, send, recv)
    me = spread.me

    barrier = pltpu.get_barrier_semaphore()
    peers = [lax.rem(me + away, n) for away in range(1, n)]
    for peer in peers:
        pl.semaphore_signal(barrier, inc=1, device_id={"dp": peer}, device_id_type=MESH)

    def rows_of(i, owner, first, rows):
        return pl.ds(pl.multiple_of(owner * g[i].shape[1] + first, 16), rows)

    order = (2, 0, 1)
    loads = {}
    for i in order:
        rows = rows_of(i, me, 0, g[i].shape[1])
        pairs = [(w_in[i].at[:, rows], w[i].at[:, rows]), (m_in[i], m[i]), (v_in[i], v[i])]
        pairs += [(g_in[i][k], g[i].at[k]) for k in range(layers)]
        loads[i] = [pltpu.make_async_copy(src, dst, load_sem.at[i, k]) for k, (src, dst) in enumerate(pairs)]
    first_weight, *other_weights = order
    for one in loads[first_weight]:
        one.start()

    total = sum(t[...] for t in squares)
    parts[pl.ds(me, 1)] = total[None]
    early = []
    for k, (i, some) in enumerate(EARLY):
        near = lambda owner, columns, ref=near_g[k]: ref.at[owner, :, columns]
        far = lambda owner, columns, ref=far_g[k]: ref.at[owner, :, columns]
        early.append(spread.copies(len(pieces) + k, near, g[i].shape[2], None, far))
    pl.semaphore_wait(barrier, n - 1)
    part_copies = []
    for k, peer in enumerate(peers):
        part_copies.append(
            pltpu.make_async_remote_copy(
                parts.at[me], parts.at[me], part_send.at[k], part_recv.at[k], device_id={"dp": peer}, device_id_type=MESH
            )
        )
        part_copies[-1].start()
    for copies in early:
        spread.start_far(copies)
    for one in part_copies:
        one.wait_recv()
    every = parts[0]
    for k in range(1, n):
        every += parts[k]
    mean = jnp.sum(every, keepdims=True) / count
    factor = jnp.minimum(1.0, 0.5 * lax.rsqrt(mean + 1e-30))

    def stepped(grad, m_old, v_old, w_old):
        grad = grad.astype(F32) * factor
        m_new = 0.9 * m_old + 0.1 * grad
        v_new = 0.95 * v_old + 0.05 * grad * grad
        w_old = w_old.astype(F32)
        return m_new, v_new, (w_old - 0.02 * (m_new * lax.rsqrt(v_new + 1e-8) + 0.1 * w_old)).astype(BF16)

    step_rows, width = 16, 256

    def adamw(i, layer, first, rows):
        def body(step):
            start = first + step * step_rows
            at = (layer, pl.ds(pl.multiple_of(start, 16), step_rows), slice(None))
            mine = (layer, rows_of(i, me, start, step_rows), slice(None))
            m[i][at], v[i][at], w[i][mine] = stepped(g[i][at], m[i][at], v[i][at], w[i][mine])

        repeat(0, rows // step_rows, body)

    waited = set()

    def compute(i, layer, first, rows):
        if i not in waited:
            waited.add(i)
            for one in loads[i]:
                one.wait()
        adamw(i, layer, first, rows)

    made = []
    for number, (i, layer, first, rows) in enumerate(pieces):
        place = lambda owner, columns, i=i, layer=layer, first=first, rows=rows: w[i].at[layer, rows_of(i, owner, first, rows), columns]
        made.append(spread.copies(number, place, g[i].shape[2]))

    def own_piece(number):
        compute(*pieces[number])
        spread.start(made[number])

    other = lambda device: device + spread.partner - me
    units = []
    for k, (i, some) in enumerate(EARLY):
        near, far = (near_m[k], near_v[k], near_g[k]), (far_m[k], far_v[k], far_g[k])
        for refs, owners in (
            (near, (spread.partner, spread.after, spread.before)),
            (far, (other(spread.after), other(spread.before), spread.across, other(spread.across))),
        ):
            units += [(refs, i, owner, first, g[i].shape[1] - some) for owner in owners for first in range(0, some, step_rows)]

    def unit_loads(number):
        refs, _, owner, first, _ = units[number]
        slot = number % BUFFERS
        tiles = zip(refs, (m_tile, v_tile, g_tile), strict=True)
        return local_copies([(src.at[owner, pl.ds(first, step_rows)], dst.at[slot]) for src, dst in tiles], tile_sem, slot)

    def unit_rows(number):
        _, i, owner, first, start = units[number]
        return rows_of(i, owner, start + first, step_rows)

    last = layers - 1
    old_rows = local_copies(
        [tuple(t[i].at[last, unit_rows(number)] for t in (w_in, w)) for number, (_, i, _, _, _) in enumerate(units)], early_sem
    )

    def unit(number):
        (_, i, _, _, _), slot = units[number], number % BUFFERS
        if number + 1 < len(units):
            for one in unit_loads(number + 1):
                one.start()
        for one in (*unit_loads(number), old_rows[number]):
            one.wait()

        def body(step):
            columns = pl.ds(pl.multiple_of(step * width, width), width)
            its, at = (last, unit_rows(number), columns), (slot, slice(None), columns)
            *_, w[i][its] = stepped(g_tile[at], m_tile[at], v_tile[at], w[i][its])

        repeat(0, g[i].shape[-1] // width, body)

    own_piece(0)
    for i in other_weights:
        for one in loads[i]:
            one.start()
    for one in old_rows:
        one.start()
    total_pieces, done = len(pieces), 0
    for number in range(total_pieces + 2):
        if number + 1 < total_pieces:
            own_piece(number + 1)
        if number == 0:
            for copies in early:
                spread.pass_last(copies)
        if 1 <= number <= total_pieces:
            spread.pass_on(made[number - 1])
        if 2 <= number:
            spread.pass_last(made[number - 2])
        if number == 2:
            for copies in early:
                spread.end_far(copies)
            for one in unit_loads(0):
                one.start()
        if 3 <= number < total_pieces:
            for k in range(min(3, len(units) - done)):
                unit(done + k)
            done += min(3, len(units) - done)
    for k in range(done, len(units)):
        unit(k)
    for i, some in EARLY:
        compute(i, last, g[i].shape[1] - some, some)
    for copies in made:
        spread.end(copies)
    for one in part_copies:
        one.wait_send()


def store_kernel(*refs):
    *refs, sem = refs
    some = len(refs) // 2
    copies = local_copies([(refs[k], refs[some + k]) for k in range(some)], sem)
    for one in copies:
        one.start()
    for one in copies:
        one.wait()


def early_shapes(n, blocks, dtype, times=1):
    return [jax.ShapeDtypeStruct((n, some, blocks[i][0].shape[-1]), dtype) for _ in range(times) for i, some in EARLY]


def finish(n, gradients, squares, weights, m, v, early):
    count = float(sum(w.size for w in weights))
    layers = len(gradients[0])
    pieces = []
    for i in (2, 0, 1):
        rows, _ = gradients[i][0].shape
        for layer in range(layers):
            half = rows // 2
            cuts = [half, half]
            if (i, layer) == (2, 0):
                cuts = [48, half - 48, half]
            elif layer == layers - 1 and i in dict(EARLY):
                rest = half - dict(EARLY)[i]
                cuts = [half, rest - 16, 16] if i == 1 else [half, rest]
            for cut in cuts:
                pieces.append((i, layer, sum(p[3] for p in pieces if p[:2] == (i, layer)), cut))
    anywhere, inside = pl.BlockSpec(memory_space=pl.ANY), pl.BlockSpec(memory_space=pltpu.VMEM)
    dma = pltpu.SemaphoreType.DMA
    results = [*weights, *m, *v]
    tile = lambda dtype: pltpu.VMEM((BUFFERS, 16, max(gradients[i][0].shape[1] for i, _ in EARLY)), dtype)
    ready = pl.pallas_call(
        functools.partial(finish_kernel, n, count, layers, tuple(pieces)),
        out_shape=[pltpu.VMEM(t.shape, t.dtype) for t in results]
        + early_shapes(n, gradients, BF16),
        in_specs=[inside] * layers + [anywhere] * (WEIGHTS * layers + len(results) + len(early)),
        out_specs=[inside] * len(results) + [anywhere] * len(EARLY),
        scratch_shapes=[
            *[pltpu.VMEM((layers, *one[0].shape), BF16) for one in gradients],
            pltpu.VMEM((n, 8, 128), F32), tile(F32), tile(F32), tile(BF16),
            dma((WEIGHTS, layers + 3)), dma((sum(some for _, some in EARLY) // 16 * (n - 1),)), dma((3, BUFFERS)), *[dma((n - 1,))] * 2,
            *Spread.semaphores(len(pieces) + len(EARLY)),
        ],
        compiler_params=pltpu.CompilerParams(collective_id=4, has_side_effects=True, vmem_limit_bytes=8 * MIB),
        name="finish",
    )(*squares, *sum(gradients, ()), *weights, *m, *v, *early)[: len(results)]
    return pl.pallas_call(
        store_kernel,
        out_shape=[jax.ShapeDtypeStruct(t.shape, t.dtype) for t in results],
        in_specs=[inside] * len(results),
        out_specs=[anywhere] * len(results),
        scratch_shapes=[dma((len(results),))],
        compiler_params=pltpu.CompilerParams(vmem_limit_bytes=8 * MIB),
        name="store",
    )(*[pltpu.with_memory_space_constraint(t, pltpu.VMEM) for t in ready])


def dot(a, b, contract=((1,), (0,))):
    return lax.dot_general(a, b, (contract, ((), ())), preferred_element_type=F32)


def normed(h):
    wide = h.astype(F32)
    return (wide * lax.rsqrt(jnp.mean(wide * wide, -1, keepdims=True) + 1e-6)).astype(BF16)


def by_norm(h, by_a):
    wide = h.astype(F32)
    scale = lax.rsqrt(jnp.mean(wide * wide, -1, keepdims=True) + 1e-6)
    return scale * by_a - wide * (scale * scale * scale * jnp.mean(by_a * wide, -1, keepdims=True))


def by_units(gate, up, by_hidden):
    by_hidden = by_hidden.astype(BF16).astype(F32)
    s = jax.nn.sigmoid(gate)
    silu = gate * s
    return silu * up, by_hidden * up * (s + silu * (1.0 - s)), by_hidden * silu


def forward_kernel(n, *refs):
    (x_in, w_gate, w_up, w_down), moments, outs, early, refs = split(refs, 4, 2 * len(EARLY), 7, 2 * len(EARLY))
    gate_out, up_out, ht_out, at_out, h_out, b_out, bt_out = outs
    (wg, wu, wd, hidden, x, gate, up, hidden_t, a_t, h, b, b_t, w_sem, x_sem, sem, late_sem, send, recv) = refs
    spread = Spread(n, send, recv)
    rows = x.shape[1]
    tiles = x_in.shape[0] // rows
    ff = wg.shape[1]
    width = 256
    groups = [range(at, min(at + 3 * width, ff), width) for at in range(0, ff, 3 * width)]
    tall = lambda ref, t: ref.at[pl.ds(pl.multiple_of(t * rows, rows), rows)]
    wide = lambda ref, t: ref.at[:, pl.ds(pl.multiple_of(t * rows, rows), rows)]

    def load_x(t):
        return pltpu.make_async_copy(tall(x_in, t), x.at[lax.rem(t, x.shape[0])], x_sem.at[lax.rem(t, x.shape[0])])

    def stores(t, first):
        slot = turn(t)
        if first:
            pairs = [(gate, tall(gate_out, t)), (up, tall(up_out, t)), (hidden_t, wide(ht_out, t)), (a_t, wide(at_out, t))]
        else:
            pairs = [(h, tall(h_out, t)), (b, tall(b_out, t)), (b_t, wide(bt_out, t))]
        return local_copies([(src.at[slot], dst) for src, dst in pairs], sem if first else late_sem, slot)

    w_loads = []
    for k, group in enumerate(groups):
        columns = slice(group[0], group[-1] + width)
        w_loads.append([
            pltpu.make_async_copy(src.at[0, :, columns], dst.at[:, columns], w_sem.at[j, k]) for j, (src, dst) in enumerate(((w_gate, wg), (w_up, wu)))
        ])
    down_load = pltpu.make_async_copy(w_down.at[0], wd, w_sem.at[2, 0])
    for one in (load_x(0), *w_loads[0], *w_loads[1], load_x(1)):
        one.start()
    spread.barrier()
    pieces = []
    for number, (src, dst) in enumerate(zip(moments, early, strict=True)):
        some = dst.shape[1]
        own = src.at[src.shape[0] - 1, pl.ds(src.shape[1] - some, some)]
        pieces.append(spread.copies(number, lambda owner, columns, dst=dst: dst.at[owner, :, columns], dst.shape[2], own))
    for copies in pieces:
        spread.start(copies)

    def first_part(t, group, a):
        slot = turn(t)
        for at in group:
            columns = slice(at, at + width)
            g, u = dot(a, wg[:, columns]), dot(a, wu[:, columns])
            gate[slot, :, columns] = g
            up[slot, :, columns] = u
            units = (g * jax.nn.sigmoid(g) * u).astype(BF16)
            hidden[:, columns] = units
            hidden_t[slot, columns] = units.T

    def second_part(t):
        slot = turn(t)
        out = x[lax.rem(t, x.shape[0])] + dot(hidden[...], wd[...]).astype(BF16)
        h[slot] = out
        after = normed(out)
        b[slot] = after
        b_t[slot] = after.T

    def normed_tile(t):
        a = normed(x[lax.rem(t, x.shape[0])])
        a_t[turn(t)] = a.T
        return a

    load_x(0).wait()
    a = normed_tile(0)
    for k, group in enumerate(groups):
        for one in w_loads[k]:
            one.wait()
        for one in w_loads[k + 2] if k + 2 < len(groups) else ([down_load] if k + 2 == len(groups) else []):
            one.start()
        first_part(0, group, a)
    for one in stores(0, True):
        one.start()
    down_load.wait()

    def tile(t):
        load_x(t).wait()

        @pl.when(t + 1 < tiles)
        def _():
            load_x(t + 1).start()

        @pl.when(t >= BUFFERS)
        def _():
            for one in stores(t - BUFFERS, True):
                one.wait()

        @pl.when(t > BUFFERS)
        def _():
            for one in stores(t - 1 - BUFFERS, False):
                one.wait()

        a = normed_tile(t)
        second_part(t - 1)
        first_part(t, range(0, ff, width), a)
        for one in (*stores(t - 1, False), *stores(t, True)):
            one.start()

    repeat(1, tiles, tile)
    last = tiles - 1
    for one in stores(last - BUFFERS, False):
        one.wait()
    second_part(last)
    for one in stores(last, False):
        one.start()
    for copies in pieces:
        spread.end_near(copies)
    for t in (last - 1, last):
        for one in (*stores(t, True), *stores(t, False)):
            one.wait()


def layer_0(n, x, w_gate, w_up, w_down, m, v):
    tokens, d = x.shape
    ff = w_gate.shape[2]
    rows = 256
    anywhere = pl.BlockSpec(memory_space=pl.ANY)
    dma = pltpu.SemaphoreType.DMA
    vmem = lambda *shape: pltpu.VMEM(shape, BF16)
    return pl.pallas_call(
        functools.partial(forward_kernel, n),
        in_specs=[anywhere] * (4 + 2 * len(EARLY)),
        out_specs=[anywhere] * (7 + 2 * len(EARLY)),
        out_shape=[
            jax.ShapeDtypeStruct((tokens, ff), F32),
            jax.ShapeDtypeStruct((tokens, ff), F32),
            jax.ShapeDtypeStruct((ff, tokens), BF16),
            jax.ShapeDtypeStruct((d, tokens), BF16),
            jax.ShapeDtypeStruct((tokens, d), BF16),
            jax.ShapeDtypeStruct((tokens, d), BF16),
            jax.ShapeDtypeStruct((d, tokens), BF16),
            *early_shapes(n, m, F32, 2),
        ],
        scratch_shapes=[
            vmem(d, ff), vmem(d, ff), vmem(ff, d), vmem(rows, ff), vmem(3, rows, d),
            *[pltpu.VMEM((BUFFERS, rows, ff), F32)] * 2, *[vmem(BUFFERS, *t) for t in ((ff, rows), (d, rows), (rows, d), (rows, d), (d, rows))],
            dma((WEIGHTS, 4)), dma((3,)), dma((4, BUFFERS)), dma((3, BUFFERS)), *Spread.semaphores(2 * len(EARLY)),
        ],
        compiler_params=pltpu.CompilerParams(collective_id=1, has_side_effects=True, vmem_limit_bytes=60 * MIB),
        name="forward",
    )(x, w_gate, w_up, w_down, *[t[i] for t in (m, v) for i, _ in EARLY])


class Exchange:
    def __init__(self, n, refs, kinds, lags):
        self.mine, self.pair, self.out2, self.out3, self.in2, self.in3, self.own, self.side, self.pair_sem, self.sem2, self.sem3 = refs
        self.kinds = kinds
        self.lags = lags
        self.me, self.core, self.partner, self.after, self.before, _ = places("dp", n)
        chips = n // CORES
        self.chip = lax.div(self.me, CORES)
        self.chip_after, self.chip_before, self.chip_across = (lax.rem(self.chip + k, chips) for k in (1, chips - 1, chips // 2))
        half = self.out3.shape[-1]
        self.left, self.right = slice(0, half), slice(half, 2 * half)

    @staticmethod
    def scratch(n, rows, width, lags):
        chips, half, dma = n // CORES, width // 2, pltpu.SemaphoreType.DMA
        _, two, three, four = lags
        slots1, slots2, slots3 = two + 3, 2 * (three - two) + 2, 2 * (four - three) + 2
        return [
            pltpu.VMEM((two + 1, chips, CORES, rows, width), BF16),
            pltpu.VMEM((slots1, chips, rows, width), BF16),
            pltpu.VMEM((2, three - two + 1, rows, width), BF16),
            pltpu.VMEM((2, four - three + 1, rows, half), BF16),
            pltpu.VMEM((2, slots2, rows, width), BF16),
            pltpu.VMEM((2, slots3, rows, half), BF16),
            pltpu.VMEM((four - two + 1, rows, width), F32),
            pltpu.VMEM((2, three - two + 1, rows, half), F32),
            dma((2, slots1)), dma((2, 2, slots2)), dma((2, 2, slots3)),
        ]

    def held(self, p):
        return lax.rem(p, self.mine.shape[0])

    def barrier(self):
        barrier = pltpu.get_barrier_semaphore()
        for peer in (self.partner, self.after, self.before):
            pl.semaphore_signal(barrier, inc=1, device_id={"dp": peer}, device_id_type=MESH)
        pl.semaphore_wait(barrier, 3)

    def copy1(self, p, rows):
        slot = lax.rem(p, self.pair.shape[0])
        return pltpu.make_async_remote_copy(
            self.mine.at[self.held(p), :, 1 - self.core, pl.ds(0, rows)], self.pair.at[slot, :, pl.ds(0, rows)],
            self.pair_sem.at[0, slot], self.pair_sem.at[1, slot], device_id={"dp": self.partner}, device_id_type=MESH,
        )

    def copies(self, p, rows, out, into, sem):
        slot = lax.rem(p, into.shape[1])
        return [
            pltpu.make_async_remote_copy(
                out.at[way, lax.rem(p, out.shape[1]), pl.ds(0, rows)], into.at[way, slot, pl.ds(0, rows)],
                sem.at[0, way, slot], sem.at[1, way, slot], device_id={"dp": to}, device_id_type=MESH,
            )
            for way, to in enumerate((self.after, self.before))
        ]

    def copies2(self, p, rows):
        return self.copies(p, rows, self.out2, self.in2, self.sem2)

    def copies3(self, p, rows):
        return self.copies(p, rows, self.out3, self.in3, self.sem3)

    def stage1(self, p, rows, _):
        self.copy1(p, rows).start()

    def stage2(self, p, rows, _):
        self.copy1(p, rows).wait()
        slot, own, side = (lax.rem(p, t.shape[k]) for t, k in ((self.out2, 1), (self.own, 0), (self.side, 1)))
        at = slice(0, rows)

        def of_chip(chip, columns):
            a = self.mine[self.held(p), chip, self.core, at, columns].astype(F32)
            return a + self.pair[lax.rem(p, self.pair.shape[0]), chip, at, columns].astype(F32)

        self.out2[0, slot, at, self.left] = of_chip(self.chip_across, self.left).astype(BF16)
        self.out2[0, slot, at, self.right] = of_chip(self.chip_after, self.right).astype(BF16)
        self.out2[1, slot, at, self.left] = of_chip(self.chip_before, self.left).astype(BF16)
        self.out2[1, slot, at, self.right] = of_chip(self.chip_across, self.right).astype(BF16)
        for one in self.copies2(p, rows):
            one.start()
        self.side[0, side, at] = of_chip(self.chip_after, self.left)
        self.side[1, side, at] = of_chip(self.chip_before, self.right)
        for columns in (self.left, self.right):
            self.own[own, at, columns] = of_chip(self.chip, columns)

    def stage3(self, p, rows, _):
        for one in self.copies2(p, rows):
            one.wait()
        slot, arrived, own, side = (lax.rem(p, t.shape[k]) for t, k in ((self.out3, 1), (self.in2, 1), (self.own, 0), (self.side, 1)))
        at = slice(0, rows)
        self.out3[0, slot, at] = (self.side[0, side, at] + self.in2[0, arrived, at, self.left].astype(F32)).astype(BF16)
        self.out3[1, slot, at] = (self.side[1, side, at] + self.in2[1, arrived, at, self.right].astype(F32)).astype(BF16)
        for one in self.copies3(p, rows):
            one.start()
        self.own[own, at, self.left] += self.in2[1, arrived, at, self.left].astype(F32)
        self.own[own, at, self.right] += self.in2[0, arrived, at, self.right].astype(F32)

    def stage4(self, p, rows, keep):
        for one in self.copies3(p, rows):
            one.wait()
        arrived, own = lax.rem(p, self.in3.shape[1]), lax.rem(p, self.own.shape[0])
        at = slice(0, rows)
        a = self.own[own, at, self.left] + self.in3[0, arrived, at].astype(F32)
        b = self.own[own, at, self.right] + self.in3[1, arrived, at].astype(F32)
        keep(p, a.astype(BF16), b.astype(BF16))

    def finish(self, step, packets):
        for step in range(step, packets + self.lags[-1]):
            self.move(step, step, step + 1)

    def move(self, step, low, high):
        for lag, stage in zip(self.lags, (self.stage1, self.stage2, self.stage3, self.stage4), strict=True):
            for first, end, rows, keep in self.kinds:
                if high - 1 - lag < first or low - lag >= end:
                    continue
                p = step - lag
                if low - lag >= first and high - 1 - lag < end:
                    stage(p, rows, keep)
                else:
                    pl.when((p >= first) & (p < end))(functools.partial(stage, p, rows, keep))


def add_squares(total, *blocks):
    for block in blocks:
        wide = block.astype(F32)
        wide = wide * wide
        rows, columns = wide.shape
        sums = [wide[r : r + 8, c : c + 128] for r in range(0, rows, 8) for c in range(0, columns, 128)]
        while len(sums) > 1:
            sums = [a + b for a, b in zip(sums[::2], sums[1::2])] + ([sums[-1]] if len(sums) % 2 else [])
        total[...] += sums[0]


def keep_columns(first, gate, up, width, squares):
    def keep(p, left, right):
        columns = pl.ds(pl.multiple_of((p - first) * width, width), width)
        gate[:, columns] = left
        up[:, columns] = right
        add_squares(squares, left, right)

    return keep


def keep_tall(first, down, rows, width, squares):
    def keep(p, left, right):
        columns = pl.ds(pl.multiple_of((p - first) * width, width), width)
        down[:rows, columns] = left
        down[rows:, columns] = right
        add_squares(squares, left, right)

    return keep


def keep_down(first, down, rows, width, squares):
    def keep(p, left, right):
        half = width // 2
        which = p - first
        at = pl.ds(pl.multiple_of(lax.rem(which, 2) * rows, 16), rows)
        start = lax.div(which, 2) * width
        down[at, pl.ds(pl.multiple_of(start, half), half)] = left
        down[at, pl.ds(pl.multiple_of(start + half, half), half)] = right
        add_squares(squares, left, right)

    return keep


def tall_packet(exchange, step, first, hidden_t, by_out):
    _, chips, cores, rows, width = exchange.mine.shape
    half = width // 2
    by_out = by_out[:, pl.ds(pl.multiple_of((step - first) * half, half), half)]
    for k in range(chips * cores):
        block = dot(hidden_t[2 * rows * k : 2 * rows * (k + 1), :], by_out).astype(BF16)
        for part in range(2):
            exchange.mine[exchange.held(step), k // cores, k % cores, :, part * half : (part + 1) * half] = block[part * rows : (part + 1) * rows]


def down_packet(exchange, step, first, hidden_t, by_out):
    n_rows = hidden_t.shape[0]
    _, chips, cores, rows, width = exchange.mine.shape
    which = step - first
    start = pl.multiple_of(lax.rem(which, 2) * rows, 16)
    columns = pl.ds(pl.multiple_of(lax.div(which, 2) * width, width), width)
    share = n_rows // (chips * cores)
    by_out = by_out[:, columns]
    for k in range(chips * cores):
        lhs = hidden_t[pl.ds(pl.multiple_of(k * share + start, 16), rows), :]
        exchange.mine[exchange.held(step), k // cores, k % cores] = dot(lhs, by_out).astype(BF16)


def wide_packet(exchange, step, a_t, by_both):
    _, chips, cores, _, width = exchange.mine.shape
    rows = a_t.shape[0] // (chips * cores)
    half = width // 2
    for k in range(2):
        columns = slice(k * half, k * half + half)
        block = dot(a_t[...], by_both[:, columns]).astype(BF16)
        exchange.mine[exchange.held(step), :, :, pl.ds(0, rows), columns] = block.reshape(chips, cores, rows, half)


MB = 1024
TOP_LAGS = (0, 1, 4, 6)
BOTTOM_LAGS = (0, 1, 4, 7)


def top_kernel(n, *refs):
    several = 2 * len(EARLY)
    ins, near, outs, far, (send, recv), refs = split(refs, 7, several, 7, several, 2)
    a_in, at_in, h_in, dy_in, w_gate, w_up, w_down = ins
    g_gate, g_up, g_down, squares, by_h, bg_hbm, bu_hbm = outs
    spread = Spread(n, send, recv)
    (a, a_t, dy, wg, wu, hidden_t, wd, both, h_tile, by_tile, load_sem, wd_sem, both_sem, tile_sem, by_sem), refs = split(refs, 15)
    tokens, d = a.shape
    ff = wg.shape[1]
    width = 256
    chunks = ff // width
    downs = 4
    wide_rows, down_rows = d // n, ff // n // 2
    exchange = Exchange(
        n, refs,
        (
            (0, chunks, wide_rows, keep_columns(0, g_gate, g_up, width, squares)),
            (chunks, chunks + downs, down_rows, keep_tall(chunks, g_down, down_rows, width, squares)),
        ),
        TOP_LAGS,
    )
    layer = w_gate.shape[0] - 1
    first, rest = pl.ds(0, width), pl.ds(width, ff - width)
    columns_of = lambda columns: [(src.at[layer, :, columns], dst.at[:, columns]) for src, dst in ((w_gate, wg), (w_up, wu))]
    loads = local_copies([(a_in, a), (dy_in, dy), (at_in, a_t), *columns_of(first), *columns_of(rest)], load_sem)
    def down_chunk(c):
        slot = turn(c)
        return pltpu.make_async_copy(w_down.at[layer, pl.ds(pl.multiple_of(c * width, width), width)], wd.at[slot], wd_sem.at[slot])

    loads, later_loads = split(loads, 5)
    for one in (*loads, down_chunk(0)):
        one.start()
    squares[...] = jnp.zeros_like(squares)
    exchange.barrier()

    early = []
    for number, (src, dst) in enumerate(zip(near, far, strict=True)):
        places = [lambda owner, columns, ref=ref: ref.at[owner, :, columns] for ref in (src, dst)]
        early.append(spread.copies(number, places[0], src.shape[2], None, places[1]))
    for copies in early:
        spread.start_far(copies)

    def store_both(c):
        slot = turn(c)
        to = pl.ds(pl.multiple_of(c * width, width), width)
        return local_copies([(both.at[slot, :, pl.ds(k * width, width)], ref.at[:, to]) for k, ref in enumerate((bg_hbm, bu_hbm))], both_sem, slot)

    def chunk(c):
        slot = turn(c)

        @pl.when(c == 0)
        def _():
            for one in loads:
                one.wait()
            for one in later_loads:
                one.start()

        @pl.when(c == 1)
        def _():
            for one in later_loads:
                one.wait()

        @pl.when(c >= BUFFERS)
        def _():
            for one in store_both(c - BUFFERS):
                one.wait()

        @pl.when(c == chunks // 2)
        def _():
            for copies in early:
                spread.pass_last(copies)

        down_chunk(c).wait()

        @pl.when(c + 1 < chunks)
        def _():
            down_chunk(c + 1).start()

        columns = pl.ds(pl.multiple_of(c * width, width), width)
        wg_c, wu_c, wd_c = wg[:, columns], wu[:, columns], wd[slot]
        for at in range(0, tokens, MB):
            rows = slice(at, at + MB)
            hidden, by_gate, by_up = by_units(dot(a[rows], wg_c), dot(a[rows], wu_c), dot(dy[rows], wd_c, TRANSPOSED))
            hidden_t[columns, rows] = hidden.astype(BF16).T
            both[slot, rows, :width] = by_gate.astype(BF16)
            both[slot, rows, width:] = by_up.astype(BF16)
        wide_packet(exchange, c, a_t, both.at[slot])
        for one in store_both(c):
            one.start()
        exchange.move(c, 0, chunks)

    repeat(0, chunks, chunk)
    for c in range(chunks - BUFFERS, chunks):
        for one in store_both(c):
            one.wait()

    tile_rows = 256
    tiles = tokens // tile_rows
    split_at = a_t.shape[1]

    def tile_loads(t):
        slot = turn(t)
        rows = pl.ds(pl.multiple_of(t * tile_rows, tile_rows), tile_rows)
        pairs = [(h_in.at[rows], h_tile.at[slot])]
        for k, src in enumerate((bg_hbm, bu_hbm)):
            to = pl.ds(pl.multiple_of((slot * 2 + k) * tile_rows, tile_rows), tile_rows)
            pairs.append((src.at[rows, pl.ds(0, split_at)], a_t.at[to]))
            pairs.append((src.at[rows, pl.ds(split_at, ff - split_at)], a.at[to, pl.ds(0, ff - split_at)]))
        return local_copies(pairs, tile_sem, slot)

    def tile_store(t):
        slot = turn(t)
        return pltpu.make_async_copy(by_tile.at[slot], by_h.at[pl.ds(pl.multiple_of(t * tile_rows, tile_rows), tile_rows)], by_sem.at[slot])

    for one in tile_loads(0):
        one.start()

    def tile(step):
        t = step - chunks

        @pl.when(t < downs)
        def _():
            tall_packet(exchange, step, chunks, hidden_t, dy)

        exchange.move(step, chunks, chunks + tiles)
        slot = turn(t)
        for one in tile_loads(t):
            one.wait()

        @pl.when(t + 1 < tiles)
        def _():
            for one in tile_loads(t + 1):
                one.start()

        @pl.when(t >= BUFFERS)
        def _():
            tile_store(t - BUFFERS).wait()

        total = None
        for k, w in enumerate((wg, wu)):
            at = pl.ds(pl.multiple_of((slot * 2 + k) * tile_rows, tile_rows), tile_rows)
            term = dot(a_t[at], w[:, :split_at], TRANSPOSED) + dot(a[at, : ff - split_at], w[:, split_at:], TRANSPOSED)
            total = term if total is None else total + term
        rows = pl.ds(pl.multiple_of(t * tile_rows, tile_rows), tile_rows)
        by_tile[slot] = (dy[rows].astype(F32) + by_norm(h_tile[slot], total)).astype(BF16)
        tile_store(t).start()

    repeat(chunks, chunks + tiles, tile)
    exchange.finish(chunks + tiles, chunks + downs)
    for t in range(tiles - BUFFERS, tiles):
        tile_store(t).wait()
    for copies in early:
        spread.end_far(copies)


def top_layer(n, a, a_t, h, dy, w_gate, w_up, w_down, near):
    tokens, d = a.shape
    ff = w_gate.shape[2]
    width = 256
    anywhere, inside = pl.BlockSpec(memory_space=pl.ANY), pl.BlockSpec(memory_space=pltpu.VMEM)
    dma = pltpu.SemaphoreType.DMA
    return pl.pallas_call(
        functools.partial(top_kernel, n),
        in_specs=[anywhere] * (7 + len(near)),
        out_specs=[inside] * 4 + [anywhere] * (3 + len(near)),
        out_shape=[
            jax.ShapeDtypeStruct((d // n, ff), BF16),
            jax.ShapeDtypeStruct((d // n, ff), BF16),
            jax.ShapeDtypeStruct((ff // n, d), BF16),
            jax.ShapeDtypeStruct((8, 128), F32),
            jax.ShapeDtypeStruct((tokens, d), BF16),
            jax.ShapeDtypeStruct((tokens, ff), BF16),
            jax.ShapeDtypeStruct((tokens, ff), BF16),
            *[jax.ShapeDtypeStruct(t.shape, t.dtype) for t in near],
        ],
        scratch_shapes=[
            *Spread.semaphores(len(near)),
            *[pltpu.VMEM(t, BF16) for t in ((tokens, d), (d, tokens), (tokens, d), (d, ff), (d, ff), (ff, tokens))],
            *[pltpu.VMEM((BUFFERS, *t), BF16) for t in ((width, d), (tokens, 2 * width), (width, d), (width, d))],
            dma((7,)), dma((BUFFERS,)), dma((2, BUFFERS)), dma((5, BUFFERS)), dma((BUFFERS,)),
            *Exchange.scratch(n, ff // n // 2, 2 * width, TOP_LAGS),
        ],
        compiler_params=pltpu.CompilerParams(collective_id=2, has_side_effects=True, vmem_limit_bytes=ALL_VMEM),
        name="top",
    )(a, a_t, h, dy, w_gate, w_up, w_down, *near)


def bottom_kernel(n, *refs):
    some = len(EARLY)
    ins, summed, (g_gate, g_up, g_down, squares), near, (send, recv), refs = split(refs, 6, some, 4, some, 2)
    by_in, ht_in, at_in, gate_in, up_in, w_down = ins
    spread = Spread(n, send, recv)
    (by, hidden_t, a_t, wd, gate, up, both, load_sem, unit_sem), refs = split(refs, 9)
    tokens, d = by.shape
    ff = hidden_t.shape[0]
    width = 256
    chunks = ff // width
    downs = 4
    wide_rows, down_rows = d // n, ff // n // 2
    exchange = Exchange(
        n, refs,
        (
            (0, downs, down_rows, keep_down(0, g_down, down_rows, 2 * width, squares)),
            (downs, downs + chunks, wide_rows, keep_columns(downs, g_gate, g_up, width, squares)),
        ),
        BOTTOM_LAGS,
    )
    share = ff // n
    halves = lambda ref, k: ref.at[:, pl.ds(k * 2 * width, 2 * width)]
    pairs = [(halves(by_in, 0), halves(by, 0))]
    for k in range(2):
        for to in range(n):
            rows = pl.ds(to * share + k * down_rows, down_rows)
            pairs.append((ht_in.at[rows], hidden_t.at[rows]))
    pairs += [(halves(by_in, 1), halves(by, 1)), (at_in, a_t)]
    loads = local_copies(pairs, load_sem)

    def chunk_loads(c):
        slot = turn(c)
        columns = pl.ds(pl.multiple_of(c * width, width), width)
        pairs = [(w_down.at[0, columns], wd.at[slot]), (gate_in.at[:, columns], gate.at[slot]), (up_in.at[:, columns], up.at[slot])]
        return local_copies(pairs, unit_sem, slot)

    first, second, third = split(loads, 1 + n, n)
    third += chunk_loads(0)
    for one in first:
        one.start()
    squares[...] = jnp.zeros_like(squares)
    exchange.barrier()

    early = []
    for number, (src, dst) in enumerate(zip(summed, near, strict=True)):
        some = dst.shape[1]
        own = src.at[pl.ds(src.shape[0] - some, some)]
        early.append(spread.copies(number, lambda owner, columns, dst=dst: dst.at[owner, :, columns], dst.shape[2], own))
    for copies in early:
        spread.start(copies)

    def down(step):
        @pl.when(step == 0)
        def _():
            for one in first:
                one.wait()
            for one in second:
                one.start()

        @pl.when(step == 1)
        def _():
            for one in second:
                one.wait()
            for one in third:
                one.start()

        @pl.when(step == 2)
        def _():
            for one in third[:2]:
                one.wait()

        down_packet(exchange, step, 0, hidden_t, by)
        exchange.move(step, 0, downs)

    repeat(0, downs, down)

    def chunk(step):
        c = step - downs
        slot = turn(c)
        for one in chunk_loads(c):
            one.wait()

        @pl.when(c + 1 < chunks)
        def _():
            for one in chunk_loads(c + 1):
                one.start()

        wd_c = wd[slot]
        for at in range(0, tokens, MB):
            rows = slice(at, at + MB)
            _, by_gate, by_up = by_units(gate[slot, rows], up[slot, rows], dot(by[rows], wd_c, TRANSPOSED))
            both[rows, :width] = by_gate.astype(BF16)
            both[rows, width:] = by_up.astype(BF16)
        wide_packet(exchange, step, a_t, both)
        exchange.move(step, downs, downs + chunks)

    repeat(downs, downs + chunks, chunk)
    exchange.finish(downs + chunks, downs + chunks)
    for copies in early:
        spread.end_near(copies)


def bottom_layer(n, by, hidden_t, a_t, gate, up, w_down, summed):
    tokens, d = by.shape
    ff = hidden_t.shape[0]
    width = 256
    anywhere, inside = pl.BlockSpec(memory_space=pl.ANY), pl.BlockSpec(memory_space=pltpu.VMEM)
    dma = pltpu.SemaphoreType.DMA
    return pl.pallas_call(
        functools.partial(bottom_kernel, n),
        in_specs=[anywhere] * (6 + len(summed)),
        out_specs=[inside] * 4 + [anywhere] * len(summed),
        out_shape=[
            jax.ShapeDtypeStruct((d // n, ff), BF16),
            jax.ShapeDtypeStruct((d // n, ff), BF16),
            jax.ShapeDtypeStruct((ff // n, d), BF16),
            jax.ShapeDtypeStruct((8, 128), F32),
            *[jax.ShapeDtypeStruct((n, some, ff), BF16) for _, some in EARLY],
        ],
        scratch_shapes=[
            *Spread.semaphores(len(summed)),
            *[pltpu.VMEM(t, BF16) for t in ((tokens, d), (ff, tokens), (d, tokens), (BUFFERS, width, d))],
            *[pltpu.VMEM((BUFFERS, tokens, width), F32)] * 2, pltpu.VMEM((tokens, 2 * width), BF16),
            dma((3 + 2 * n,)), dma((3, BUFFERS)),
            *Exchange.scratch(n, ff // n // 2, 2 * width, BOTTOM_LAGS),
        ],
        compiler_params=pltpu.CompilerParams(collective_id=3, has_side_effects=True, vmem_limit_bytes=ALL_VMEM),
        name="bottom",
    )(by, hidden_t, a_t, gate, up, w_down, *summed)


def solution(mesh):
    n = mesh.shape["dp"]

    def step(x, dy, w_gate, w_up, w_down, *moments):
        m, v = split(moments, WEIGHTS)
        gate, up, hidden_t, a_t, h, next_a, next_a_t, *early = layer_0(n, x[0], w_gate, w_up, w_down, m, v)
        top = top_layer(n, next_a, next_a_t, h, dy[0], w_gate, w_up, w_down, early)
        top, (squares_1, by_h, _, _), far = split(top, WEIGHTS, 4)
        bottom = bottom_layer(n, by_h, hidden_t, a_t, gate, up, w_down, [top[i] for i, _ in EARLY])
        bottom, (squares_0,), near = split(bottom, WEIGHTS, 1)
        gradients = list(zip(bottom, top, strict=True))
        return tuple(finish(n, gradients, (squares_0, squares_1), (w_gate, w_up, w_down), m, v, (*early, *far, *near)))

    sharded = P(None, "dp", None)
    return jax.shard_map(
        step,
        mesh=mesh,
        in_specs=(P(("rep", "dp")), P(("rep", "dp")), P(), P(), P(), *[sharded] * 6),
        out_specs=(*[P("rep")] * 3, *[P("rep", "dp")] * 6),
        check_vma=False,
    )
```

```python
import functools

import jax
import jax.numpy as jnp
from jax import lax
from jax.experimental import pallas as pl
from jax.experimental.pallas import tpu as pltpu
from jax.sharding import PartitionSpec as P

MESH = pl.DeviceIdType.MESH
F32, BF16 = jnp.float32, jnp.bfloat16
CORES = 2
BUFFERS = 2
WEIGHTS = 3
MIB = 2**20
ALL_VMEM = 67043328
TRANSPOSED = ((1,), (1,))


def turn(t):
    return lax.rem(t, BUFFERS)


def repeat(low, high, body):
    def step(i, nothing):
        body(i)
        return nothing

    lax.fori_loop(low, high, step, None)


def split(refs, *sizes):
    left = iter(refs)
    runs = [[next(left) for _ in range(size)] for size in sizes]
    return *runs, list(left)


def local_copies(pairs, sem, *at):
    return [pltpu.make_async_copy(src, dst, sem.at[(k, *at)]) for k, (src, dst) in enumerate(pairs)]


def places(axis, n):
    me = lax.axis_index(axis)
    chips = n // CORES
    core, chip = lax.rem(me, CORES), lax.div(me, CORES)
    at = lambda away: lax.rem(chip + away, chips) * CORES + core
    return me, core, me + 1 - 2 * core, at(1), at(chips - 1), at(2)


class Spread:
    KINDS = 9

    def __init__(self, n, send, recv):
        self.send, self.recv = send, recv
        self.me, _, self.partner, self.after, self.before, self.across = places("dp", n)

    @staticmethod
    def semaphores(pieces):
        return [pltpu.SemaphoreType.DMA((Spread.KINDS, pieces))] * 2

    def barrier(self):
        barrier = pltpu.get_barrier_semaphore()
        for peer in (self.partner, self.after, self.before):
            pl.semaphore_signal(barrier, inc=1, device_id={"dp": peer}, device_id_type=MESH)
        pl.semaphore_wait(barrier, 3)

    def copies(self, number, place, width, own=None, far=None):
        far = far or place
        every, left, right = pl.ds(0, width), pl.ds(0, width // 2), pl.ds(width // 2, width // 2)

        class Copies(dict):
            def __missing__(_, kind):
                to, src, dst = routes[kind]
                sems = (t.at[list(routes).index(kind), number] for t in (self.send, self.recv))
                return pltpu.make_async_remote_copy(src, dst, *sems, device_id={"dp": to}, device_id_type=MESH)

        me, after, before, across = self.me, self.after, self.before, self.across
        own = place(me, every) if own is None else own
        routes = {
            "after": (after, own, place(me, every)),
            "before": (before, own, place(me, every)),
            "partner": (self.partner, own, place(me, every)),
            "on": (after, place(before, left), far(before, left)),
            "back": (before, place(after, right), far(after, right)),
            "partner_before": (self.partner, place(before, every), far(before, every)),
            "partner_after": (self.partner, place(after, every), far(after, every)),
            "partner_left": (self.partner, far(across, left), far(across, left)),
            "partner_right": (self.partner, far(across, right), far(across, right)),
        }
        return Copies()

    @staticmethod
    def start(copies):
        for kind in ("after", "before", "partner"):
            copies[kind].start()

    @staticmethod
    def pass_on(copies):
        copies["after"].wait_recv()
        copies["on"].start()
        copies["partner_before"].start()
        copies["before"].wait_recv()
        copies["back"].start()
        copies["partner_after"].start()

    @staticmethod
    def pass_last(copies):
        copies["on"].wait_recv()
        copies["partner_left"].start()
        copies["back"].wait_recv()
        copies["partner_right"].start()

    @staticmethod
    def end(copies):
        for kind in ("partner", "partner_before", "partner_after", "partner_left", "partner_right"):
            copies[kind].wait_recv()
        for kind in (*Spread.NEAR, *Spread.THEN, *Spread.LAST):
            copies[kind].wait_send()


    NEAR, THEN, LAST = ("after", "before", "partner"), ("on", "back", "partner_before", "partner_after"), ("partner_left", "partner_right")

    @staticmethod
    def end_near(copies):
        for kind in Spread.NEAR:
            copies[kind].wait()

    @staticmethod
    def start_far(copies):
        for kind in Spread.THEN:
            copies[kind].start()

    @staticmethod
    def end_far(copies):
        for kind in Spread.THEN:
            copies[kind].wait_send()
        for kind in (*Spread.THEN[2:], *Spread.LAST):
            copies[kind].wait_recv()
        for kind in Spread.LAST:
            copies[kind].wait_send()


EARLY = ((0, 32), (1, 32))


def finish_kernel(n, count, layers, pieces, *refs):
    some = len(EARLY)
    squares, *g_in = zip(*[iter(refs[: layers + layers * WEIGHTS])] * layers)
    refs = refs[layers + layers * WEIGHTS :]
    w_in, m_in, v_in, near_m, near_v, far_m, far_v, near_g, w, m, v, far_g, g, refs = split(
        refs, *[WEIGHTS] * 3, *[some] * 5, *[WEIGHTS] * 3, some, WEIGHTS
    )
    parts, m_tile, v_tile, g_tile, load_sem, early_sem, tile_sem, part_send, part_recv, send, recv = refs
    spread = Spread(n, send, recv)
    me = spread.me

    barrier = pltpu.get_barrier_semaphore()
    peers = [lax.rem(me + away, n) for away in range(1, n)]
    for peer in peers:
        pl.semaphore_signal(barrier, inc=1, device_id={"dp": peer}, device_id_type=MESH)

    def rows_of(i, owner, first, rows):
        return pl.ds(pl.multiple_of(owner * g[i].shape[1] + first, 16), rows)

    order = (2, 0, 1)
    loads = {}
    for i in order:
        rows = rows_of(i, me, 0, g[i].shape[1])
        pairs = [(w_in[i].at[:, rows], w[i].at[:, rows]), (m_in[i], m[i]), (v_in[i], v[i])]
        pairs += [(g_in[i][k], g[i].at[k]) for k in range(layers)]
        loads[i] = [pltpu.make_async_copy(src, dst, load_sem.at[i, k]) for k, (src, dst) in enumerate(pairs)]
    first_weight, *other_weights = order
    for one in loads[first_weight]:
        one.start()

    total = sum(t[...] for t in squares)
    parts[pl.ds(me, 1)] = total[None]
    early = []
    for k, (i, some) in enumerate(EARLY):
        near = lambda owner, columns, ref=near_g[k]: ref.at[owner, :, columns]
        far = lambda owner, columns, ref=far_g[k]: ref.at[owner, :, columns]
        early.append(spread.copies(len(pieces) + k, near, g[i].shape[2], None, far))
    pl.semaphore_wait(barrier, n - 1)
    part_copies = []
    for k, peer in enumerate(peers):
        part_copies.append(
            pltpu.make_async_remote_copy(
                parts.at[me], parts.at[me], part_send.at[k], part_recv.at[k], device_id={"dp": peer}, device_id_type=MESH
            )
        )
        part_copies[-1].start()
    for copies in early:
        spread.start_far(copies)
    for one in part_copies:
        one.wait_recv()
    every = parts[0]
    for k in range(1, n):
        every += parts[k]
    mean = jnp.sum(every, keepdims=True) / count
    factor = jnp.minimum(1.0, 0.5 * lax.rsqrt(mean + 1e-30))

    def stepped(grad, m_old, v_old, w_old):
        grad = grad.astype(F32) * factor
        m_new = 0.9 * m_old + 0.1 * grad
        v_new = 0.95 * v_old + 0.05 * grad * grad
        w_old = w_old.astype(F32)
        return m_new, v_new, (w_old - 0.02 * (m_new * lax.rsqrt(v_new + 1e-8) + 0.1 * w_old)).astype(BF16)

    step_rows, width = 16, 256

    def adamw(i, layer, first, rows):
        def body(step):
            start = first + step * step_rows
            at = (layer, pl.ds(pl.multiple_of(start, 16), step_rows), slice(None))
            mine = (layer, rows_of(i, me, start, step_rows), slice(None))
            m[i][at], v[i][at], w[i][mine] = stepped(g[i][at], m[i][at], v[i][at], w[i][mine])

        repeat(0, rows // step_rows, body)

    waited = set()

    def compute(i, layer, first, rows):
        if i not in waited:
            waited.add(i)
            for one in loads[i]:
                one.wait()
        adamw(i, layer, first, rows)

    made = []
    for number, (i, layer, first, rows) in enumerate(pieces):
        place = lambda owner, columns, i=i, layer=layer, first=first, rows=rows: w[i].at[layer, rows_of(i, owner, first, rows), columns]
        made.append(spread.copies(number, place, g[i].shape[2]))

    def own_piece(number):
        compute(*pieces[number])
        spread.start(made[number])

    other = lambda device: device + spread.partner - me
    units = []
    for k, (i, some) in enumerate(EARLY):
        near, far = (near_m[k], near_v[k], near_g[k]), (far_m[k], far_v[k], far_g[k])
        for refs, owners in (
            (near, (spread.partner, spread.after, spread.before)),
            (far, (other(spread.after), other(spread.before), spread.across, other(spread.across))),
        ):
            units += [(refs, i, owner, first, g[i].shape[1] - some) for owner in owners for first in range(0, some, step_rows)]

    def unit_loads(number):
        refs, _, owner, first, _ = units[number]
        slot = number % BUFFERS
        tiles = zip(refs, (m_tile, v_tile, g_tile), strict=True)
        return local_copies([(src.at[owner, pl.ds(first, step_rows)], dst.at[slot]) for src, dst in tiles], tile_sem, slot)

    def unit_rows(number):
        _, i, owner, first, start = units[number]
        return rows_of(i, owner, start + first, step_rows)

    last = layers - 1
    old_rows = local_copies(
        [tuple(t[i].at[last, unit_rows(number)] for t in (w_in, w)) for number, (_, i, _, _, _) in enumerate(units)], early_sem
    )

    def unit(number):
        (_, i, _, _, _), slot = units[number], number % BUFFERS
        if number + 1 < len(units):
            for one in unit_loads(number + 1):
                one.start()
        for one in (*unit_loads(number), old_rows[number]):
            one.wait()

        def body(step):
            columns = pl.ds(pl.multiple_of(step * width, width), width)
            its, at = (last, unit_rows(number), columns), (slot, slice(None), columns)
            *_, w[i][its] = stepped(g_tile[at], m_tile[at], v_tile[at], w[i][its])

        repeat(0, g[i].shape[-1] // width, body)

    own_piece(0)
    for i in other_weights:
        for one in loads[i]:
            one.start()
    for one in old_rows:
        one.start()
    total_pieces, done = len(pieces), 0
    for number in range(total_pieces + 2):
        if number + 1 < total_pieces:
            own_piece(number + 1)
        if number == 0:
            for copies in early:
                spread.pass_last(copies)
        if 1 <= number <= total_pieces:
            spread.pass_on(made[number - 1])
        if 2 <= number:
            spread.pass_last(made[number - 2])
        if number == 2:
            for copies in early:
                spread.end_far(copies)
            for one in unit_loads(0):
                one.start()
        if 3 <= number < total_pieces:
            for k in range(min(3, len(units) - done)):
                unit(done + k)
            done += min(3, len(units) - done)
        if number == 3:
            for i, some in EARLY:
                compute(i, last, g[i].shape[1] - some, some)
    for k in range(done, len(units)):
        unit(k)
    for copies in made:
        spread.end(copies)
    for one in part_copies:
        one.wait_send()


def store_kernel(*refs):
    *refs, sem = refs
    some = len(refs) // 2
    copies = local_copies([(refs[k], refs[some + k]) for k in range(some)], sem)
    for one in copies:
        one.start()
    for one in copies:
        one.wait()


def early_shapes(n, blocks, dtype, times=1, kind=jax.ShapeDtypeStruct):
    return [kind((n, some, blocks[i][0].shape[-1]), dtype) for _ in range(times) for i, some in EARLY]


def finish(n, gradients, squares, weights, m, v, early):
    count = float(sum(w.size for w in weights))
    layers = len(gradients[0])
    pieces = []
    for i in (2, 0, 1):
        rows, _ = gradients[i][0].shape
        for layer in range(layers):
            half = rows // 2
            cuts = [half, half]
            if (i, layer) == (2, 0):
                cuts = [48, half - 48, half]
            elif layer == layers - 1 and i in dict(EARLY):
                rest = half - dict(EARLY)[i]
                cuts = [half + rest - 16, 16] if i == 1 else [half + rest]
            for cut in cuts:
                pieces.append((i, layer, sum(p[3] for p in pieces if p[:2] == (i, layer)), cut))
    anywhere, inside = pl.BlockSpec(memory_space=pl.ANY), pl.BlockSpec(memory_space=pltpu.VMEM)
    dma = pltpu.SemaphoreType.DMA
    results = [*weights, *m, *v]
    tile = lambda dtype: pltpu.VMEM((BUFFERS, 16, max(gradients[i][0].shape[1] for i, _ in EARLY)), dtype)
    ready = pl.pallas_call(
        functools.partial(finish_kernel, n, count, layers, tuple(pieces)),
        out_shape=[pltpu.VMEM(t.shape, t.dtype) for t in results]
        + early_shapes(n, gradients, BF16),
        in_specs=[inside] * layers + [anywhere] * (WEIGHTS * layers + len(results) + len(early)),
        out_specs=[inside] * len(results) + [anywhere] * len(EARLY),
        scratch_shapes=[
            *[pltpu.VMEM((layers, *one[0].shape), BF16) for one in gradients],
            pltpu.VMEM((n, 8, 128), F32), tile(F32), tile(F32), tile(BF16),
            dma((WEIGHTS, layers + 3)), dma((sum(some for _, some in EARLY) // 16 * (n - 1),)), dma((3, BUFFERS)), *[dma((n - 1,))] * 2,
            *Spread.semaphores(len(pieces) + len(EARLY)),
        ],
        compiler_params=pltpu.CompilerParams(collective_id=4, has_side_effects=True, vmem_limit_bytes=8 * MIB),
        name="finish",
    )(*squares, *sum(gradients, ()), *weights, *m, *v, *early)[: len(results)]
    return pl.pallas_call(
        store_kernel,
        out_shape=[jax.ShapeDtypeStruct(t.shape, t.dtype) for t in results],
        in_specs=[inside] * len(results),
        out_specs=[anywhere] * len(results),
        scratch_shapes=[dma((len(results),))],
        compiler_params=pltpu.CompilerParams(vmem_limit_bytes=8 * MIB),
        name="store",
    )(*[pltpu.with_memory_space_constraint(t, pltpu.VMEM) for t in ready])


def dot(a, b, contract=((1,), (0,))):
    return lax.dot_general(a, b, (contract, ((), ())), preferred_element_type=F32)


def normed(h):
    wide = h.astype(F32)
    return (wide * lax.rsqrt(jnp.mean(wide * wide, -1, keepdims=True) + 1e-6)).astype(BF16)


def by_norm(h, by_a):
    wide = h.astype(F32)
    scale = lax.rsqrt(jnp.mean(wide * wide, -1, keepdims=True) + 1e-6)
    return scale * by_a - wide * (scale * scale * scale * jnp.mean(by_a * wide, -1, keepdims=True))


def by_units(gate, up, by_hidden):
    by_hidden = by_hidden.astype(BF16).astype(F32)
    s = jax.nn.sigmoid(gate)
    silu = gate * s
    return silu * up, by_hidden * up * (s + silu * (1.0 - s)), by_hidden * silu


def forward_kernel(n, *refs):
    (x_in, w_gate, w_up, w_down), moments, outs, early, refs = split(refs, 4, 2 * len(EARLY), 7, 2 * len(EARLY))
    gate_out, up_out, ht_out, at_out, h_out, b_out, bt_out = outs
    (wg, wu, wd, hidden, x, gate, up, hidden_t, a_t, h, b, b_t, w_sem, x_sem, sem, late_sem, send, recv) = refs
    spread = Spread(n, send, recv)
    rows = x.shape[1]
    tiles = x_in.shape[0] // rows
    ff = wg.shape[1]
    width = 256
    groups = [range(at, min(at + 3 * width, ff), width) for at in range(0, ff, 3 * width)]
    tall = lambda ref, t: ref.at[pl.ds(pl.multiple_of(t * rows, rows), rows)]
    wide = lambda ref, t: ref.at[:, pl.ds(pl.multiple_of(t * rows, rows), rows)]

    def load_x(t):
        return pltpu.make_async_copy(tall(x_in, t), x.at[lax.rem(t, x.shape[0])], x_sem.at[lax.rem(t, x.shape[0])])

    def stores(t, first):
        slot = turn(t)
        if first:
            pairs = [(gate, tall(gate_out, t)), (up, tall(up_out, t)), (hidden_t, wide(ht_out, t)), (a_t, wide(at_out, t))]
        else:
            pairs = [(h, tall(h_out, t)), (b, tall(b_out, t)), (b_t, wide(bt_out, t))]
        return local_copies([(src.at[slot], dst) for src, dst in pairs], sem if first else late_sem, slot)

    w_loads = []
    for k, group in enumerate(groups):
        columns = slice(group[0], group[-1] + width)
        w_loads.append([
            pltpu.make_async_copy(src.at[0, :, columns], dst.at[:, columns], w_sem.at[j, k]) for j, (src, dst) in enumerate(((w_gate, wg), (w_up, wu)))
        ])
    down_load = pltpu.make_async_copy(w_down.at[0], wd, w_sem.at[2, 0])
    for one in (load_x(0), *w_loads[0], *w_loads[1], load_x(1)):
        one.start()
    spread.barrier()
    pieces = []
    for number, (src, dst) in enumerate(zip(moments, early, strict=True)):
        some = dst.shape[1]
        own = src.at[src.shape[0] - 1, pl.ds(src.shape[1] - some, some)]
        pieces.append(spread.copies(number, lambda owner, columns, dst=dst: dst.at[owner, :, columns], dst.shape[2], own))
    for copies in pieces:
        spread.start(copies)

    def first_part(t, group, a):
        slot = turn(t)
        for at in group:
            columns = slice(at, at + width)
            g, u = dot(a, wg[:, columns]), dot(a, wu[:, columns])
            gate[slot, :, columns] = g
            up[slot, :, columns] = u
            units = (g * jax.nn.sigmoid(g) * u).astype(BF16)
            hidden[:, columns] = units
            hidden_t[slot, columns] = units.T

    def second_part(t):
        slot = turn(t)
        out = x[lax.rem(t, x.shape[0])] + dot(hidden[...], wd[...]).astype(BF16)
        h[slot] = out
        after = normed(out)
        b[slot] = after
        b_t[slot] = after.T

    def normed_tile(t):
        a = normed(x[lax.rem(t, x.shape[0])])
        a_t[turn(t)] = a.T
        return a

    load_x(0).wait()
    a = normed_tile(0)
    for k, group in enumerate(groups):
        for one in w_loads[k]:
            one.wait()
        for one in w_loads[k + 2] if k + 2 < len(groups) else ([down_load] if k + 2 == len(groups) else []):
            one.start()
        first_part(0, group, a)
    for one in stores(0, True):
        one.start()
    down_load.wait()

    def tile(t):
        load_x(t).wait()

        @pl.when(t + 1 < tiles)
        def _():
            load_x(t + 1).start()

        @pl.when(t >= BUFFERS)
        def _():
            for one in stores(t - BUFFERS, True):
                one.wait()

        @pl.when(t > BUFFERS)
        def _():
            for one in stores(t - 1 - BUFFERS, False):
                one.wait()

        a = normed_tile(t)
        second_part(t - 1)
        first_part(t, range(0, ff, width), a)
        for one in (*stores(t - 1, False), *stores(t, True)):
            one.start()

    repeat(1, tiles, tile)
    last = tiles - 1
    for one in stores(last - BUFFERS, False):
        one.wait()
    second_part(last)
    for one in stores(last, False):
        one.start()
    for copies in pieces:
        spread.end_near(copies)
    for t in (last - 1, last):
        for one in (*stores(t, True), *stores(t, False)):
            one.wait()


def layer_0(n, x, w_gate, w_up, w_down, m, v):
    tokens, d = x.shape
    ff = w_gate.shape[2]
    rows = 256
    anywhere = pl.BlockSpec(memory_space=pl.ANY)
    dma = pltpu.SemaphoreType.DMA
    vmem = lambda *shape: pltpu.VMEM(shape, BF16)
    return pl.pallas_call(
        functools.partial(forward_kernel, n),
        in_specs=[anywhere] * (4 + 2 * len(EARLY)),
        out_specs=[anywhere] * (7 + 2 * len(EARLY)),
        out_shape=[
            pltpu.HBM((tokens, ff), F32),
            pltpu.HBM((tokens, ff), F32),
            pltpu.HBM((ff, tokens), BF16),
            pltpu.HBM((d, tokens), BF16),
            pltpu.HBM((tokens, d), BF16),
            pltpu.HBM((tokens, d), BF16),
            pltpu.HBM((d, tokens), BF16),
            *early_shapes(n, m, F32, 2, pltpu.HBM),
        ],
        scratch_shapes=[
            vmem(d, ff), vmem(d, ff), vmem(ff, d), vmem(rows, ff), vmem(3, rows, d),
            *[pltpu.VMEM((BUFFERS, rows, ff), F32)] * 2, *[vmem(BUFFERS, *t) for t in ((ff, rows), (d, rows), (rows, d), (rows, d), (d, rows))],
            dma((WEIGHTS, 4)), dma((3,)), dma((4, BUFFERS)), dma((3, BUFFERS)), *Spread.semaphores(2 * len(EARLY)),
        ],
        compiler_params=pltpu.CompilerParams(collective_id=1, has_side_effects=True, vmem_limit_bytes=48 * MIB),
        name="forward",
    )(*[pltpu.with_memory_space_constraint(t, pltpu.HBM) for t in (x, w_gate, w_up, w_down, *[t[i] for t in (m, v) for i, _ in EARLY])])


class Exchange:
    def __init__(self, n, refs, kinds, lags):
        self.mine, self.pair, self.out2, self.out3, self.in2, self.in3, self.own, self.side, self.pair_sem, self.sem2, self.sem3 = refs
        self.kinds = kinds
        self.lags = lags
        self.me, self.core, self.partner, self.after, self.before, _ = places("dp", n)
        chips = n // CORES
        self.chip = lax.div(self.me, CORES)
        self.chip_after, self.chip_before, self.chip_across = (lax.rem(self.chip + k, chips) for k in (1, chips - 1, chips // 2))
        half = self.out3.shape[-1]
        self.left, self.right = slice(0, half), slice(half, 2 * half)

    @staticmethod
    def scratch(n, rows, width, lags):
        chips, half, dma = n // CORES, width // 2, pltpu.SemaphoreType.DMA
        _, two, three, four = lags
        slots1, slots2, slots3 = two + 3, 2 * (three - two) + 2, 2 * (four - three) + 2
        return [
            pltpu.VMEM((two + 1, chips, CORES, rows, width), BF16),
            pltpu.VMEM((slots1, chips, rows, width), BF16),
            pltpu.VMEM((2, three - two + 1, rows, width), BF16),
            pltpu.VMEM((2, four - three + 1, rows, half), BF16),
            pltpu.VMEM((2, slots2, rows, width), BF16),
            pltpu.VMEM((2, slots3, rows, half), BF16),
            pltpu.VMEM((four - two + 1, rows, width), F32),
            pltpu.VMEM((2, three - two + 1, rows, half), F32),
            dma((2, slots1)), dma((2, 2, slots2)), dma((2, 2, slots3)),
        ]

    def held(self, p):
        return lax.rem(p, self.mine.shape[0])

    def barrier(self):
        barrier = pltpu.get_barrier_semaphore()
        for peer in (self.partner, self.after, self.before):
            pl.semaphore_signal(barrier, inc=1, device_id={"dp": peer}, device_id_type=MESH)
        pl.semaphore_wait(barrier, 3)

    def copy1(self, p, rows):
        slot = lax.rem(p, self.pair.shape[0])
        return pltpu.make_async_remote_copy(
            self.mine.at[self.held(p), :, 1 - self.core, pl.ds(0, rows)], self.pair.at[slot, :, pl.ds(0, rows)],
            self.pair_sem.at[0, slot], self.pair_sem.at[1, slot], device_id={"dp": self.partner}, device_id_type=MESH,
        )

    def copies(self, p, rows, out, into, sem):
        slot = lax.rem(p, into.shape[1])
        return [
            pltpu.make_async_remote_copy(
                out.at[way, lax.rem(p, out.shape[1]), pl.ds(0, rows)], into.at[way, slot, pl.ds(0, rows)],
                sem.at[0, way, slot], sem.at[1, way, slot], device_id={"dp": to}, device_id_type=MESH,
            )
            for way, to in enumerate((self.after, self.before))
        ]

    def copies2(self, p, rows):
        return self.copies(p, rows, self.out2, self.in2, self.sem2)

    def copies3(self, p, rows):
        return self.copies(p, rows, self.out3, self.in3, self.sem3)

    def stage1(self, p, rows, _):
        self.copy1(p, rows).start()

    def stage2(self, p, rows, _):
        self.copy1(p, rows).wait()
        slot, own, side = (lax.rem(p, t.shape[k]) for t, k in ((self.out2, 1), (self.own, 0), (self.side, 1)))
        at = slice(0, rows)

        def of_chip(chip, columns):
            a = self.mine[self.held(p), chip, self.core, at, columns].astype(F32)
            return a + self.pair[lax.rem(p, self.pair.shape[0]), chip, at, columns].astype(F32)

        self.out2[0, slot, at, self.left] = of_chip(self.chip_across, self.left).astype(BF16)
        self.out2[0, slot, at, self.right] = of_chip(self.chip_after, self.right).astype(BF16)
        self.out2[1, slot, at, self.left] = of_chip(self.chip_before, self.left).astype(BF16)
        self.out2[1, slot, at, self.right] = of_chip(self.chip_across, self.right).astype(BF16)
        for one in self.copies2(p, rows):
            one.start()
        self.side[0, side, at] = of_chip(self.chip_after, self.left)
        self.side[1, side, at] = of_chip(self.chip_before, self.right)
        for columns in (self.left, self.right):
            self.own[own, at, columns] = of_chip(self.chip, columns)

    def stage3(self, p, rows, _):
        for one in self.copies2(p, rows):
            one.wait()
        slot, arrived, own, side = (lax.rem(p, t.shape[k]) for t, k in ((self.out3, 1), (self.in2, 1), (self.own, 0), (self.side, 1)))
        at = slice(0, rows)
        self.out3[0, slot, at] = (self.side[0, side, at] + self.in2[0, arrived, at, self.left].astype(F32)).astype(BF16)
        self.out3[1, slot, at] = (self.side[1, side, at] + self.in2[1, arrived, at, self.right].astype(F32)).astype(BF16)
        for one in self.copies3(p, rows):
            one.start()
        self.own[own, at, self.left] += self.in2[1, arrived, at, self.left].astype(F32)
        self.own[own, at, self.right] += self.in2[0, arrived, at, self.right].astype(F32)

    def stage4(self, p, rows, keep):
        for one in self.copies3(p, rows):
            one.wait()
        arrived, own = lax.rem(p, self.in3.shape[1]), lax.rem(p, self.own.shape[0])
        at = slice(0, rows)
        a = self.own[own, at, self.left] + self.in3[0, arrived, at].astype(F32)
        b = self.own[own, at, self.right] + self.in3[1, arrived, at].astype(F32)
        keep(p, a.astype(BF16), b.astype(BF16))

    def finish(self, step, packets):
        for step in range(step, packets + self.lags[-1]):
            self.move(step, step, step + 1)

    def move(self, step, low, high):
        for lag, stage in zip(self.lags, (self.stage1, self.stage2, self.stage3, self.stage4), strict=True):
            for first, end, rows, keep in self.kinds:
                if high - 1 - lag < first or low - lag >= end:
                    continue
                p = step - lag
                if low - lag >= first and high - 1 - lag < end:
                    stage(p, rows, keep)
                else:
                    pl.when((p >= first) & (p < end))(functools.partial(stage, p, rows, keep))


def add_squares(total, *blocks):
    for block in blocks:
        wide = block.astype(F32)
        wide = wide * wide
        rows, columns = wide.shape
        sums = [wide[r : r + 8, c : c + 128] for r in range(0, rows, 8) for c in range(0, columns, 128)]
        while len(sums) > 1:
            sums = [a + b for a, b in zip(sums[::2], sums[1::2])] + ([sums[-1]] if len(sums) % 2 else [])
        total[...] += sums[0]


def keep_columns(first, gate, up, width, squares):
    def keep(p, left, right):
        columns = pl.ds(pl.multiple_of((p - first) * width, width), width)
        gate[:, columns] = left
        up[:, columns] = right
        add_squares(squares, left, right)

    return keep


def keep_tall(first, down, rows, width, squares):
    def keep(p, left, right):
        columns = pl.ds(pl.multiple_of((p - first) * width, width), width)
        down[:rows, columns] = left
        down[rows:, columns] = right
        add_squares(squares, left, right)

    return keep


def keep_down(first, down, rows, width, squares):
    def keep(p, left, right):
        half = width // 2
        which = p - first
        at = pl.ds(pl.multiple_of(lax.rem(which, 2) * rows, 16), rows)
        start = lax.div(which, 2) * width
        down[at, pl.ds(pl.multiple_of(start, half), half)] = left
        down[at, pl.ds(pl.multiple_of(start + half, half), half)] = right
        add_squares(squares, left, right)

    return keep


def tall_packet(exchange, step, first, hidden_t, by_out):
    _, chips, cores, rows, width = exchange.mine.shape
    half = width // 2
    by_out = by_out[:, pl.ds(pl.multiple_of((step - first) * half, half), half)]
    for k in range(chips * cores):
        block = dot(hidden_t[2 * rows * k : 2 * rows * (k + 1), :], by_out).astype(BF16)
        for part in range(2):
            exchange.mine[exchange.held(step), k // cores, k % cores, :, part * half : (part + 1) * half] = block[part * rows : (part + 1) * rows]


def down_packet(exchange, step, first, hidden_t, by_out):
    n_rows = hidden_t.shape[0]
    _, chips, cores, rows, width = exchange.mine.shape
    which = step - first
    start = pl.multiple_of(lax.rem(which, 2) * rows, 16)
    columns = pl.ds(pl.multiple_of(lax.div(which, 2) * width, width), width)
    share = n_rows // (chips * cores)
    by_out = by_out[:, columns]
    for k in range(chips * cores):
        lhs = hidden_t[pl.ds(pl.multiple_of(k * share + start, 16), rows), :]
        exchange.mine[exchange.held(step), k // cores, k % cores] = dot(lhs, by_out).astype(BF16)


def wide_packet(exchange, step, a_t, by_both):
    _, chips, cores, _, width = exchange.mine.shape
    rows = a_t.shape[0] // (chips * cores)
    half = width // 2
    for k in range(2):
        columns = slice(k * half, k * half + half)
        block = dot(a_t[...], by_both[:, columns]).astype(BF16)
        exchange.mine[exchange.held(step), :, :, pl.ds(0, rows), columns] = block.reshape(chips, cores, rows, half)


MB = 1024
TOP_LAGS = (0, 1, 4, 6)
BOTTOM_LAGS = (0, 1, 4, 7)


def top_kernel(n, *refs):
    several = 2 * len(EARLY)
    ins, near, outs, far, (send, recv), refs = split(refs, 7, several, 7, several, 2)
    a_in, at_in, h_in, dy, w_gate, w_up, w_down = ins
    g_gate, g_up, g_down, squares, by_h, bg_hbm, bu_hbm = outs
    spread = Spread(n, send, recv)
    (a, a_t, wg, wu, hidden_t, wd, both, h_tile, by_tile, load_sem, wd_sem, both_sem, tile_sem, by_sem), refs = split(refs, 14)
    tokens, d = a.shape
    ff = wg.shape[1]
    width = 256
    chunks = ff // width
    downs = 4
    wide_rows, down_rows = d // n, ff // n // 2
    exchange = Exchange(
        n, refs,
        (
            (0, chunks, wide_rows, keep_columns(0, g_gate, g_up, width, squares)),
            (chunks, chunks + downs, down_rows, keep_tall(chunks, g_down, down_rows, width, squares)),
        ),
        TOP_LAGS,
    )
    layer = w_gate.shape[0] - 1
    first, rest = pl.ds(0, width), pl.ds(width, ff - width)
    columns_of = lambda columns: [(src.at[layer, :, columns], dst.at[:, columns]) for src, dst in ((w_gate, wg), (w_up, wu))]
    loads = local_copies([(a_in, a), (at_in, a_t), *columns_of(first), *columns_of(rest)], load_sem)
    def down_chunk(c):
        slot = turn(c)
        return pltpu.make_async_copy(w_down.at[layer, pl.ds(pl.multiple_of(c * width, width), width)], wd.at[slot], wd_sem.at[slot])

    loads, later_loads = split(loads, 4)
    for one in (*loads, down_chunk(0)):
        one.start()
    squares[...] = jnp.zeros_like(squares)
    exchange.barrier()

    early = []
    for number, (src, dst) in enumerate(zip(near, far, strict=True)):
        places = [lambda owner, columns, ref=ref: ref.at[owner, :, columns] for ref in (src, dst)]
        early.append(spread.copies(number, places[0], src.shape[2], None, places[1]))
    for copies in early:
        spread.start_far(copies)

    def store_both(c):
        slot = turn(c)
        to = pl.ds(pl.multiple_of(c * width, width), width)
        return local_copies([(both.at[slot, :, pl.ds(k * width, width)], ref.at[:, to]) for k, ref in enumerate((bg_hbm, bu_hbm))], both_sem, slot)

    def chunk(c):
        slot = turn(c)

        @pl.when(c == 0)
        def _():
            for one in loads:
                one.wait()
            for one in later_loads:
                one.start()

        @pl.when(c == 1)
        def _():
            for one in later_loads:
                one.wait()

        @pl.when(c >= BUFFERS)
        def _():
            for one in store_both(c - BUFFERS):
                one.wait()

        @pl.when(c == chunks // 2)
        def _():
            for copies in early:
                spread.pass_last(copies)

        down_chunk(c).wait()

        @pl.when(c + 1 < chunks)
        def _():
            down_chunk(c + 1).start()

        columns = pl.ds(pl.multiple_of(c * width, width), width)
        wg_c, wu_c, wd_c = wg[:, columns], wu[:, columns], wd[slot]
        for at in range(0, tokens, MB):
            rows = slice(at, at + MB)
            hidden, by_gate, by_up = by_units(dot(a[rows], wg_c), dot(a[rows], wu_c), dot(dy[rows], wd_c, TRANSPOSED))
            hidden_t[columns, rows] = hidden.astype(BF16).T
            both[slot, rows, :width] = by_gate.astype(BF16)
            both[slot, rows, width:] = by_up.astype(BF16)
        wide_packet(exchange, c, a_t, both.at[slot])
        for one in store_both(c):
            one.start()
        exchange.move(c, 0, chunks)

    repeat(0, chunks, chunk)
    for c in range(chunks - BUFFERS, chunks):
        for one in store_both(c):
            one.wait()

    tile_rows = 256
    tiles = tokens // tile_rows
    split_at = a_t.shape[1]

    def tile_loads(t):
        slot = turn(t)
        rows = pl.ds(pl.multiple_of(t * tile_rows, tile_rows), tile_rows)
        pairs = [(h_in.at[rows], h_tile.at[slot])]
        for k, src in enumerate((bg_hbm, bu_hbm)):
            to = pl.ds(pl.multiple_of((slot * 2 + k) * tile_rows, tile_rows), tile_rows)
            pairs.append((src.at[rows, pl.ds(0, split_at)], a_t.at[to]))
            pairs.append((src.at[rows, pl.ds(split_at, ff - split_at)], a.at[to, pl.ds(0, ff - split_at)]))
        return local_copies(pairs, tile_sem, slot)

    def tile_store(t):
        slot = turn(t)
        return pltpu.make_async_copy(by_tile.at[slot], by_h.at[pl.ds(pl.multiple_of(t * tile_rows, tile_rows), tile_rows)], by_sem.at[slot])

    for one in tile_loads(0):
        one.start()

    def tile(step):
        t = step - chunks

        @pl.when(t < downs)
        def _():
            tall_packet(exchange, step, chunks, hidden_t, dy)

        exchange.move(step, chunks, chunks + tiles)
        slot = turn(t)
        for one in tile_loads(t):
            one.wait()

        @pl.when(t + 1 < tiles)
        def _():
            for one in tile_loads(t + 1):
                one.start()

        @pl.when(t >= BUFFERS)
        def _():
            tile_store(t - BUFFERS).wait()

        total = None
        for k, w in enumerate((wg, wu)):
            at = pl.ds(pl.multiple_of((slot * 2 + k) * tile_rows, tile_rows), tile_rows)
            term = dot(a_t[at], w[:, :split_at], TRANSPOSED) + dot(a[at, : ff - split_at], w[:, split_at:], TRANSPOSED)
            total = term if total is None else total + term
        rows = pl.ds(pl.multiple_of(t * tile_rows, tile_rows), tile_rows)
        by_tile[slot] = (dy[rows].astype(F32) + by_norm(h_tile[slot], total)).astype(BF16)
        tile_store(t).start()

    repeat(chunks, chunks + tiles, tile)
    exchange.finish(chunks + tiles, chunks + downs)
    for t in range(tiles - BUFFERS, tiles):
        tile_store(t).wait()
    for copies in early:
        spread.end_far(copies)


def top_layer(n, a, a_t, h, dy, w_gate, w_up, w_down, near):
    tokens, d = a.shape
    ff = w_gate.shape[2]
    width = 256
    anywhere, inside = pl.BlockSpec(memory_space=pl.ANY), pl.BlockSpec(memory_space=pltpu.VMEM)
    dma = pltpu.SemaphoreType.DMA
    return pl.pallas_call(
        functools.partial(top_kernel, n),
        in_specs=[*[anywhere] * 3, inside, *[anywhere] * (3 + len(near))],
        out_specs=[inside] * 4 + [anywhere] * (3 + len(near)),
        out_shape=[
            jax.ShapeDtypeStruct((d // n, ff), BF16),
            jax.ShapeDtypeStruct((d // n, ff), BF16),
            jax.ShapeDtypeStruct((ff // n, d), BF16),
            jax.ShapeDtypeStruct((8, 128), F32),
            jax.ShapeDtypeStruct((tokens, d), BF16),
            jax.ShapeDtypeStruct((tokens, ff), BF16),
            jax.ShapeDtypeStruct((tokens, ff), BF16),
            *[jax.ShapeDtypeStruct(t.shape, t.dtype) for t in near],
        ],
        scratch_shapes=[
            *Spread.semaphores(len(near)),
            *[pltpu.VMEM(t, BF16) for t in ((tokens, d), (d, tokens), (d, ff), (d, ff), (ff, tokens))],
            *[pltpu.VMEM((BUFFERS, *t), BF16) for t in ((width, d), (tokens, 2 * width), (width, d), (width, d))],
            dma((6,)), dma((BUFFERS,)), dma((2, BUFFERS)), dma((5, BUFFERS)), dma((BUFFERS,)),
            *Exchange.scratch(n, ff // n // 2, 2 * width, TOP_LAGS),
        ],
        compiler_params=pltpu.CompilerParams(collective_id=2, has_side_effects=True, vmem_limit_bytes=ALL_VMEM - 9 * MIB // 2),
        name="top",
    )(a, a_t, h, pltpu.with_memory_space_constraint(dy, pltpu.VMEM), w_gate, w_up, w_down, *near)


def bottom_kernel(n, *refs):
    some = len(EARLY)
    ins, summed, (g_gate, g_up, g_down, squares), near, (send, recv), refs = split(refs, 6, some, 4, some, 2)
    by_in, ht_in, at_in, gate_in, up_in, w_down = ins
    spread = Spread(n, send, recv)
    (by, hidden_t, a_t, wd, gate, up, both, load_sem, unit_sem), refs = split(refs, 9)
    tokens, d = by.shape
    ff = hidden_t.shape[0]
    width = 256
    chunks = ff // width
    downs = 4
    wide_rows, down_rows = d // n, ff // n // 2
    exchange = Exchange(
        n, refs,
        (
            (0, downs, down_rows, keep_down(0, g_down, down_rows, 2 * width, squares)),
            (downs, downs + chunks, wide_rows, keep_columns(downs, g_gate, g_up, width, squares)),
        ),
        BOTTOM_LAGS,
    )
    share = ff // n
    halves = lambda ref, k: ref.at[:, pl.ds(k * 2 * width, 2 * width)]
    pairs = [(halves(by_in, 0), halves(by, 0))]
    for k in range(2):
        for to in range(n):
            rows = pl.ds(to * share + k * down_rows, down_rows)
            pairs.append((ht_in.at[rows], hidden_t.at[rows]))
    pairs += [(halves(by_in, 1), halves(by, 1)), (at_in, a_t)]
    loads = local_copies(pairs, load_sem)

    def chunk_loads(c):
        slot = turn(c)
        columns = pl.ds(pl.multiple_of(c * width, width), width)
        pairs = [(w_down.at[0, columns], wd.at[slot]), (gate_in.at[:, columns], gate.at[slot]), (up_in.at[:, columns], up.at[slot])]
        return local_copies(pairs, unit_sem, slot)

    first, second, third = split(loads, 1 + n, n)
    third += chunk_loads(0)
    for one in first:
        one.start()
    squares[...] = jnp.zeros_like(squares)
    exchange.barrier()

    early = []
    for number, (src, dst) in enumerate(zip(summed, near, strict=True)):
        some = dst.shape[1]
        own = src.at[pl.ds(src.shape[0] - some, some)]
        early.append(spread.copies(number, lambda owner, columns, dst=dst: dst.at[owner, :, columns], dst.shape[2], own))
    for copies in early:
        spread.start(copies)

    def down(step):
        @pl.when(step == 0)
        def _():
            for one in first:
                one.wait()
            for one in second:
                one.start()

        @pl.when(step == 1)
        def _():
            for one in second:
                one.wait()
            for one in third:
                one.start()

        @pl.when(step == 2)
        def _():
            for one in third[:2]:
                one.wait()

        down_packet(exchange, step, 0, hidden_t, by)
        exchange.move(step, 0, downs)

    repeat(0, downs, down)

    def chunk(step):
        c = step - downs
        slot = turn(c)
        for one in chunk_loads(c):
            one.wait()

        @pl.when(c + 1 < chunks)
        def _():
            for one in chunk_loads(c + 1):
                one.start()

        wd_c = wd[slot]
        for at in range(0, tokens, MB):
            rows = slice(at, at + MB)
            _, by_gate, by_up = by_units(gate[slot, rows], up[slot, rows], dot(by[rows], wd_c, TRANSPOSED))
            both[rows, :width] = by_gate.astype(BF16)
            both[rows, width:] = by_up.astype(BF16)
        wide_packet(exchange, step, a_t, both)
        exchange.move(step, downs, downs + chunks)

    repeat(downs, downs + chunks, chunk)
    exchange.finish(downs + chunks, downs + chunks)
    for copies in early:
        spread.end_near(copies)


def bottom_layer(n, by, hidden_t, a_t, gate, up, w_down, summed):
    tokens, d = by.shape
    ff = hidden_t.shape[0]
    width = 256
    anywhere, inside = pl.BlockSpec(memory_space=pl.ANY), pl.BlockSpec(memory_space=pltpu.VMEM)
    dma = pltpu.SemaphoreType.DMA
    return pl.pallas_call(
        functools.partial(bottom_kernel, n),
        in_specs=[anywhere] * (6 + len(summed)),
        out_specs=[inside] * 4 + [anywhere] * len(summed),
        out_shape=[
            jax.ShapeDtypeStruct((d // n, ff), BF16),
            jax.ShapeDtypeStruct((d // n, ff), BF16),
            jax.ShapeDtypeStruct((ff // n, d), BF16),
            jax.ShapeDtypeStruct((8, 128), F32),
            *[jax.ShapeDtypeStruct((n, some, ff), BF16) for _, some in EARLY],
        ],
        scratch_shapes=[
            *Spread.semaphores(len(summed)),
            *[pltpu.VMEM(t, BF16) for t in ((tokens, d), (ff, tokens), (d, tokens), (BUFFERS, width, d))],
            *[pltpu.VMEM((BUFFERS, tokens, width), F32)] * 2, pltpu.VMEM((tokens, 2 * width), BF16),
            dma((3 + 2 * n,)), dma((3, BUFFERS)),
            *Exchange.scratch(n, ff // n // 2, 2 * width, BOTTOM_LAGS),
        ],
        compiler_params=pltpu.CompilerParams(collective_id=3, has_side_effects=True, vmem_limit_bytes=ALL_VMEM),
        name="bottom",
    )(by, hidden_t, a_t, gate, up, w_down, *summed)


def solution(mesh):
    n = mesh.shape["dp"]

    def step(x, dy, w_gate, w_up, w_down, *moments):
        m, v = split(moments, WEIGHTS)
        gate, up, hidden_t, a_t, h, next_a, next_a_t, *early = layer_0(n, x[0], w_gate, w_up, w_down, m, v)
        top = top_layer(n, next_a, next_a_t, h, dy[0], w_gate, w_up, w_down, early)
        top, (squares_1, by_h, _, _), far = split(top, WEIGHTS, 4)
        bottom = bottom_layer(n, by_h, hidden_t, a_t, gate, up, w_down, [top[i] for i, _ in EARLY])
        bottom, (squares_0,), near = split(bottom, WEIGHTS, 1)
        gradients = list(zip(bottom, top, strict=True))
        return tuple(finish(n, gradients, (squares_0, squares_1), (w_gate, w_up, w_down), m, v, (*early, *far, *near)))

    sharded = P(None, "dp", None)
    return jax.shard_map(
        step,
        mesh=mesh,
        in_specs=(P(("rep", "dp")), P(("rep", "dp")), P(), P(), P(), *[sharded] * 6),
        out_specs=(*[P("rep")] * 3, *[P("rep", "dp")] * 6),
        check_vma=False,
    )
```

```python
import functools

import jax
import jax.numpy as jnp
from jax import lax
from jax.experimental import pallas as pl
from jax.experimental.pallas import tpu as pltpu
from jax.sharding import PartitionSpec as P

MESH = pl.DeviceIdType.MESH
F32, BF16 = jnp.float32, jnp.bfloat16
CORES = 2
BUFFERS = 2
WEIGHTS = 3
MIB = 2**20
ALL_VMEM = 67043328
TRANSPOSED = ((1,), (1,))


def turn(t):
    return lax.rem(t, BUFFERS)


def repeat(low, high, body):
    def step(i, nothing):
        body(i)
        return nothing

    lax.fori_loop(low, high, step, None)


def split(refs, *sizes):
    left = iter(refs)
    runs = [[next(left) for _ in range(size)] for size in sizes]
    return *runs, list(left)


def local_copies(pairs, sem, *at):
    return [pltpu.make_async_copy(src, dst, sem.at[(k, *at)]) for k, (src, dst) in enumerate(pairs)]


def places(axis, n):
    me = lax.axis_index(axis)
    chips = n // CORES
    core, chip = lax.rem(me, CORES), lax.div(me, CORES)
    at = lambda away: lax.rem(chip + away, chips) * CORES + core
    return me, core, me + 1 - 2 * core, at(1), at(chips - 1), at(2)


class Spread:
    KINDS = 9

    def __init__(self, n, send, recv):
        self.send, self.recv = send, recv
        self.me, _, self.partner, self.after, self.before, self.across = places("dp", n)

    @staticmethod
    def semaphores(pieces):
        return [pltpu.SemaphoreType.DMA((Spread.KINDS, pieces))] * 2

    def barrier(self):
        barrier = pltpu.get_barrier_semaphore()
        for peer in (self.partner, self.after, self.before):
            pl.semaphore_signal(barrier, inc=1, device_id={"dp": peer}, device_id_type=MESH)
        pl.semaphore_wait(barrier, 3)

    def copies(self, number, place, width, own=None, far=None):
        far = far or place
        every, left, right = pl.ds(0, width), pl.ds(0, width // 2), pl.ds(width // 2, width // 2)

        class Copies(dict):
            def __missing__(_, kind):
                to, src, dst = routes[kind]
                sems = (t.at[list(routes).index(kind), number] for t in (self.send, self.recv))
                return pltpu.make_async_remote_copy(src, dst, *sems, device_id={"dp": to}, device_id_type=MESH)

        me, after, before, across = self.me, self.after, self.before, self.across
        own = place(me, every) if own is None else own
        routes = {
            "after": (after, own, place(me, every)),
            "before": (before, own, place(me, every)),
            "partner": (self.partner, own, place(me, every)),
            "on": (after, place(before, left), far(before, left)),
            "back": (before, place(after, right), far(after, right)),
            "partner_before": (self.partner, place(before, every), far(before, every)),
            "partner_after": (self.partner, place(after, every), far(after, every)),
            "partner_left": (self.partner, far(across, left), far(across, left)),
            "partner_right": (self.partner, far(across, right), far(across, right)),
        }
        return Copies()

    @staticmethod
    def start(copies):
        for kind in ("after", "before", "partner"):
            copies[kind].start()

    @staticmethod
    def pass_on(copies):
        copies["after"].wait_recv()
        copies["on"].start()
        copies["partner_before"].start()
        copies["before"].wait_recv()
        copies["back"].start()
        copies["partner_after"].start()

    @staticmethod
    def pass_last(copies):
        copies["on"].wait_recv()
        copies["partner_left"].start()
        copies["back"].wait_recv()
        copies["partner_right"].start()

    @staticmethod
    def end(copies):
        for kind in ("partner", "partner_before", "partner_after", "partner_left", "partner_right"):
            copies[kind].wait_recv()
        for kind in (*Spread.NEAR, *Spread.THEN, *Spread.LAST):
            copies[kind].wait_send()


    NEAR, THEN, LAST = ("after", "before", "partner"), ("on", "back", "partner_before", "partner_after"), ("partner_left", "partner_right")

    @staticmethod
    def end_near(copies):
        for kind in Spread.NEAR:
            copies[kind].wait()

    @staticmethod
    def start_far(copies):
        for kind in Spread.THEN:
            copies[kind].start()

    @staticmethod
    def end_far(copies):
        for kind in Spread.THEN:
            copies[kind].wait_send()
        for kind in (*Spread.THEN[2:], *Spread.LAST):
            copies[kind].wait_recv()
        for kind in Spread.LAST:
            copies[kind].wait_send()


EARLY = ((0, 32), (1, 32))


def finish_kernel(n, count, layers, pieces, *refs):
    some = len(EARLY)
    squares, *g_in = zip(*[iter(refs[: layers + layers * WEIGHTS])] * layers)
    refs = refs[layers + layers * WEIGHTS :]
    w_in, m_in, v_in, near_m, near_v, far_m, far_v, near_g, w, m, v, far_g, g, refs = split(
        refs, *[WEIGHTS] * 3, *[some] * 5, *[WEIGHTS] * 3, some, WEIGHTS
    )
    parts, m_tile, v_tile, g_tile, load_sem, early_sem, tile_sem, part_send, part_recv, send, recv = refs
    spread = Spread(n, send, recv)
    me = spread.me

    barrier = pltpu.get_barrier_semaphore()
    peers = [lax.rem(me + away, n) for away in range(1, n)]
    for peer in peers:
        pl.semaphore_signal(barrier, inc=1, device_id={"dp": peer}, device_id_type=MESH)

    def rows_of(i, owner, first, rows):
        return pl.ds(pl.multiple_of(owner * g[i].shape[1] + first, 16), rows)

    order = (2, 0, 1)
    loads = {}
    for i in order:
        rows = rows_of(i, me, 0, g[i].shape[1])
        pairs = [(w_in[i].at[:, rows], w[i].at[:, rows]), (m_in[i], m[i]), (v_in[i], v[i])]
        pairs += [(g_in[i][k], g[i].at[k]) for k in range(layers)]
        loads[i] = [pltpu.make_async_copy(src, dst, load_sem.at[i, k]) for k, (src, dst) in enumerate(pairs)]
    first_weight, *other_weights = order
    for one in loads[first_weight]:
        one.start()

    total = sum(t[...] for t in squares)
    parts[pl.ds(me, 1)] = total[None]
    early = []
    for k, (i, some) in enumerate(EARLY):
        near = lambda owner, columns, ref=near_g[k]: ref.at[owner, :, columns]
        far = lambda owner, columns, ref=far_g[k]: ref.at[owner, :, columns]
        early.append(spread.copies(len(pieces) + k, near, g[i].shape[2], None, far))
    pl.semaphore_wait(barrier, n - 1)
    part_copies = []
    for k, peer in enumerate(peers):
        part_copies.append(
            pltpu.make_async_remote_copy(
                parts.at[me], parts.at[me], part_send.at[k], part_recv.at[k], device_id={"dp": peer}, device_id_type=MESH
            )
        )
        part_copies[-1].start()
    for copies in early:
        spread.start_far(copies)
    for one in part_copies:
        one.wait_recv()
    every = parts[0]
    for k in range(1, n):
        every += parts[k]
    mean = jnp.sum(every, keepdims=True) / count
    factor = jnp.minimum(1.0, 0.5 * lax.rsqrt(mean + 1e-30))

    def stepped(grad, m_old, v_old, w_old):
        grad = grad.astype(F32) * factor
        m_new = 0.9 * m_old + 0.1 * grad
        v_new = 0.95 * v_old + 0.05 * grad * grad
        w_old = w_old.astype(F32)
        return m_new, v_new, (w_old - 0.02 * (m_new * lax.rsqrt(v_new + 1e-8) + 0.1 * w_old)).astype(BF16)

    step_rows, width = 16, 256

    def adamw(i, layer, first, rows):
        def body(step):
            start = first + step * step_rows
            at = (layer, pl.ds(pl.multiple_of(start, 16), step_rows), slice(None))
            mine = (layer, rows_of(i, me, start, step_rows), slice(None))
            m[i][at], v[i][at], w[i][mine] = stepped(g[i][at], m[i][at], v[i][at], w[i][mine])

        repeat(0, rows // step_rows, body)

    waited = set()

    def compute(i, layer, first, rows):
        if i not in waited:
            waited.add(i)
            for one in loads[i]:
                one.wait()
        adamw(i, layer, first, rows)

    made = []
    for number, (i, layer, first, rows) in enumerate(pieces):
        place = lambda owner, columns, i=i, layer=layer, first=first, rows=rows: w[i].at[layer, rows_of(i, owner, first, rows), columns]
        made.append(spread.copies(number, place, g[i].shape[2]))

    def own_piece(number):
        compute(*pieces[number])
        spread.start(made[number])

    other = lambda device: device + spread.partner - me
    units = []
    for k, (i, some) in enumerate(EARLY):
        near, far = (near_m[k], near_v[k], near_g[k]), (far_m[k], far_v[k], far_g[k])
        for refs, owners in (
            (near, (spread.partner, spread.after, spread.before)),
            (far, (other(spread.after), other(spread.before), spread.across, other(spread.across))),
        ):
            units += [(refs, i, owner, first, g[i].shape[1] - some) for owner in owners for first in range(0, some, step_rows)]

    def unit_loads(number):
        refs, _, owner, first, _ = units[number]
        slot = number % BUFFERS
        tiles = zip(refs, (m_tile, v_tile, g_tile), strict=True)
        return local_copies([(src.at[owner, pl.ds(first, step_rows)], dst.at[slot]) for src, dst in tiles], tile_sem, slot)

    def unit_rows(number):
        _, i, owner, first, start = units[number]
        return rows_of(i, owner, start + first, step_rows)

    last = layers - 1
    old_rows = local_copies(
        [tuple(t[i].at[last, unit_rows(number)] for t in (w_in, w)) for number, (_, i, _, _, _) in enumerate(units)], early_sem
    )

    def unit(number):
        (_, i, _, _, _), slot = units[number], number % BUFFERS
        if number + 1 < len(units):
            for one in unit_loads(number + 1):
                one.start()
        for one in (*unit_loads(number), old_rows[number]):
            one.wait()

        def body(step):
            columns = pl.ds(pl.multiple_of(step * width, width), width)
            its, at = (last, unit_rows(number), columns), (slot, slice(None), columns)
            *_, w[i][its] = stepped(g_tile[at], m_tile[at], v_tile[at], w[i][its])

        repeat(0, g[i].shape[-1] // width, body)

    own_piece(0)
    for i in other_weights:
        for one in loads[i]:
            one.start()
    for one in old_rows:
        one.start()
    total_pieces, done = len(pieces), 0
    for number in range(total_pieces + 2):
        if number + 1 < total_pieces:
            own_piece(number + 1)
        if number == 0:
            for copies in early:
                spread.pass_last(copies)
        if 1 <= number <= total_pieces:
            spread.pass_on(made[number - 1])
        if 2 <= number:
            spread.pass_last(made[number - 2])
        if number == 2:
            for copies in early:
                spread.end_far(copies)
            for one in unit_loads(0):
                one.start()
        if 3 <= number < total_pieces:
            for k in range(min(3, len(units) - done)):
                unit(done + k)
            done += min(3, len(units) - done)
        if number == 3:
            for i, some in EARLY:
                compute(i, last, g[i].shape[1] - some, some)
    for k in range(done, len(units)):
        unit(k)
    for copies in made:
        spread.end(copies)
    for one in part_copies:
        one.wait_send()


def store_kernel(*refs):
    *refs, sem = refs
    some = len(refs) // 2
    copies = local_copies([(refs[k], refs[some + k]) for k in range(some)], sem)
    for one in copies:
        one.start()
    for one in copies:
        one.wait()


def early_shapes(n, blocks, dtype, times=1, kind=jax.ShapeDtypeStruct):
    return [kind((n, some, blocks[i][0].shape[-1]), dtype) for _ in range(times) for i, some in EARLY]


def finish(n, gradients, squares, weights, m, v, early):
    count = float(sum(w.size for w in weights))
    layers = len(gradients[0])
    pieces = []
    for i in (2, 0, 1):
        rows, _ = gradients[i][0].shape
        for layer in range(layers):
            half = rows // 2
            cuts = [half, half]
            if (i, layer) == (2, 0):
                cuts = [48, half - 48, half]
            elif layer == layers - 1 and i in dict(EARLY):
                rest = half - dict(EARLY)[i]
                cuts = [half + rest - 16, 16] if i == 1 else [half + rest]
            for cut in cuts:
                pieces.append((i, layer, sum(p[3] for p in pieces if p[:2] == (i, layer)), cut))
    anywhere, inside = pl.BlockSpec(memory_space=pl.ANY), pl.BlockSpec(memory_space=pltpu.VMEM)
    dma = pltpu.SemaphoreType.DMA
    results = [*weights, *m, *v]
    tile = lambda dtype: pltpu.VMEM((BUFFERS, 16, max(gradients[i][0].shape[1] for i, _ in EARLY)), dtype)
    ready = pl.pallas_call(
        functools.partial(finish_kernel, n, count, layers, tuple(pieces)),
        out_shape=[pltpu.VMEM(t.shape, t.dtype) for t in results]
        + early_shapes(n, gradients, BF16),
        in_specs=[inside] * layers + [anywhere] * (WEIGHTS * layers + len(results) + len(early)),
        out_specs=[inside] * len(results) + [anywhere] * len(EARLY),
        scratch_shapes=[
            *[pltpu.VMEM((layers, *one[0].shape), BF16) for one in gradients],
            pltpu.VMEM((n, 8, 128), F32), tile(F32), tile(F32), tile(BF16),
            dma((WEIGHTS, layers + 3)), dma((sum(some for _, some in EARLY) // 16 * (n - 1),)), dma((3, BUFFERS)), *[dma((n - 1,))] * 2,
            *Spread.semaphores(len(pieces) + len(EARLY)),
        ],
        compiler_params=pltpu.CompilerParams(collective_id=4, has_side_effects=True, vmem_limit_bytes=8 * MIB),
        name="finish",
    )(*squares, *sum(gradients, ()), *weights, *m, *v, *early)[: len(results)]
    return pl.pallas_call(
        store_kernel,
        out_shape=[jax.ShapeDtypeStruct(t.shape, t.dtype) for t in results],
        in_specs=[inside] * len(results),
        out_specs=[anywhere] * len(results),
        scratch_shapes=[dma((len(results),))],
        compiler_params=pltpu.CompilerParams(vmem_limit_bytes=8 * MIB),
        name="store",
    )(*[pltpu.with_memory_space_constraint(t, pltpu.VMEM) for t in ready])


def dot(a, b, contract=((1,), (0,))):
    return lax.dot_general(a, b, (contract, ((), ())), preferred_element_type=F32)


def normed(h):
    wide = h.astype(F32)
    return (wide * lax.rsqrt(jnp.mean(wide * wide, -1, keepdims=True) + 1e-6)).astype(BF16)


def by_norm(h, by_a):
    wide = h.astype(F32)
    scale = lax.rsqrt(jnp.mean(wide * wide, -1, keepdims=True) + 1e-6)
    return scale * by_a - wide * (scale * scale * scale * jnp.mean(by_a * wide, -1, keepdims=True))


def by_units(gate, up, by_hidden):
    by_hidden = by_hidden.astype(BF16).astype(F32)
    s = jax.nn.sigmoid(gate)
    silu = gate * s
    return silu * up, by_hidden * up * (s + silu * (1.0 - s)), by_hidden * silu


def forward_kernel(n, *refs):
    (x_in, w_gate, w_up, w_down), moments, outs, early, refs = split(refs, 4, 2 * len(EARLY), 7, 2 * len(EARLY))
    gate_out, up_out, ht_out, at_out, h_out, b_out, bt_out = outs
    (wg, wu, wd, hidden, x, gate, up, hidden_t, a_t, h, b, b_t, w_sem, x_sem, sem, late_sem, send, recv) = refs
    spread = Spread(n, send, recv)
    rows = x.shape[1]
    tiles = x_in.shape[0] // rows
    ff = wg.shape[1]
    width = 256
    groups = [range(at, min(at + 3 * width, ff), width) for at in range(0, ff, 3 * width)]
    tall = lambda ref, t: ref.at[pl.ds(pl.multiple_of(t * rows, rows), rows)]
    wide = lambda ref, t: ref.at[:, pl.ds(pl.multiple_of(t * rows, rows), rows)]

    def load_x(t):
        return pltpu.make_async_copy(tall(x_in, t), x.at[lax.rem(t, x.shape[0])], x_sem.at[lax.rem(t, x.shape[0])])

    def stores(t, first):
        slot = turn(t)
        if first:
            pairs = [(gate, tall(gate_out, t)), (up, tall(up_out, t)), (hidden_t, wide(ht_out, t)), (a_t, wide(at_out, t))]
        else:
            pairs = [(h, tall(h_out, t)), (b, tall(b_out, t)), (b_t, wide(bt_out, t))]
        return local_copies([(src.at[slot], dst) for src, dst in pairs], sem if first else late_sem, slot)

    w_loads = []
    for k, group in enumerate(groups):
        columns = slice(group[0], group[-1] + width)
        w_loads.append([
            pltpu.make_async_copy(src.at[0, :, columns], dst.at[:, columns], w_sem.at[j, k]) for j, (src, dst) in enumerate(((w_gate, wg), (w_up, wu)))
        ])
    down_load = pltpu.make_async_copy(w_down.at[0], wd, w_sem.at[2, 0])
    for one in (load_x(0), *w_loads[0], *w_loads[1], load_x(1)):
        one.start()
    spread.barrier()
    pieces = []
    for number, (src, dst) in enumerate(zip(moments, early, strict=True)):
        some = dst.shape[1]
        own = src.at[src.shape[0] - 1, pl.ds(src.shape[1] - some, some)]
        pieces.append(spread.copies(number, lambda owner, columns, dst=dst: dst.at[owner, :, columns], dst.shape[2], own))
    for copies in pieces:
        spread.start(copies)

    def first_part(t, group, a):
        slot = turn(t)
        for at in group:
            columns = slice(at, at + width)
            g, u = dot(a, wg[:, columns]), dot(a, wu[:, columns])
            gate[slot, :, columns] = g
            up[slot, :, columns] = u
            units = (g * jax.nn.sigmoid(g) * u).astype(BF16)
            hidden[:, columns] = units
            hidden_t[slot, columns] = units.T

    def second_part(t):
        slot = turn(t)
        out = x[lax.rem(t, x.shape[0])] + dot(hidden[...], wd[...]).astype(BF16)
        h[slot] = out
        after = normed(out)
        b[slot] = after
        b_t[slot] = after.T

    def normed_tile(t):
        a = normed(x[lax.rem(t, x.shape[0])])
        a_t[turn(t)] = a.T
        return a

    load_x(0).wait()
    a = normed_tile(0)
    for k, group in enumerate(groups):
        for one in w_loads[k]:
            one.wait()
        for one in w_loads[k + 2] if k + 2 < len(groups) else ([down_load] if k + 2 == len(groups) else []):
            one.start()
        first_part(0, group, a)
    for one in stores(0, True):
        one.start()
    down_load.wait()

    def tile(t):
        load_x(t).wait()

        @pl.when(t + 1 < tiles)
        def _():
            load_x(t + 1).start()

        @pl.when(t >= BUFFERS)
        def _():
            for one in stores(t - BUFFERS, True):
                one.wait()

        @pl.when(t > BUFFERS)
        def _():
            for one in stores(t - 1 - BUFFERS, False):
                one.wait()

        a = normed_tile(t)
        second_part(t - 1)
        first_part(t, range(0, ff, width), a)
        for one in (*stores(t - 1, False), *stores(t, True)):
            one.start()

    repeat(1, tiles, tile)
    last = tiles - 1
    for one in stores(last - BUFFERS, False):
        one.wait()
    second_part(last)
    for one in stores(last, False):
        one.start()
    for copies in pieces:
        spread.end_near(copies)
    for t in (last - 1, last):
        for one in (*stores(t, True), *stores(t, False)):
            one.wait()


def layer_0(n, x, w_gate, w_up, w_down, m, v):
    tokens, d = x.shape
    ff = w_gate.shape[2]
    rows = 256
    anywhere = pl.BlockSpec(memory_space=pl.ANY)
    dma = pltpu.SemaphoreType.DMA
    vmem = lambda *shape: pltpu.VMEM(shape, BF16)
    return pl.pallas_call(
        functools.partial(forward_kernel, n),
        in_specs=[anywhere] * (4 + 2 * len(EARLY)),
        out_specs=[anywhere] * (7 + 2 * len(EARLY)),
        out_shape=[
            pltpu.HBM((tokens, ff), F32),
            pltpu.HBM((tokens, ff), F32),
            pltpu.HBM((ff, tokens), BF16),
            pltpu.HBM((d, tokens), BF16),
            pltpu.HBM((tokens, d), BF16),
            pltpu.HBM((tokens, d), BF16),
            pltpu.HBM((d, tokens), BF16),
            *early_shapes(n, m, F32, 2, pltpu.HBM),
        ],
        scratch_shapes=[
            vmem(d, ff), vmem(d, ff), vmem(ff, d), vmem(rows, ff), vmem(3, rows, d),
            *[pltpu.VMEM((BUFFERS, rows, ff), F32)] * 2, *[vmem(BUFFERS, *t) for t in ((ff, rows), (d, rows), (rows, d), (rows, d), (d, rows))],
            dma((WEIGHTS, 4)), dma((3,)), dma((4, BUFFERS)), dma((3, BUFFERS)), *Spread.semaphores(2 * len(EARLY)),
        ],
        compiler_params=pltpu.CompilerParams(collective_id=1, has_side_effects=True, vmem_limit_bytes=48 * MIB),
        name="forward",
    )(*[pltpu.with_memory_space_constraint(t, pltpu.HBM) for t in (x, w_gate, w_up, w_down, *[t[i] for t in (m, v) for i, _ in EARLY])])


class Exchange:
    def __init__(self, n, refs, kinds, lags):
        self.mine, self.pair, self.out2, self.out3, self.in2, self.in3, self.own, self.side, self.pair_sem, self.sem2, self.sem3 = refs
        self.kinds = kinds
        self.lags = lags
        self.me, self.core, self.partner, self.after, self.before, _ = places("dp", n)
        chips = n // CORES
        self.chip = lax.div(self.me, CORES)
        self.chip_after, self.chip_before, self.chip_across = (lax.rem(self.chip + k, chips) for k in (1, chips - 1, chips // 2))
        half = self.out3.shape[-1]
        self.left, self.right = slice(0, half), slice(half, 2 * half)

    @staticmethod
    def scratch(n, rows, width, lags):
        chips, half, dma = n // CORES, width // 2, pltpu.SemaphoreType.DMA
        _, two, three, four = lags
        slots1, slots2, slots3 = two + 3, 2 * (three - two) + 2, 2 * (four - three) + 2
        return [
            pltpu.VMEM((two + 1, chips, CORES, rows, width), BF16),
            pltpu.VMEM((slots1, chips, rows, width), BF16),
            pltpu.VMEM((2, three - two + 1, rows, width), BF16),
            pltpu.VMEM((2, four - three + 1, rows, half), BF16),
            pltpu.VMEM((2, slots2, rows, width), BF16),
            pltpu.VMEM((2, slots3, rows, half), BF16),
            pltpu.VMEM((four - two + 1, rows, width), F32),
            pltpu.VMEM((2, three - two + 1, rows, half), F32),
            dma((2, slots1)), dma((2, 2, slots2)), dma((2, 2, slots3)),
        ]

    def held(self, p):
        return lax.rem(p, self.mine.shape[0])

    def barrier(self):
        barrier = pltpu.get_barrier_semaphore()
        for peer in (self.partner, self.after, self.before):
            pl.semaphore_signal(barrier, inc=1, device_id={"dp": peer}, device_id_type=MESH)
        pl.semaphore_wait(barrier, 3)

    def copy1(self, p, rows):
        slot = lax.rem(p, self.pair.shape[0])
        return pltpu.make_async_remote_copy(
            self.mine.at[self.held(p), :, 1 - self.core, pl.ds(0, rows)], self.pair.at[slot, :, pl.ds(0, rows)],
            self.pair_sem.at[0, slot], self.pair_sem.at[1, slot], device_id={"dp": self.partner}, device_id_type=MESH,
        )

    def copies(self, p, rows, out, into, sem):
        slot = lax.rem(p, into.shape[1])
        return [
            pltpu.make_async_remote_copy(
                out.at[way, lax.rem(p, out.shape[1]), pl.ds(0, rows)], into.at[way, slot, pl.ds(0, rows)],
                sem.at[0, way, slot], sem.at[1, way, slot], device_id={"dp": to}, device_id_type=MESH,
            )
            for way, to in enumerate((self.after, self.before))
        ]

    def copies2(self, p, rows):
        return self.copies(p, rows, self.out2, self.in2, self.sem2)

    def copies3(self, p, rows):
        return self.copies(p, rows, self.out3, self.in3, self.sem3)

    def stage1(self, p, rows, _):
        self.copy1(p, rows).start()

    def stage2(self, p, rows, _):
        self.copy1(p, rows).wait()
        slot, own, side = (lax.rem(p, t.shape[k]) for t, k in ((self.out2, 1), (self.own, 0), (self.side, 1)))
        at = slice(0, rows)

        def of_chip(chip, columns):
            a = self.mine[self.held(p), chip, self.core, at, columns].astype(F32)
            return a + self.pair[lax.rem(p, self.pair.shape[0]), chip, at, columns].astype(F32)

        self.out2[0, slot, at, self.left] = of_chip(self.chip_across, self.left).astype(BF16)
        self.out2[0, slot, at, self.right] = of_chip(self.chip_after, self.right).astype(BF16)
        self.out2[1, slot, at, self.left] = of_chip(self.chip_before, self.left).astype(BF16)
        self.out2[1, slot, at, self.right] = of_chip(self.chip_across, self.right).astype(BF16)
        for one in self.copies2(p, rows):
            one.start()
        self.side[0, side, at] = of_chip(self.chip_after, self.left)
        self.side[1, side, at] = of_chip(self.chip_before, self.right)
        for columns in (self.left, self.right):
            self.own[own, at, columns] = of_chip(self.chip, columns)

    def stage3(self, p, rows, _):
        for one in self.copies2(p, rows):
            one.wait()
        slot, arrived, own, side = (lax.rem(p, t.shape[k]) for t, k in ((self.out3, 1), (self.in2, 1), (self.own, 0), (self.side, 1)))
        at = slice(0, rows)
        self.out3[0, slot, at] = (self.side[0, side, at] + self.in2[0, arrived, at, self.left].astype(F32)).astype(BF16)
        self.out3[1, slot, at] = (self.side[1, side, at] + self.in2[1, arrived, at, self.right].astype(F32)).astype(BF16)
        for one in self.copies3(p, rows):
            one.start()
        self.own[own, at, self.left] += self.in2[1, arrived, at, self.left].astype(F32)
        self.own[own, at, self.right] += self.in2[0, arrived, at, self.right].astype(F32)

    def stage4(self, p, rows, keep):
        for one in self.copies3(p, rows):
            one.wait()
        arrived, own = lax.rem(p, self.in3.shape[1]), lax.rem(p, self.own.shape[0])
        at = slice(0, rows)
        a = self.own[own, at, self.left] + self.in3[0, arrived, at].astype(F32)
        b = self.own[own, at, self.right] + self.in3[1, arrived, at].astype(F32)
        keep(p, a.astype(BF16), b.astype(BF16))

    def finish(self, step, packets):
        for step in range(step, packets + self.lags[-1]):
            self.move(step, step, step + 1)

    def move(self, step, low, high):
        one, two, three, four = zip(self.lags, (self.stage1, self.stage2, self.stage3, self.stage4), strict=True)
        for lag, stage in (one, three, two, four):
            for first, end, rows, keep in self.kinds:
                if high - 1 - lag < first or low - lag >= end:
                    continue
                p = step - lag
                if low - lag >= first and high - 1 - lag < end:
                    stage(p, rows, keep)
                else:
                    pl.when((p >= first) & (p < end))(functools.partial(stage, p, rows, keep))


def add_squares(total, *blocks):
    for block in blocks:
        wide = block.astype(F32)
        wide = wide * wide
        rows, columns = wide.shape
        sums = [wide[r : r + 8, c : c + 128] for r in range(0, rows, 8) for c in range(0, columns, 128)]
        while len(sums) > 1:
            sums = [a + b for a, b in zip(sums[::2], sums[1::2])] + ([sums[-1]] if len(sums) % 2 else [])
        total[...] += sums[0]


def keep_columns(first, gate, up, width, squares):
    def keep(p, left, right):
        columns = pl.ds(pl.multiple_of((p - first) * width, width), width)
        gate[:, columns] = left
        up[:, columns] = right
        add_squares(squares, left, right)

    return keep


def keep_tall(first, down, rows, width, squares):
    def keep(p, left, right):
        columns = pl.ds(pl.multiple_of((p - first) * width, width), width)
        down[:rows, columns] = left
        down[rows:, columns] = right
        add_squares(squares, left, right)

    return keep


def keep_down(first, down, rows, width, squares):
    def keep(p, left, right):
        half = width // 2
        which = p - first
        at = pl.ds(pl.multiple_of(lax.rem(which, 2) * rows, 16), rows)
        start = lax.div(which, 2) * width
        down[at, pl.ds(pl.multiple_of(start, half), half)] = left
        down[at, pl.ds(pl.multiple_of(start + half, half), half)] = right
        add_squares(squares, left, right)

    return keep


def tall_packet(exchange, step, first, hidden_t, by_out):
    _, chips, cores, rows, width = exchange.mine.shape
    half = width // 2
    by_out = by_out[:, pl.ds(pl.multiple_of((step - first) * half, half), half)]
    for k in range(chips * cores):
        block = dot(hidden_t[2 * rows * k : 2 * rows * (k + 1), :], by_out).astype(BF16)
        for part in range(2):
            exchange.mine[exchange.held(step), k // cores, k % cores, :, part * half : (part + 1) * half] = block[part * rows : (part + 1) * rows]


def down_packet(exchange, step, first, hidden_t, by_out):
    n_rows = hidden_t.shape[0]
    _, chips, cores, rows, width = exchange.mine.shape
    which = step - first
    start = pl.multiple_of(lax.rem(which, 2) * rows, 16)
    columns = pl.ds(pl.multiple_of(lax.div(which, 2) * width, width), width)
    share = n_rows // (chips * cores)
    by_out = by_out[:, columns]
    for k in range(chips * cores):
        lhs = hidden_t[pl.ds(pl.multiple_of(k * share + start, 16), rows), :]
        exchange.mine[exchange.held(step), k // cores, k % cores] = dot(lhs, by_out).astype(BF16)


def wide_packet(exchange, step, a_t, by_both):
    _, chips, cores, _, width = exchange.mine.shape
    rows = a_t.shape[0] // (chips * cores)
    half = width // 2
    for k in range(2):
        columns = slice(k * half, k * half + half)
        block = dot(a_t[...], by_both[:, columns]).astype(BF16)
        exchange.mine[exchange.held(step), :, :, pl.ds(0, rows), columns] = block.reshape(chips, cores, rows, half)


MB = 1024
TOP_LAGS = (0, 1, 4, 6)
BOTTOM_LAGS = (0, 1, 5, 9)


def top_kernel(n, *refs):
    several = 2 * len(EARLY)
    ins, near, outs, far, (send, recv), refs = split(refs, 7, several, 7, several, 2)
    a_in, at_in, h_in, dy, w_gate, w_up, w_down = ins
    g_gate, g_up, g_down, squares, by_h, bg_hbm, bu_hbm = outs
    spread = Spread(n, send, recv)
    (a, a_t, wg, wu, hidden_t, wd, both, h_tile, by_tile, load_sem, wd_sem, both_sem, tile_sem, by_sem), refs = split(refs, 14)
    tokens, d = a.shape
    ff = wg.shape[1]
    width = 256
    chunks = ff // width
    downs = 4
    wide_rows, down_rows = d // n, ff // n // 2
    exchange = Exchange(
        n, refs,
        (
            (0, chunks, wide_rows, keep_columns(0, g_gate, g_up, width, squares)),
            (chunks, chunks + downs, down_rows, keep_tall(chunks, g_down, down_rows, width, squares)),
        ),
        TOP_LAGS,
    )
    layer = w_gate.shape[0] - 1
    first, rest = pl.ds(0, width), pl.ds(width, ff - width)
    columns_of = lambda columns: [(src.at[layer, :, columns], dst.at[:, columns]) for src, dst in ((w_gate, wg), (w_up, wu))]
    loads = local_copies([(a_in, a), (at_in, a_t), *columns_of(first), *columns_of(rest)], load_sem)
    def down_chunk(c):
        slot = turn(c)
        return pltpu.make_async_copy(w_down.at[layer, pl.ds(pl.multiple_of(c * width, width), width)], wd.at[slot], wd_sem.at[slot])

    loads, later_loads = split(loads, 4)
    for one in (*loads, down_chunk(0)):
        one.start()
    squares[...] = jnp.zeros_like(squares)
    exchange.barrier()

    early = []
    for number, (src, dst) in enumerate(zip(near, far, strict=True)):
        places = [lambda owner, columns, ref=ref: ref.at[owner, :, columns] for ref in (src, dst)]
        early.append(spread.copies(number, places[0], src.shape[2], None, places[1]))
    for copies in early:
        spread.start_far(copies)

    def store_both(c):
        slot = turn(c)
        to = pl.ds(pl.multiple_of(c * width, width), width)
        return local_copies([(both.at[slot, :, pl.ds(k * width, width)], ref.at[:, to]) for k, ref in enumerate((bg_hbm, bu_hbm))], both_sem, slot)

    def chunk(c):
        slot = turn(c)

        @pl.when(c == 0)
        def _():
            for one in loads:
                one.wait()
            for one in later_loads:
                one.start()

        @pl.when(c == 1)
        def _():
            for one in later_loads:
                one.wait()

        @pl.when(c >= BUFFERS)
        def _():
            for one in store_both(c - BUFFERS):
                one.wait()

        @pl.when(c == chunks // 2)
        def _():
            for copies in early:
                spread.pass_last(copies)

        down_chunk(c).wait()

        @pl.when(c + 1 < chunks)
        def _():
            down_chunk(c + 1).start()

        columns = pl.ds(pl.multiple_of(c * width, width), width)
        wg_c, wu_c, wd_c = wg[:, columns], wu[:, columns], wd[slot]
        for at in range(0, tokens, MB):
            rows = slice(at, at + MB)
            hidden, by_gate, by_up = by_units(dot(a[rows], wg_c), dot(a[rows], wu_c), dot(dy[rows], wd_c, TRANSPOSED))
            hidden_t[columns, rows] = hidden.astype(BF16).T
            both[slot, rows, :width] = by_gate.astype(BF16)
            both[slot, rows, width:] = by_up.astype(BF16)
        wide_packet(exchange, c, a_t, both.at[slot])
        for one in store_both(c):
            one.start()
        exchange.move(c, 0, chunks)

    repeat(0, chunks, chunk)
    for c in range(chunks - BUFFERS, chunks):
        for one in store_both(c):
            one.wait()

    tile_rows = 256
    tiles = tokens // tile_rows
    split_at = a_t.shape[1]

    def tile_loads(t):
        slot = turn(t)
        rows = pl.ds(pl.multiple_of(t * tile_rows, tile_rows), tile_rows)
        pairs = [(h_in.at[rows], h_tile.at[slot])]
        for k, src in enumerate((bg_hbm, bu_hbm)):
            to = pl.ds(pl.multiple_of((slot * 2 + k) * tile_rows, tile_rows), tile_rows)
            pairs.append((src.at[rows, pl.ds(0, split_at)], a_t.at[to]))
            pairs.append((src.at[rows, pl.ds(split_at, ff - split_at)], a.at[to, pl.ds(0, ff - split_at)]))
        return local_copies(pairs, tile_sem, slot)

    def tile_store(t):
        slot = turn(t)
        return pltpu.make_async_copy(by_tile.at[slot], by_h.at[pl.ds(pl.multiple_of(t * tile_rows, tile_rows), tile_rows)], by_sem.at[slot])

    for one in tile_loads(0):
        one.start()

    def tile(step):
        t = step - chunks

        @pl.when(t < downs)
        def _():
            tall_packet(exchange, step, chunks, hidden_t, dy)

        exchange.move(step, chunks, chunks + tiles)
        slot = turn(t)
        for one in tile_loads(t):
            one.wait()

        @pl.when(t + 1 < tiles)
        def _():
            for one in tile_loads(t + 1):
                one.start()

        @pl.when(t >= BUFFERS)
        def _():
            tile_store(t - BUFFERS).wait()

        total = None
        for k, w in enumerate((wg, wu)):
            at = pl.ds(pl.multiple_of((slot * 2 + k) * tile_rows, tile_rows), tile_rows)
            term = dot(a_t[at], w[:, :split_at], TRANSPOSED) + dot(a[at, : ff - split_at], w[:, split_at:], TRANSPOSED)
            total = term if total is None else total + term
        rows = pl.ds(pl.multiple_of(t * tile_rows, tile_rows), tile_rows)
        by_tile[slot] = (dy[rows].astype(F32) + by_norm(h_tile[slot], total)).astype(BF16)
        tile_store(t).start()

    repeat(chunks, chunks + tiles, tile)
    exchange.finish(chunks + tiles, chunks + downs)
    for t in range(tiles - BUFFERS, tiles):
        tile_store(t).wait()
    for copies in early:
        spread.end_far(copies)


def top_layer(n, a, a_t, h, dy, w_gate, w_up, w_down, near):
    tokens, d = a.shape
    ff = w_gate.shape[2]
    width = 256
    anywhere, inside = pl.BlockSpec(memory_space=pl.ANY), pl.BlockSpec(memory_space=pltpu.VMEM)
    dma = pltpu.SemaphoreType.DMA
    return pl.pallas_call(
        functools.partial(top_kernel, n),
        in_specs=[*[anywhere] * 3, inside, *[anywhere] * (3 + len(near))],
        out_specs=[inside] * 4 + [anywhere] * (3 + len(near)),
        out_shape=[
            jax.ShapeDtypeStruct((d // n, ff), BF16),
            jax.ShapeDtypeStruct((d // n, ff), BF16),
            jax.ShapeDtypeStruct((ff // n, d), BF16),
            jax.ShapeDtypeStruct((8, 128), F32),
            jax.ShapeDtypeStruct((tokens, d), BF16),
            jax.ShapeDtypeStruct((tokens, ff), BF16),
            jax.ShapeDtypeStruct((tokens, ff), BF16),
            *[jax.ShapeDtypeStruct(t.shape, t.dtype) for t in near],
        ],
        scratch_shapes=[
            *Spread.semaphores(len(near)),
            *[pltpu.VMEM(t, BF16) for t in ((tokens, d), (d, tokens), (d, ff), (d, ff), (ff, tokens))],
            *[pltpu.VMEM((BUFFERS, *t), BF16) for t in ((width, d), (tokens, 2 * width), (width, d), (width, d))],
            dma((6,)), dma((BUFFERS,)), dma((2, BUFFERS)), dma((5, BUFFERS)), dma((BUFFERS,)),
            *Exchange.scratch(n, ff // n // 2, 2 * width, TOP_LAGS),
        ],
        compiler_params=pltpu.CompilerParams(collective_id=2, has_side_effects=True, vmem_limit_bytes=ALL_VMEM - 9 * MIB // 2),
        name="top",
    )(a, a_t, h, pltpu.with_memory_space_constraint(dy, pltpu.VMEM), w_gate, w_up, w_down, *near)


def bottom_kernel(n, *refs):
    some = len(EARLY)
    ins, summed, (g_gate, g_up, g_down, squares), near, (send, recv), refs = split(refs, 6, some, 4, some, 2)
    by_in, ht_in, at_in, gate_in, up_in, w_down = ins
    spread = Spread(n, send, recv)
    (by, hidden_t, a_t, wd, gate, up, both, load_sem, unit_sem), refs = split(refs, 9)
    tokens, d = by.shape
    ff = hidden_t.shape[0]
    width = 256
    chunks = ff // width
    downs = 4
    wide_rows, down_rows = d // n, ff // n // 2
    exchange = Exchange(
        n, refs,
        (
            (0, downs, down_rows, keep_down(0, g_down, down_rows, 2 * width, squares)),
            (downs, downs + chunks, wide_rows, keep_columns(downs, g_gate, g_up, width, squares)),
        ),
        BOTTOM_LAGS,
    )
    share = ff // n
    halves = lambda ref, k: ref.at[:, pl.ds(k * 2 * width, 2 * width)]
    pairs = [(halves(by_in, 0), halves(by, 0))]
    for k in range(2):
        for to in range(n):
            rows = pl.ds(to * share + k * down_rows, down_rows)
            pairs.append((ht_in.at[rows], hidden_t.at[rows]))
    pairs += [(halves(by_in, 1), halves(by, 1)), (at_in, a_t)]
    loads = local_copies(pairs, load_sem)

    def chunk_loads(c):
        slot = turn(c)
        columns = pl.ds(pl.multiple_of(c * width, width), width)
        pairs = [(w_down.at[0, columns], wd.at[slot]), (gate_in.at[:, columns], gate.at[slot]), (up_in.at[:, columns], up.at[slot])]
        return local_copies(pairs, unit_sem, slot)

    first, second, third = split(loads, 1 + n, n)
    third += chunk_loads(0)
    for one in first:
        one.start()
    squares[...] = jnp.zeros_like(squares)
    exchange.barrier()

    early = []
    for number, (src, dst) in enumerate(zip(summed, near, strict=True)):
        some = dst.shape[1]
        own = src.at[pl.ds(src.shape[0] - some, some)]
        early.append(spread.copies(number, lambda owner, columns, dst=dst: dst.at[owner, :, columns], dst.shape[2], own))
    for copies in early:
        spread.start(copies)

    def down(step):
        @pl.when(step == 0)
        def _():
            for one in first:
                one.wait()
            for one in second:
                one.start()

        @pl.when(step == 1)
        def _():
            for one in second:
                one.wait()
            for one in third:
                one.start()

        @pl.when(step == 2)
        def _():
            for one in third[:2]:
                one.wait()

        down_packet(exchange, step, 0, hidden_t, by)
        exchange.move(step, 0, downs)

    repeat(0, downs, down)

    def chunk(step):
        c = step - downs
        slot = turn(c)
        for one in chunk_loads(c):
            one.wait()

        @pl.when(c + 1 < chunks)
        def _():
            for one in chunk_loads(c + 1):
                one.start()

        wd_c = wd[slot]
        for at in range(0, tokens, MB):
            rows = slice(at, at + MB)
            _, by_gate, by_up = by_units(gate[slot, rows], up[slot, rows], dot(by[rows], wd_c, TRANSPOSED))
            both[rows, :width] = by_gate.astype(BF16)
            both[rows, width:] = by_up.astype(BF16)
        wide_packet(exchange, step, a_t, both)
        exchange.move(step, downs, downs + chunks)

    repeat(downs, downs + chunks, chunk)
    exchange.finish(downs + chunks, downs + chunks)
    for copies in early:
        spread.end_near(copies)


def bottom_layer(n, by, hidden_t, a_t, gate, up, w_down, summed):
    tokens, d = by.shape
    ff = hidden_t.shape[0]
    width = 256
    anywhere, inside = pl.BlockSpec(memory_space=pl.ANY), pl.BlockSpec(memory_space=pltpu.VMEM)
    dma = pltpu.SemaphoreType.DMA
    return pl.pallas_call(
        functools.partial(bottom_kernel, n),
        in_specs=[anywhere] * (6 + len(summed)),
        out_specs=[inside] * 4 + [anywhere] * len(summed),
        out_shape=[
            jax.ShapeDtypeStruct((d // n, ff), BF16),
            jax.ShapeDtypeStruct((d // n, ff), BF16),
            jax.ShapeDtypeStruct((ff // n, d), BF16),
            jax.ShapeDtypeStruct((8, 128), F32),
            *[jax.ShapeDtypeStruct((n, some, ff), BF16) for _, some in EARLY],
        ],
        scratch_shapes=[
            *Spread.semaphores(len(summed)),
            *[pltpu.VMEM(t, BF16) for t in ((tokens, d), (ff, tokens), (d, tokens), (BUFFERS, width, d))],
            *[pltpu.VMEM((BUFFERS, tokens, width), F32)] * 2, pltpu.VMEM((tokens, 2 * width), BF16),
            dma((3 + 2 * n,)), dma((3, BUFFERS)),
            *Exchange.scratch(n, ff // n // 2, 2 * width, BOTTOM_LAGS),
        ],
        compiler_params=pltpu.CompilerParams(collective_id=3, has_side_effects=True, vmem_limit_bytes=ALL_VMEM),
        name="bottom",
    )(by, hidden_t, a_t, gate, up, w_down, *summed)


def solution(mesh):
    n = mesh.shape["dp"]

    def step(x, dy, w_gate, w_up, w_down, *moments):
        m, v = split(moments, WEIGHTS)
        gate, up, hidden_t, a_t, h, next_a, next_a_t, *early = layer_0(n, x[0], w_gate, w_up, w_down, m, v)
        top = top_layer(n, next_a, next_a_t, h, dy[0], w_gate, w_up, w_down, early)
        top, (squares_1, by_h, _, _), far = split(top, WEIGHTS, 4)
        bottom = bottom_layer(n, by_h, hidden_t, a_t, gate, up, w_down, [top[i] for i, _ in EARLY])
        bottom, (squares_0,), near = split(bottom, WEIGHTS, 1)
        gradients = list(zip(bottom, top, strict=True))
        return tuple(finish(n, gradients, (squares_0, squares_1), (w_gate, w_up, w_down), m, v, (*early, *far, *near)))

    sharded = P(None, "dp", None)
    return jax.shard_map(
        step,
        mesh=mesh,
        in_specs=(P(("rep", "dp")), P(("rep", "dp")), P(), P(), P(), *[sharded] * 6),
        out_specs=(*[P("rep")] * 3, *[P("rep", "dp")] * 6),
        check_vma=False,
    )
```

```python
import functools

import jax
import jax.numpy as jnp
from jax import lax
from jax.experimental import pallas as pl
from jax.experimental.pallas import tpu as pltpu
from jax.sharding import PartitionSpec as P

MESH = pl.DeviceIdType.MESH
F32, BF16 = jnp.float32, jnp.bfloat16
CORES = 2
BUFFERS = 2
WEIGHTS = 3
MIB = 2**20
ALL_VMEM = 67043328
TRANSPOSED = ((1,), (1,))


def turn(t):
    return lax.rem(t, BUFFERS)


def repeat(low, high, body):
    def step(i, nothing):
        body(i)
        return nothing

    lax.fori_loop(low, high, step, None)


def split(refs, *sizes):
    left = iter(refs)
    runs = [[next(left) for _ in range(size)] for size in sizes]
    return *runs, list(left)


def local_copies(pairs, sem, *at):
    return [pltpu.make_async_copy(src, dst, sem.at[(k, *at)]) for k, (src, dst) in enumerate(pairs)]


def places(axis, n):
    me = lax.axis_index(axis)
    chips = n // CORES
    core, chip = lax.rem(me, CORES), lax.div(me, CORES)
    at = lambda away: lax.rem(chip + away, chips) * CORES + core
    return me, core, me + 1 - 2 * core, at(1), at(chips - 1), at(2)


class Spread:
    KINDS = 9

    def __init__(self, n, send, recv):
        self.send, self.recv = send, recv
        self.me, _, self.partner, self.after, self.before, self.across = places("dp", n)

    @staticmethod
    def semaphores(pieces):
        return [pltpu.SemaphoreType.DMA((Spread.KINDS, pieces))] * 2

    def barrier(self):
        barrier = pltpu.get_barrier_semaphore()
        for peer in (self.partner, self.after, self.before):
            pl.semaphore_signal(barrier, inc=1, device_id={"dp": peer}, device_id_type=MESH)
        pl.semaphore_wait(barrier, 3)

    def copies(self, number, place, width, own=None, far=None):
        far = far or place
        every, left, right = pl.ds(0, width), pl.ds(0, width // 2), pl.ds(width // 2, width // 2)

        class Copies(dict):
            def __missing__(_, kind):
                to, src, dst = routes[kind]
                sems = (t.at[list(routes).index(kind), number] for t in (self.send, self.recv))
                return pltpu.make_async_remote_copy(src, dst, *sems, device_id={"dp": to}, device_id_type=MESH)

        me, after, before, across = self.me, self.after, self.before, self.across
        own = place(me, every) if own is None else own
        routes = {
            "after": (after, own, place(me, every)),
            "before": (before, own, place(me, every)),
            "partner": (self.partner, own, place(me, every)),
            "on": (after, place(before, left), far(before, left)),
            "back": (before, place(after, right), far(after, right)),
            "partner_before": (self.partner, place(before, every), far(before, every)),
            "partner_after": (self.partner, place(after, every), far(after, every)),
            "partner_left": (self.partner, far(across, left), far(across, left)),
            "partner_right": (self.partner, far(across, right), far(across, right)),
        }
        return Copies()

    @staticmethod
    def start(copies):
        for kind in ("after", "before", "partner"):
            copies[kind].start()

    @staticmethod
    def pass_on(copies):
        copies["after"].wait_recv()
        copies["on"].start()
        copies["partner_before"].start()
        copies["before"].wait_recv()
        copies["back"].start()
        copies["partner_after"].start()

    @staticmethod
    def pass_last(copies):
        copies["on"].wait_recv()
        copies["partner_left"].start()
        copies["back"].wait_recv()
        copies["partner_right"].start()

    @staticmethod
    def end(copies):
        for kind in ("partner", "partner_before", "partner_after", "partner_left", "partner_right"):
            copies[kind].wait_recv()
        for kind in (*Spread.NEAR, *Spread.THEN, *Spread.LAST):
            copies[kind].wait_send()


    NEAR, THEN, LAST = ("after", "before", "partner"), ("on", "back", "partner_before", "partner_after"), ("partner_left", "partner_right")

    @staticmethod
    def end_near(copies):
        for kind in Spread.NEAR:
            copies[kind].wait()

    @staticmethod
    def start_far(copies):
        for kind in Spread.THEN:
            copies[kind].start()

    @staticmethod
    def end_far(copies):
        for kind in Spread.THEN:
            copies[kind].wait_send()
        for kind in (*Spread.THEN[2:], *Spread.LAST):
            copies[kind].wait_recv()
        for kind in Spread.LAST:
            copies[kind].wait_send()


EARLY = ((0, 32), (1, 32))


def finish_kernel(n, count, layers, pieces, *refs):
    some = len(EARLY)
    squares, *g_in = zip(*[iter(refs[: layers + layers * WEIGHTS])] * layers)
    refs = refs[layers + layers * WEIGHTS :]
    w_in, m_in, v_in, near_m, near_v, far_m, far_v, near_g, w, m, v, far_g, g, refs = split(
        refs, *[WEIGHTS] * 3, *[some] * 5, *[WEIGHTS] * 3, some, WEIGHTS
    )
    parts, m_tile, v_tile, g_tile, load_sem, early_sem, tile_sem, part_send, part_recv, send, recv = refs
    spread = Spread(n, send, recv)
    me = spread.me

    barrier = pltpu.get_barrier_semaphore()
    peers = [lax.rem(me + away, n) for away in range(1, n)]
    for peer in peers:
        pl.semaphore_signal(barrier, inc=1, device_id={"dp": peer}, device_id_type=MESH)

    def rows_of(i, owner, first, rows):
        return pl.ds(pl.multiple_of(owner * g[i].shape[1] + first, 16), rows)

    order = (2, 0, 1)
    loads = {}
    for i in order:
        rows = rows_of(i, me, 0, g[i].shape[1])
        pairs = [(w_in[i].at[:, rows], w[i].at[:, rows]), (m_in[i], m[i]), (v_in[i], v[i])]
        pairs += [(g_in[i][k], g[i].at[k]) for k in range(layers)]
        loads[i] = [pltpu.make_async_copy(src, dst, load_sem.at[i, k]) for k, (src, dst) in enumerate(pairs)]
    first_weight, *other_weights = order
    for one in loads[first_weight]:
        one.start()

    total = sum(t[...] for t in squares)
    parts[pl.ds(me, 1)] = total[None]
    early = []
    for k, (i, some) in enumerate(EARLY):
        near = lambda owner, columns, ref=near_g[k]: ref.at[owner, :, columns]
        far = lambda owner, columns, ref=far_g[k]: ref.at[owner, :, columns]
        early.append(spread.copies(len(pieces) + k, near, g[i].shape[2], None, far))
    pl.semaphore_wait(barrier, n - 1)
    part_copies = []
    for k, peer in enumerate(peers):
        part_copies.append(
            pltpu.make_async_remote_copy(
                parts.at[me], parts.at[me], part_send.at[k], part_recv.at[k], device_id={"dp": peer}, device_id_type=MESH
            )
        )
        part_copies[-1].start()
    for copies in early:
        spread.start_far(copies)
    for one in part_copies:
        one.wait_recv()
    every = parts[0]
    for k in range(1, n):
        every += parts[k]
    mean = jnp.sum(every, keepdims=True) / count
    factor = jnp.minimum(1.0, 0.5 * lax.rsqrt(mean + 1e-30))

    def stepped(grad, m_old, v_old, w_old):
        grad = grad.astype(F32) * factor
        m_new = 0.9 * m_old + 0.1 * grad
        v_new = 0.95 * v_old + 0.05 * grad * grad
        w_old = w_old.astype(F32)
        return m_new, v_new, (w_old - 0.02 * (m_new * lax.rsqrt(v_new + 1e-8) + 0.1 * w_old)).astype(BF16)

    step_rows, width = 16, 256

    def adamw(i, layer, first, rows):
        def body(step):
            start = first + step * step_rows
            at = (layer, pl.ds(pl.multiple_of(start, 16), step_rows), slice(None))
            mine = (layer, rows_of(i, me, start, step_rows), slice(None))
            m[i][at], v[i][at], w[i][mine] = stepped(g[i][at], m[i][at], v[i][at], w[i][mine])

        repeat(0, rows // step_rows, body)

    waited = set()

    def compute(i, layer, first, rows):
        if i not in waited:
            waited.add(i)
            for one in loads[i]:
                one.wait()
        adamw(i, layer, first, rows)

    made = []
    for number, (i, layer, first, rows) in enumerate(pieces):
        place = lambda owner, columns, i=i, layer=layer, first=first, rows=rows: w[i].at[layer, rows_of(i, owner, first, rows), columns]
        made.append(spread.copies(number, place, g[i].shape[2]))

    def own_piece(number):
        compute(*pieces[number])
        spread.start(made[number])

    other = lambda device: device + spread.partner - me
    units = []
    for k, (i, some) in enumerate(EARLY):
        near, far = (near_m[k], near_v[k], near_g[k]), (far_m[k], far_v[k], far_g[k])
        for refs, owners in (
            (near, (spread.partner, spread.after, spread.before)),
            (far, (other(spread.after), other(spread.before), spread.across, other(spread.across))),
        ):
            units += [(refs, i, owner, first, g[i].shape[1] - some) for owner in owners for first in range(0, some, step_rows)]

    def unit_loads(number):
        refs, _, owner, first, _ = units[number]
        slot = number % BUFFERS
        tiles = zip(refs, (m_tile, v_tile, g_tile), strict=True)
        return local_copies([(src.at[owner, pl.ds(first, step_rows)], dst.at[slot]) for src, dst in tiles], tile_sem, slot)

    def unit_rows(number):
        _, i, owner, first, start = units[number]
        return rows_of(i, owner, start + first, step_rows)

    last = layers - 1
    old_rows = local_copies(
        [tuple(t[i].at[last, unit_rows(number)] for t in (w_in, w)) for number, (_, i, _, _, _) in enumerate(units)], early_sem
    )

    def unit(number):
        (_, i, _, _, _), slot = units[number], number % BUFFERS
        if number + 1 < len(units):
            for one in unit_loads(number + 1):
                one.start()
        for one in (*unit_loads(number), old_rows[number]):
            one.wait()

        def body(step):
            columns = pl.ds(pl.multiple_of(step * width, width), width)
            its, at = (last, unit_rows(number), columns), (slot, slice(None), columns)
            *_, w[i][its] = stepped(g_tile[at], m_tile[at], v_tile[at], w[i][its])

        repeat(0, g[i].shape[-1] // width, body)

    own_piece(0)
    for i in other_weights:
        for one in loads[i]:
            one.start()
    for one in old_rows:
        one.start()
    total_pieces, done = len(pieces), 0
    for number in range(total_pieces + 2):
        if number + 1 < total_pieces:
            own_piece(number + 1)
        if number == 0:
            for copies in early:
                spread.pass_last(copies)
        if 1 <= number <= total_pieces:
            spread.pass_on(made[number - 1])
        if 2 <= number:
            spread.pass_last(made[number - 2])
        if number == 2:
            for copies in early:
                spread.end_far(copies)
            for one in unit_loads(0):
                one.start()
        if 3 <= number < total_pieces:
            for k in range(min(3, len(units) - done)):
                unit(done + k)
            done += min(3, len(units) - done)
        if number == 3:
            for i, some in EARLY:
                compute(i, last, g[i].shape[1] - some, some)
    for k in range(done, len(units)):
        unit(k)
    for copies in made:
        spread.end(copies)
    for one in part_copies:
        one.wait_send()


def store_kernel(*refs):
    *refs, sem = refs
    some = len(refs) // 2
    copies = local_copies([(refs[k].at[layer], refs[some + k].at[layer]) for layer in range(refs[0].shape[0]) for k in range(some)], sem)
    for one in copies:
        one.start()
    for one in copies:
        one.wait()


def early_shapes(n, blocks, dtype, times=1, kind=jax.ShapeDtypeStruct):
    return [kind((n, some, blocks[i][0].shape[-1]), dtype) for _ in range(times) for i, some in EARLY]


def finish(n, gradients, squares, weights, m, v, early):
    count = float(sum(w.size for w in weights))
    layers = len(gradients[0])
    pieces = []
    for i in (2, 0, 1):
        rows, _ = gradients[i][0].shape
        for layer in range(layers):
            half = rows // 2
            cuts = [half, half]
            if (i, layer) == (2, 0):
                cuts = [48, half - 48, half]
            elif layer == layers - 1 and i in dict(EARLY):
                rest = half - dict(EARLY)[i]
                cuts = [half + rest - 16, 16] if i == 1 else [half + rest]
            for cut in cuts:
                pieces.append((i, layer, sum(p[3] for p in pieces if p[:2] == (i, layer)), cut))
    anywhere, inside = pl.BlockSpec(memory_space=pl.ANY), pl.BlockSpec(memory_space=pltpu.VMEM)
    dma = pltpu.SemaphoreType.DMA
    results = [*weights, *m, *v]
    tile = lambda dtype: pltpu.VMEM((BUFFERS, 16, max(gradients[i][0].shape[1] for i, _ in EARLY)), dtype)
    ready = pl.pallas_call(
        functools.partial(finish_kernel, n, count, layers, tuple(pieces)),
        out_shape=[pltpu.VMEM(t.shape, t.dtype) for t in results]
        + early_shapes(n, gradients, BF16),
        in_specs=[inside] * layers + [anywhere] * (WEIGHTS * layers + len(results) + len(early)),
        out_specs=[inside] * len(results) + [anywhere] * len(EARLY),
        scratch_shapes=[
            *[pltpu.VMEM((layers, *one[0].shape), BF16) for one in gradients],
            pltpu.VMEM((n, 8, 128), F32), tile(F32), tile(F32), tile(BF16),
            dma((WEIGHTS, layers + 3)), dma((sum(some for _, some in EARLY) // 16 * (n - 1),)), dma((3, BUFFERS)), *[dma((n - 1,))] * 2,
            *Spread.semaphores(len(pieces) + len(EARLY)),
        ],
        compiler_params=pltpu.CompilerParams(collective_id=4, has_side_effects=True, vmem_limit_bytes=8 * MIB),
        name="finish",
    )(*squares, *sum(gradients, ()), *weights, *m, *v, *early)[: len(results)]
    return pl.pallas_call(
        store_kernel,
        out_shape=[jax.ShapeDtypeStruct(t.shape, t.dtype) for t in results],
        in_specs=[inside] * len(results),
        out_specs=[anywhere] * len(results),
        scratch_shapes=[dma((len(results) * layers,))],
        compiler_params=pltpu.CompilerParams(vmem_limit_bytes=8 * MIB),
        name="store",
    )(*[pltpu.with_memory_space_constraint(t, pltpu.VMEM) for t in ready])


def dot(a, b, contract=((1,), (0,))):
    return lax.dot_general(a, b, (contract, ((), ())), preferred_element_type=F32)


def normed(h):
    wide = h.astype(F32)
    return (wide * lax.rsqrt(jnp.mean(wide * wide, -1, keepdims=True) + 1e-6)).astype(BF16)


def by_norm(h, by_a):
    wide = h.astype(F32)
    scale = lax.rsqrt(jnp.mean(wide * wide, -1, keepdims=True) + 1e-6)
    return scale * by_a - wide * (scale * scale * scale * jnp.mean(by_a * wide, -1, keepdims=True))


def by_units(gate, up, by_hidden):
    by_hidden = by_hidden.astype(BF16).astype(F32)
    s = jax.nn.sigmoid(gate)
    silu = gate * s
    return silu * up, by_hidden * up * (s + silu * (1.0 - s)), by_hidden * silu


def forward_kernel(n, *refs):
    (x_in, w_gate, w_up, w_down), moments, outs, early, refs = split(refs, 4, 2 * len(EARLY), 7, 2 * len(EARLY))
    gate_out, up_out, ht_out, at_out, h_out, b_out, bt_out = outs
    (wg, wu, wd, hidden, x, gate, up, hidden_t, a_t, h, b, b_t, w_sem, x_sem, sem, late_sem, send, recv) = refs
    spread = Spread(n, send, recv)
    rows = x.shape[1]
    tiles = x_in.shape[0] // rows
    ff = wg.shape[1]
    width = 256
    groups = [range(at, min(at + 3 * width, ff), width) for at in range(0, ff, 3 * width)]
    tall = lambda ref, t: ref.at[pl.ds(pl.multiple_of(t * rows, rows), rows)]
    wide = lambda ref, t: ref.at[:, pl.ds(pl.multiple_of(t * rows, rows), rows)]

    def load_x(t):
        return pltpu.make_async_copy(tall(x_in, t), x.at[lax.rem(t, x.shape[0])], x_sem.at[lax.rem(t, x.shape[0])])

    def stores(t, first):
        slot = turn(t)
        if first:
            pairs = [(gate, tall(gate_out, t)), (up, tall(up_out, t)), (hidden_t, wide(ht_out, t)), (a_t, wide(at_out, t))]
        else:
            pairs = [(h, tall(h_out, t)), (b, tall(b_out, t)), (b_t, wide(bt_out, t))]
        return local_copies([(src.at[slot], dst) for src, dst in pairs], sem if first else late_sem, slot)

    w_loads = []
    for k, group in enumerate(groups):
        columns = slice(group[0], group[-1] + width)
        w_loads.append([
            pltpu.make_async_copy(src.at[0, :, columns], dst.at[:, columns], w_sem.at[j, k]) for j, (src, dst) in enumerate(((w_gate, wg), (w_up, wu)))
        ])
    down_load = pltpu.make_async_copy(w_down.at[0], wd, w_sem.at[2, 0])
    for one in (load_x(0), *w_loads[0], *w_loads[1], load_x(1)):
        one.start()
    spread.barrier()
    pieces = []
    for number, (src, dst) in enumerate(zip(moments, early, strict=True)):
        some = dst.shape[1]
        own = src.at[src.shape[0] - 1, pl.ds(src.shape[1] - some, some)]
        pieces.append(spread.copies(number, lambda owner, columns, dst=dst: dst.at[owner, :, columns], dst.shape[2], own))
    for copies in pieces:
        spread.start(copies)

    def first_part(t, group, a):
        slot = turn(t)
        for at in group:
            columns = slice(at, at + width)
            g, u = dot(a, wg[:, columns]), dot(a, wu[:, columns])
            gate[slot, :, columns] = g
            up[slot, :, columns] = u
            units = (g * jax.nn.sigmoid(g) * u).astype(BF16)
            hidden[:, columns] = units
            hidden_t[slot, columns] = units.T

    def second_part(t):
        slot = turn(t)
        out = x[lax.rem(t, x.shape[0])] + dot(hidden[...], wd[...]).astype(BF16)
        h[slot] = out
        after = normed(out)
        b[slot] = after
        b_t[slot] = after.T

    def normed_tile(t):
        a = normed(x[lax.rem(t, x.shape[0])])
        a_t[turn(t)] = a.T
        return a

    load_x(0).wait()
    a = normed_tile(0)
    for k, group in enumerate(groups):
        for one in w_loads[k]:
            one.wait()
        for one in w_loads[k + 2] if k + 2 < len(groups) else ([down_load] if k + 2 == len(groups) else []):
            one.start()
        first_part(0, group, a)
    for one in stores(0, True):
        one.start()
    down_load.wait()

    def tile(t):
        load_x(t).wait()

        @pl.when(t + 1 < tiles)
        def _():
            load_x(t + 1).start()

        @pl.when(t >= BUFFERS)
        def _():
            for one in stores(t - BUFFERS, True):
                one.wait()

        @pl.when(t > BUFFERS)
        def _():
            for one in stores(t - 1 - BUFFERS, False):
                one.wait()

        a = normed_tile(t)
        second_part(t - 1)
        first_part(t, range(0, ff, width), a)
        for one in (*stores(t - 1, False), *stores(t, True)):
            one.start()

    repeat(1, tiles, tile)
    last = tiles - 1
    for one in stores(last - BUFFERS, False):
        one.wait()
    second_part(last)
    for one in stores(last, False):
        one.start()
    for copies in pieces:
        spread.end_near(copies)
    for t in (last - 1, last):
        for one in (*stores(t, True), *stores(t, False)):
            one.wait()


def layer_0(n, x, w_gate, w_up, w_down, m, v):
    tokens, d = x.shape
    ff = w_gate.shape[2]
    rows = 256
    anywhere = pl.BlockSpec(memory_space=pl.ANY)
    dma = pltpu.SemaphoreType.DMA
    vmem = lambda *shape: pltpu.VMEM(shape, BF16)
    return pl.pallas_call(
        functools.partial(forward_kernel, n),
        in_specs=[anywhere] * (4 + 2 * len(EARLY)),
        out_specs=[anywhere] * (7 + 2 * len(EARLY)),
        out_shape=[
            pltpu.HBM((tokens, ff), F32),
            pltpu.HBM((tokens, ff), F32),
            pltpu.HBM((ff, tokens), BF16),
            pltpu.HBM((d, tokens), BF16),
            pltpu.HBM((tokens, d), BF16),
            pltpu.HBM((tokens, d), BF16),
            pltpu.HBM((d, tokens), BF16),
            *early_shapes(n, m, F32, 2, pltpu.HBM),
        ],
        scratch_shapes=[
            vmem(d, ff), vmem(d, ff), vmem(ff, d), vmem(rows, ff), vmem(3, rows, d),
            *[pltpu.VMEM((BUFFERS, rows, ff), F32)] * 2, *[vmem(BUFFERS, *t) for t in ((ff, rows), (d, rows), (rows, d), (rows, d), (d, rows))],
            dma((WEIGHTS, 4)), dma((3,)), dma((4, BUFFERS)), dma((3, BUFFERS)), *Spread.semaphores(2 * len(EARLY)),
        ],
        compiler_params=pltpu.CompilerParams(collective_id=1, has_side_effects=True, vmem_limit_bytes=48 * MIB),
        name="forward",
    )(*[pltpu.with_memory_space_constraint(t, pltpu.HBM) for t in (x, w_gate, w_up, w_down, *[t[i] for t in (m, v) for i, _ in EARLY])])


class Exchange:
    def __init__(self, n, refs, kinds, lags):
        self.mine, self.pair, self.out2, self.out3, self.in2, self.in3, self.own, self.side, self.pair_sem, self.sem2, self.sem3 = refs
        self.kinds = kinds
        self.lags = lags
        self.me, self.core, self.partner, self.after, self.before, _ = places("dp", n)
        chips = n // CORES
        self.chip = lax.div(self.me, CORES)
        self.chip_after, self.chip_before, self.chip_across = (lax.rem(self.chip + k, chips) for k in (1, chips - 1, chips // 2))
        half = self.out3.shape[-1]
        self.left, self.right = slice(0, half), slice(half, 2 * half)

    @staticmethod
    def scratch(n, rows, width, lags):
        chips, half, dma = n // CORES, width // 2, pltpu.SemaphoreType.DMA
        _, two, three, four = lags
        slots1, slots2, slots3 = two + 3, 2 * (three - two) + 2, 2 * (four - three) + 2
        return [
            pltpu.VMEM((two + 1, chips, CORES, rows, width), BF16),
            pltpu.VMEM((slots1, chips, rows, width), BF16),
            pltpu.VMEM((2, three - two + 1, rows, width), BF16),
            pltpu.VMEM((2, four - three + 1, rows, half), BF16),
            pltpu.VMEM((2, slots2, rows, width), BF16),
            pltpu.VMEM((2, slots3, rows, half), BF16),
            pltpu.VMEM((four - two + 1, rows, width), F32),
            pltpu.VMEM((2, three - two + 1, rows, half), F32),
            dma((2, slots1)), dma((2, 2, slots2)), dma((2, 2, slots3)),
        ]

    def held(self, p):
        return lax.rem(p, self.mine.shape[0])

    def barrier(self):
        barrier = pltpu.get_barrier_semaphore()
        for peer in (self.partner, self.after, self.before):
            pl.semaphore_signal(barrier, inc=1, device_id={"dp": peer}, device_id_type=MESH)
        pl.semaphore_wait(barrier, 3)

    def copy1(self, p, rows):
        slot = lax.rem(p, self.pair.shape[0])
        return pltpu.make_async_remote_copy(
            self.mine.at[self.held(p), :, 1 - self.core, pl.ds(0, rows)], self.pair.at[slot, :, pl.ds(0, rows)],
            self.pair_sem.at[0, slot], self.pair_sem.at[1, slot], device_id={"dp": self.partner}, device_id_type=MESH,
        )

    def copies(self, p, rows, out, into, sem):
        slot = lax.rem(p, into.shape[1])
        return [
            pltpu.make_async_remote_copy(
                out.at[way, lax.rem(p, out.shape[1]), pl.ds(0, rows)], into.at[way, slot, pl.ds(0, rows)],
                sem.at[0, way, slot], sem.at[1, way, slot], device_id={"dp": to}, device_id_type=MESH,
            )
            for way, to in enumerate((self.after, self.before))
        ]

    def copies2(self, p, rows):
        return self.copies(p, rows, self.out2, self.in2, self.sem2)

    def copies3(self, p, rows):
        return self.copies(p, rows, self.out3, self.in3, self.sem3)

    def stage1(self, p, rows, _):
        self.copy1(p, rows).start()

    def stage2(self, p, rows, _):
        self.copy1(p, rows).wait()
        slot, own, side = (lax.rem(p, t.shape[k]) for t, k in ((self.out2, 1), (self.own, 0), (self.side, 1)))
        at = slice(0, rows)

        def of_chip(chip, columns):
            a = self.mine[self.held(p), chip, self.core, at, columns].astype(F32)
            return a + self.pair[lax.rem(p, self.pair.shape[0]), chip, at, columns].astype(F32)

        self.out2[0, slot, at, self.left] = of_chip(self.chip_across, self.left).astype(BF16)
        self.out2[0, slot, at, self.right] = of_chip(self.chip_after, self.right).astype(BF16)
        self.out2[1, slot, at, self.left] = of_chip(self.chip_before, self.left).astype(BF16)
        self.out2[1, slot, at, self.right] = of_chip(self.chip_across, self.right).astype(BF16)
        for one in self.copies2(p, rows):
            one.start()
        self.side[0, side, at] = of_chip(self.chip_after, self.left)
        self.side[1, side, at] = of_chip(self.chip_before, self.right)
        for columns in (self.left, self.right):
            self.own[own, at, columns] = of_chip(self.chip, columns)

    def stage3(self, p, rows, _):
        for one in self.copies2(p, rows):
            one.wait()
        slot, arrived, own, side = (lax.rem(p, t.shape[k]) for t, k in ((self.out3, 1), (self.in2, 1), (self.own, 0), (self.side, 1)))
        at = slice(0, rows)
        self.out3[0, slot, at] = (self.side[0, side, at] + self.in2[0, arrived, at, self.left].astype(F32)).astype(BF16)
        self.out3[1, slot, at] = (self.side[1, side, at] + self.in2[1, arrived, at, self.right].astype(F32)).astype(BF16)
        for one in self.copies3(p, rows):
            one.start()
        self.own[own, at, self.left] += self.in2[1, arrived, at, self.left].astype(F32)
        self.own[own, at, self.right] += self.in2[0, arrived, at, self.right].astype(F32)

    def stage4(self, p, rows, keep):
        for one in self.copies3(p, rows):
            one.wait()
        arrived, own = lax.rem(p, self.in3.shape[1]), lax.rem(p, self.own.shape[0])
        at = slice(0, rows)
        a = self.own[own, at, self.left] + self.in3[0, arrived, at].astype(F32)
        b = self.own[own, at, self.right] + self.in3[1, arrived, at].astype(F32)
        keep(p, a.astype(BF16), b.astype(BF16))

    def finish(self, step, packets):
        for step in range(step, packets + self.lags[-1]):
            self.move(step, step, step + 1)

    def move(self, step, low, high):
        one, two, three, four = zip(self.lags, (self.stage1, self.stage2, self.stage3, self.stage4), strict=True)
        for lag, stage in (one, three, two, four):
            for first, end, rows, keep in self.kinds:
                if high - 1 - lag < first or low - lag >= end:
                    continue
                p = step - lag
                if low - lag >= first and high - 1 - lag < end:
                    stage(p, rows, keep)
                else:
                    pl.when((p >= first) & (p < end))(functools.partial(stage, p, rows, keep))


def add_squares(total, *blocks):
    for block in blocks:
        wide = block.astype(F32)
        wide = wide * wide
        rows, columns = wide.shape
        sums = [wide[r : r + 8, c : c + 128] for r in range(0, rows, 8) for c in range(0, columns, 128)]
        while len(sums) > 1:
            sums = [a + b for a, b in zip(sums[::2], sums[1::2])] + ([sums[-1]] if len(sums) % 2 else [])
        total[...] += sums[0]


def keep_columns(first, gate, up, width, squares):
    def keep(p, left, right):
        columns = pl.ds(pl.multiple_of((p - first) * width, width), width)
        gate[:, columns] = left
        up[:, columns] = right
        add_squares(squares, left, right)

    return keep


def keep_tall(first, down, rows, width, squares):
    def keep(p, left, right):
        columns = pl.ds(pl.multiple_of((p - first) * width, width), width)
        down[:rows, columns] = left
        down[rows:, columns] = right
        add_squares(squares, left, right)

    return keep


def keep_down(first, down, rows, width, squares):
    def keep(p, left, right):
        half = width // 2
        which = p - first
        at = pl.ds(pl.multiple_of(lax.rem(which, 2) * rows, 16), rows)
        start = lax.div(which, 2) * width
        down[at, pl.ds(pl.multiple_of(start, half), half)] = left
        down[at, pl.ds(pl.multiple_of(start + half, half), half)] = right
        add_squares(squares, left, right)

    return keep


def tall_packet(exchange, step, first, hidden_t, by_out):
    _, chips, cores, rows, width = exchange.mine.shape
    half = width // 2
    by_out = by_out[:, pl.ds(pl.multiple_of((step - first) * half, half), half)]
    for k in range(chips * cores):
        block = dot(hidden_t[2 * rows * k : 2 * rows * (k + 1), :], by_out).astype(BF16)
        for part in range(2):
            exchange.mine[exchange.held(step), k // cores, k % cores, :, part * half : (part + 1) * half] = block[part * rows : (part + 1) * rows]


def down_packet(exchange, step, first, hidden_t, by_out):
    n_rows = hidden_t.shape[0]
    _, chips, cores, rows, width = exchange.mine.shape
    which = step - first
    start = pl.multiple_of(lax.rem(which, 2) * rows, 16)
    columns = pl.ds(pl.multiple_of(lax.div(which, 2) * width, width), width)
    share = n_rows // (chips * cores)
    by_out = by_out[:, columns]
    for k in range(chips * cores):
        lhs = hidden_t[pl.ds(pl.multiple_of(k * share + start, 16), rows), :]
        exchange.mine[exchange.held(step), k // cores, k % cores] = dot(lhs, by_out).astype(BF16)


def wide_packet(exchange, step, a_t, by_both):
    _, chips, cores, _, width = exchange.mine.shape
    rows = a_t.shape[0] // (chips * cores)
    half = width // 2
    for k in range(2):
        columns = slice(k * half, k * half + half)
        block = dot(a_t[...], by_both[:, columns]).astype(BF16)
        exchange.mine[exchange.held(step), :, :, pl.ds(0, rows), columns] = block.reshape(chips, cores, rows, half)


MB = 1024
TOP_LAGS = (0, 1, 4, 6)
BOTTOM_LAGS = (0, 1, 5, 9)


def top_kernel(n, *refs):
    several = 2 * len(EARLY)
    ins, near, outs, far, (send, recv), refs = split(refs, 7, several, 7, several, 2)
    a_in, at_in, h_in, dy, w_gate, w_up, w_down = ins
    g_gate, g_up, g_down, squares, by_h, bg_hbm, bu_hbm = outs
    spread = Spread(n, send, recv)
    (a, a_t, wg, wu, hidden_t, wd, both, h_tile, by_tile, load_sem, wd_sem, both_sem, tile_sem, by_sem), refs = split(refs, 14)
    tokens, d = a.shape
    ff = wg.shape[1]
    width = 256
    chunks = ff // width
    downs = 4
    wide_rows, down_rows = d // n, ff // n // 2
    exchange = Exchange(
        n, refs,
        (
            (0, chunks, wide_rows, keep_columns(0, g_gate, g_up, width, squares)),
            (chunks, chunks + downs, down_rows, keep_tall(chunks, g_down, down_rows, width, squares)),
        ),
        TOP_LAGS,
    )
    layer = w_gate.shape[0] - 1
    first, rest = pl.ds(0, width), pl.ds(width, ff - width)
    columns_of = lambda columns: [(src.at[layer, :, columns], dst.at[:, columns]) for src, dst in ((w_gate, wg), (w_up, wu))]
    loads = local_copies([(a_in, a), (at_in, a_t), *columns_of(first), *columns_of(rest)], load_sem)
    def down_chunk(c):
        slot = turn(c)
        return pltpu.make_async_copy(w_down.at[layer, pl.ds(pl.multiple_of(c * width, width), width)], wd.at[slot], wd_sem.at[slot])

    loads, later_loads = split(loads, 4)
    for one in (*loads, down_chunk(0)):
        one.start()
    squares[...] = jnp.zeros_like(squares)
    exchange.barrier()

    early = []
    for number, (src, dst) in enumerate(zip(near, far, strict=True)):
        places = [lambda owner, columns, ref=ref: ref.at[owner, :, columns] for ref in (src, dst)]
        early.append(spread.copies(number, places[0], src.shape[2], None, places[1]))
    for copies in early:
        spread.start_far(copies)

    def store_both(c):
        slot = turn(c)
        to = pl.ds(pl.multiple_of(c * width, width), width)
        return local_copies([(both.at[slot, :, pl.ds(k * width, width)], ref.at[:, to]) for k, ref in enumerate((bg_hbm, bu_hbm))], both_sem, slot)

    def chunk(c):
        slot = turn(c)

        @pl.when(c == 0)
        def _():
            for one in loads:
                one.wait()
            for one in later_loads:
                one.start()

        @pl.when(c == 1)
        def _():
            for one in later_loads:
                one.wait()

        @pl.when(c >= BUFFERS)
        def _():
            for one in store_both(c - BUFFERS):
                one.wait()

        @pl.when(c == chunks // 2)
        def _():
            for copies in early:
                spread.pass_last(copies)

        down_chunk(c).wait()

        @pl.when(c + 1 < chunks)
        def _():
            down_chunk(c + 1).start()

        columns = pl.ds(pl.multiple_of(c * width, width), width)
        wg_c, wu_c, wd_c = wg[:, columns], wu[:, columns], wd[slot]
        for at in range(0, tokens, MB):
            rows = slice(at, at + MB)
            hidden, by_gate, by_up = by_units(dot(a[rows], wg_c), dot(a[rows], wu_c), dot(dy[rows], wd_c, TRANSPOSED))
            hidden_t[columns, rows] = hidden.astype(BF16).T
            both[slot, rows, :width] = by_gate.astype(BF16)
            both[slot, rows, width:] = by_up.astype(BF16)
        wide_packet(exchange, c, a_t, both.at[slot])
        for one in store_both(c):
            one.start()
        exchange.move(c, 0, chunks)

    repeat(0, chunks, chunk)
    for c in range(chunks - BUFFERS, chunks):
        for one in store_both(c):
            one.wait()

    tile_rows = 256
    tiles = tokens // tile_rows
    split_at = a_t.shape[1]

    def tile_loads(t):
        slot = turn(t)
        rows = pl.ds(pl.multiple_of(t * tile_rows, tile_rows), tile_rows)
        pairs = [(h_in.at[rows], h_tile.at[slot])]
        for k, src in enumerate((bg_hbm, bu_hbm)):
            to = pl.ds(pl.multiple_of((slot * 2 + k) * tile_rows, tile_rows), tile_rows)
            pairs.append((src.at[rows, pl.ds(0, split_at)], a_t.at[to]))
            pairs.append((src.at[rows, pl.ds(split_at, ff - split_at)], a.at[to, pl.ds(0, ff - split_at)]))
        return local_copies(pairs, tile_sem, slot)

    def tile_store(t):
        slot = turn(t)
        return pltpu.make_async_copy(by_tile.at[slot], by_h.at[pl.ds(pl.multiple_of(t * tile_rows, tile_rows), tile_rows)], by_sem.at[slot])

    for one in tile_loads(0):
        one.start()

    def tile(step):
        t = step - chunks

        @pl.when(t < downs)
        def _():
            tall_packet(exchange, step, chunks, hidden_t, dy)

        exchange.move(step, chunks, chunks + tiles)
        slot = turn(t)
        for one in tile_loads(t):
            one.wait()

        @pl.when(t + 1 < tiles)
        def _():
            for one in tile_loads(t + 1):
                one.start()

        @pl.when(t >= BUFFERS)
        def _():
            tile_store(t - BUFFERS).wait()

        total = None
        for k, w in enumerate((wg, wu)):
            at = pl.ds(pl.multiple_of((slot * 2 + k) * tile_rows, tile_rows), tile_rows)
            term = dot(a_t[at], w[:, :split_at], TRANSPOSED) + dot(a[at, : ff - split_at], w[:, split_at:], TRANSPOSED)
            total = term if total is None else total + term
        rows = pl.ds(pl.multiple_of(t * tile_rows, tile_rows), tile_rows)
        by_tile[slot] = (dy[rows].astype(F32) + by_norm(h_tile[slot], total)).astype(BF16)
        tile_store(t).start()

    repeat(chunks, chunks + tiles, tile)
    exchange.finish(chunks + tiles, chunks + downs)
    for t in range(tiles - BUFFERS, tiles):
        tile_store(t).wait()
    for copies in early:
        spread.end_far(copies)


def top_layer(n, a, a_t, h, dy, w_gate, w_up, w_down, near):
    tokens, d = a.shape
    ff = w_gate.shape[2]
    width = 256
    anywhere, inside = pl.BlockSpec(memory_space=pl.ANY), pl.BlockSpec(memory_space=pltpu.VMEM)
    dma = pltpu.SemaphoreType.DMA
    return pl.pallas_call(
        functools.partial(top_kernel, n),
        in_specs=[*[anywhere] * 3, inside, *[anywhere] * (3 + len(near))],
        out_specs=[inside] * 4 + [anywhere] * (3 + len(near)),
        out_shape=[
            jax.ShapeDtypeStruct((d // n, ff), BF16),
            jax.ShapeDtypeStruct((d // n, ff), BF16),
            jax.ShapeDtypeStruct((ff // n, d), BF16),
            jax.ShapeDtypeStruct((8, 128), F32),
            jax.ShapeDtypeStruct((tokens, d), BF16),
            jax.ShapeDtypeStruct((tokens, ff), BF16),
            jax.ShapeDtypeStruct((tokens, ff), BF16),
            *[jax.ShapeDtypeStruct(t.shape, t.dtype) for t in near],
        ],
        scratch_shapes=[
            *Spread.semaphores(len(near)),
            *[pltpu.VMEM(t, BF16) for t in ((tokens, d), (d, tokens), (d, ff), (d, ff), (ff, tokens))],
            *[pltpu.VMEM((BUFFERS, *t), BF16) for t in ((width, d), (tokens, 2 * width), (width, d), (width, d))],
            dma((6,)), dma((BUFFERS,)), dma((2, BUFFERS)), dma((5, BUFFERS)), dma((BUFFERS,)),
            *Exchange.scratch(n, ff // n // 2, 2 * width, TOP_LAGS),
        ],
        compiler_params=pltpu.CompilerParams(collective_id=2, has_side_effects=True, vmem_limit_bytes=ALL_VMEM - 9 * MIB // 2),
        name="top",
    )(a, a_t, h, pltpu.with_memory_space_constraint(dy, pltpu.VMEM), w_gate, w_up, w_down, *near)


def bottom_kernel(n, *refs):
    some = len(EARLY)
    ins, summed, (g_gate, g_up, g_down, squares), near, (send, recv), refs = split(refs, 6, some, 4, some, 2)
    by_in, ht_in, at_in, gate_in, up_in, w_down = ins
    spread = Spread(n, send, recv)
    (by, hidden_t, a_t, wd, gate, up, both, load_sem, unit_sem), refs = split(refs, 9)
    tokens, d = by.shape
    ff = hidden_t.shape[0]
    width = 256
    chunks = ff // width
    downs = 4
    wide_rows, down_rows = d // n, ff // n // 2
    exchange = Exchange(
        n, refs,
        (
            (0, downs, down_rows, keep_down(0, g_down, down_rows, 2 * width, squares)),
            (downs, downs + chunks, wide_rows, keep_columns(downs, g_gate, g_up, width, squares)),
        ),
        BOTTOM_LAGS,
    )
    share = ff // n
    halves = lambda ref, k: ref.at[:, pl.ds(k * 2 * width, 2 * width)]
    pairs = [(halves(by_in, 0), halves(by, 0))]
    for k in range(2):
        for to in range(n):
            rows = pl.ds(to * share + k * down_rows, down_rows)
            pairs.append((ht_in.at[rows], hidden_t.at[rows]))
    pairs += [(halves(by_in, 1), halves(by, 1)), (at_in, a_t)]
    loads = local_copies(pairs, load_sem)

    def chunk_loads(c):
        slot = turn(c)
        columns = pl.ds(pl.multiple_of(c * width, width), width)
        pairs = [(w_down.at[0, columns], wd.at[slot]), (gate_in.at[:, columns], gate.at[slot]), (up_in.at[:, columns], up.at[slot])]
        return local_copies(pairs, unit_sem, slot)

    first, second, third = split(loads, 1 + n, n)
    third += chunk_loads(0)
    for one in first:
        one.start()
    squares[...] = jnp.zeros_like(squares)
    exchange.barrier()

    early = []
    for number, (src, dst) in enumerate(zip(summed, near, strict=True)):
        some = dst.shape[1]
        own = src.at[pl.ds(src.shape[0] - some, some)]
        early.append(spread.copies(number, lambda owner, columns, dst=dst: dst.at[owner, :, columns], dst.shape[2], own))
    for copies in early:
        spread.start(copies)

    def down(step):
        @pl.when(step == 0)
        def _():
            for one in first:
                one.wait()
            for one in second:
                one.start()

        @pl.when(step == 1)
        def _():
            for one in second:
                one.wait()
            for one in third:
                one.start()

        @pl.when(step == 2)
        def _():
            for one in third[:2]:
                one.wait()

        down_packet(exchange, step, 0, hidden_t, by)
        exchange.move(step, 0, downs)

    repeat(0, downs, down)

    def chunk(step):
        c = step - downs
        slot = turn(c)
        for one in chunk_loads(c):
            one.wait()

        @pl.when(c + 1 < chunks)
        def _():
            for one in chunk_loads(c + 1):
                one.start()

        wd_c = wd[slot]
        for at in range(0, tokens, MB):
            rows = slice(at, at + MB)
            _, by_gate, by_up = by_units(gate[slot, rows], up[slot, rows], dot(by[rows], wd_c, TRANSPOSED))
            both[rows, :width] = by_gate.astype(BF16)
            both[rows, width:] = by_up.astype(BF16)
        wide_packet(exchange, step, a_t, both)
        exchange.move(step, downs, downs + chunks)

    repeat(downs, downs + chunks, chunk)
    exchange.finish(downs + chunks, downs + chunks)
    for copies in early:
        spread.end_near(copies)


def bottom_layer(n, by, hidden_t, a_t, gate, up, w_down, summed):
    tokens, d = by.shape
    ff = hidden_t.shape[0]
    width = 256
    anywhere, inside = pl.BlockSpec(memory_space=pl.ANY), pl.BlockSpec(memory_space=pltpu.VMEM)
    dma = pltpu.SemaphoreType.DMA
    return pl.pallas_call(
        functools.partial(bottom_kernel, n),
        in_specs=[anywhere] * (6 + len(summed)),
        out_specs=[inside] * 4 + [anywhere] * len(summed),
        out_shape=[
            jax.ShapeDtypeStruct((d // n, ff), BF16),
            jax.ShapeDtypeStruct((d // n, ff), BF16),
            jax.ShapeDtypeStruct((ff // n, d), BF16),
            jax.ShapeDtypeStruct((8, 128), F32),
            *[jax.ShapeDtypeStruct((n, some, ff), BF16) for _, some in EARLY],
        ],
        scratch_shapes=[
            *Spread.semaphores(len(summed)),
            *[pltpu.VMEM(t, BF16) for t in ((tokens, d), (ff, tokens), (d, tokens), (BUFFERS, width, d))],
            *[pltpu.VMEM((BUFFERS, tokens, width), F32)] * 2, pltpu.VMEM((tokens, 2 * width), BF16),
            dma((3 + 2 * n,)), dma((3, BUFFERS)),
            *Exchange.scratch(n, ff // n // 2, 2 * width, BOTTOM_LAGS),
        ],
        compiler_params=pltpu.CompilerParams(collective_id=3, has_side_effects=True, vmem_limit_bytes=ALL_VMEM),
        name="bottom",
    )(by, hidden_t, a_t, gate, up, w_down, *summed)


def solution(mesh):
    n = mesh.shape["dp"]

    def step(x, dy, w_gate, w_up, w_down, *moments):
        m, v = split(moments, WEIGHTS)
        gate, up, hidden_t, a_t, h, next_a, next_a_t, *early = layer_0(n, x[0], w_gate, w_up, w_down, m, v)
        top = top_layer(n, next_a, next_a_t, h, dy[0], w_gate, w_up, w_down, early)
        top, (squares_1, by_h, _, _), far = split(top, WEIGHTS, 4)
        bottom = bottom_layer(n, by_h, hidden_t, a_t, gate, up, w_down, [top[i] for i, _ in EARLY])
        bottom, (squares_0,), near = split(bottom, WEIGHTS, 1)
        gradients = list(zip(bottom, top, strict=True))
        return tuple(finish(n, gradients, (squares_0, squares_1), (w_gate, w_up, w_down), m, v, (*early, *far, *near)))

    sharded = P(None, "dp", None)
    return jax.shard_map(
        step,
        mesh=mesh,
        in_specs=(P(("rep", "dp")), P(("rep", "dp")), P(), P(), P(), *[sharded] * 6),
        out_specs=(*[P("rep")] * 3, *[P("rep", "dp")] * 6),
        check_vma=False,
    )
```
